32 devices in a mesh: seg: 4 (over z), ch: 8 (over y, x, core).
Axes of the slice: x: 2, y: 2, z: 4, core: 2. Of those that a mesh axis runs over, the one named last changes fastest.
Arguments:
- gate_in: bfloat16 [1536, 16384], P('ch', 'seg'), may hold values from -6 to 6
- key_in: bfloat16 [1536, 16384], P('ch', 'seg'), may hold values from -6 to 6
- value_in: bfloat16 [1536, 16384], P('ch', 'seg'), may hold values from -6 to 6
- kernel: float32 [1536, 16384], P('ch'), may hold values from -0.046875 to 0.046875
- skip_gain: float32 [1536], P('ch'), may hold values from -1 to 1
- out_weight: bfloat16 [1536, 1536], P('ch'), may hold values from -0.15625 to 0.15625
Outputs:
- output: bfloat16 [16384, 1536], P(('seg', 'ch'))
The draws below stay inside these ranges and needn't reach their ends.
All inputs are finite; a program needn't handle non-finite values.
Results may differ from the reference program's by a relative error of at most 0.0095.
Values may be sent and summed in bfloat16 or wider, within the bound.
A program may use at most 128 MiB of HBM per device.

```python
import jax
import jax.numpy as jnp
from jax import lax

D = 1536
SEQ = 16384


def level_of(rng, extent, cuts, least, top_value):
    level = 1.0
    for axis_at, shards_of in cuts:
        heights = jax.random.uniform(jax.random.fold_in(jax.random.fold_in(rng, 6), axis_at), (shards_of,), jnp.float32, least / len(cuts), top_value / len(cuts))
        level = level * jnp.repeat(jnp.exp(heights), extent[axis_at] // shards_of).reshape((-1,) + (1,) * (len(extent) - 1 - axis_at))
    return level


def bell_draw(key, extent, deviation, bound, split=(), dtype=jnp.bfloat16):
    drawn = deviation * jax.random.normal(key, extent, jnp.float32)
    if split:
        drawn = drawn * level_of(key, extent, split, -0.22, 0.18)
    return jnp.clip(drawn, -bound, bound).astype(dtype)


def setup_inputs(seed: int = 0) -> dict:
    key_list = jax.random.split(jax.random.key(seed), 7)
    gate_in = bell_draw(key_list[0], (D, SEQ), 1.0, 6.0, ((0, 8), (1, 4)))
    key_in = bell_draw(key_list[1], (D, SEQ), 1.0, 6.0, ((0, 8), (1, 4)))
    value_in = bell_draw(key_list[2], (D, SEQ), 1.0, 6.0, ((0, 8), (1, 4)))
    kernel = bell_draw(key_list[3], (D, SEQ), SEQ ** -0.5, 0.046875, ((0, 8),), jnp.float32)
    skip_gain = jnp.clip(jax.random.uniform(key_list[4], (D,), jnp.float32, -1.0, 1.0) * level_of(key_list[4], (D,), ((0, 8),), -0.4, 0.0), -1.0, 1.0)
    out_weight = bell_draw(key_list[5], (D, D), D ** -0.5, 0.15625, ((0, 8),))
    return dict(gate_in=gate_in, key_in=key_in, value_in=value_in, kernel=kernel, skip_gain=skip_gain, out_weight=out_weight)


def reference(gate_in, key_in, value_in, kernel, skip_gain, out_weight):
    mixed_in = key_in.astype(jnp.float32) * value_in.astype(jnp.float32)
    length = mixed_in.shape[1]
    product = jnp.fft.rfft(mixed_in, n=2 * length, axis=1) * jnp.fft.rfft(kernel, n=2 * length, axis=1)
    convolved = jnp.fft.irfft(product, n=2 * length, axis=1)[:, :length]
    gated = (gate_in.astype(jnp.float32) * (convolved + skip_gain[:, None] * mixed_in)).astype(jnp.bfloat16)
    result = lax.dot_general(gated, out_weight, (((0,), (0,)), ((), ())), preferred_element_type=jnp.float32)
    return result.astype(jnp.bfloat16)
```

```python
import functools
import math

import jax
import jax.numpy as jnp
import numpy as np
from jax import lax
from jax.experimental import pallas as pl
from jax.experimental.pallas import tpu as pltpu
from jax.sharding import PartitionSpec as P

lane_width = 128
bf16 = jnp.bfloat16
f32 = jnp.float32


def angles(rows, cols, period):
    theta = (rows[:, None] * cols[None, :] % (4 * period)) * (2.0 * math.pi / (4 * period))
    return np.cos(theta), np.sin(theta)


def make_tables(outer):
    quarter = 4 * np.arange(outer) + 1
    row = np.arange(outer)
    lane = np.arange(lane_width)
    cos_o, sin_o = angles(quarter, row, outer)
    cos_t, sin_t = angles(quarter, lane, outer * lane_width)
    cos_i, sin_i = angles(4 * lane, lane, lane_width)
    first = np.concatenate([cos_o, -sin_o], axis=0)
    last = np.concatenate([cos_o.T, -sin_o.T], axis=1) / (outer * lane_width)
    inner = np.block([[cos_i, -sin_i], [sin_i, cos_i]])
    inner_back = np.block([[cos_i, sin_i], [-sin_i, cos_i]])
    narrow = [jnp.asarray(m.astype(np.float32).astype(bf16)) for m in (first, last, inner, inner_back)]
    return (*narrow, jnp.asarray(cos_t.astype(np.float32)), jnp.asarray(sin_t.astype(np.float32)))


def forward(signal, first, inner, cos_t, sin_t):
    outer = cos_t.shape[0]
    rows = []
    for at in range(0, len(signal), 2):
        pair = signal[at : at + 2]
        wide = jnp.dot(first, jnp.concatenate(pair, axis=1), preferred_element_type=f32)
        for i in range(len(pair)):
            part = wide[:, i * lane_width : (i + 1) * lane_width]
            real, imag = part[:outer], part[outer:]
            rows.append(
                jnp.concatenate(
                    [
                        (real * cos_t + imag * sin_t).astype(bf16),
                        (imag * cos_t - real * sin_t).astype(bf16),
                    ],
                    axis=1,
                )
            )
    return jnp.dot(jnp.concatenate(rows, axis=0), inner, preferred_element_type=f32)


def filter_kernel(first, inner, cos_t, sin_t, taps, spectrum):
    count, outer = taps.shape[0], taps.shape[1]
    signal = [taps[i].astype(bf16) for i in range(count)]
    out = forward(signal, first[...], inner[...], cos_t[...], sin_t[...])
    spectrum[...] = out.astype(bf16).reshape(count, outer, 2 * lane_width)


def convolve_block(tables, signal, filt):
    first, last, inner, inner_back, cos, sin = tables
    outer = cos.shape[0]
    sig = forward(signal, first, inner, cos, sin)
    filt = filt.astype(f32)
    sig_re, sig_im = sig[:, :lane_width], sig[:, lane_width:]
    filt_re, filt_im = filt[:, :lane_width], filt[:, lane_width:]
    prod = jnp.concatenate(
        [
            (filt_re * sig_re - filt_im * sig_im).astype(bf16),
            (filt_re * sig_im + filt_im * sig_re).astype(bf16),
        ],
        axis=1,
    )
    back = jnp.dot(prod, inner_back, preferred_element_type=f32)
    parts = []
    for at in range(0, len(signal), 2):
        cols = []
        for i in range(at, min(at + 2, len(signal))):
            rows = back[i * outer : (i + 1) * outer]
            real, imag = rows[:, :lane_width], rows[:, lane_width:]
            cols.append(
                jnp.concatenate(
                    [
                        (real * cos - imag * sin).astype(bf16),
                        (imag * cos + real * sin).astype(bf16),
                    ],
                    axis=0,
                )
            )
        wide = jnp.dot(last, jnp.concatenate(cols, axis=1), preferred_element_type=f32)
        for i in range(len(cols)):
            parts.append(wide[:, i * lane_width : (i + 1) * lane_width])
    return parts


def conv_kernel(first, last, inner, inner_back, cos_t, sin_t, mixed, spectrum, conv):
    count, outer = mixed.shape[0], mixed.shape[1]
    tables = (first[...], last[...], inner[...], inner_back[...], cos_t[...], sin_t[...])
    filt = spectrum[...].reshape(count * outer, 2 * lane_width)
    parts = convolve_block(tables, [mixed[i] for i in range(count)], filt)
    for i in range(count):
        conv[i] = parts[i].astype(bf16)


def whole(array):
    return pl.BlockSpec(array.shape, lambda i: (0,) * array.ndim)


def block_of(count):
    return max(b for b in range(1, 9) if count % b == 0)


def transform_filter(tables, taps):
    first, last, inner, inner_back, cos_t, sin_t = tables
    count, outer, lanes = taps.shape
    block = block_of(count)
    fixed = (first, inner, cos_t, sin_t)
    return pl.pallas_call(
        filter_kernel,
        grid=(count // block,),
        in_specs=[whole(a) for a in fixed] + [pl.BlockSpec((block, outer, lanes), lambda i: (i, 0, 0))],
        out_specs=pl.BlockSpec((block, outer, 2 * lanes), lambda i: (i, 0, 0)),
        out_shape=jax.ShapeDtypeStruct((count, outer, 2 * lanes), bf16),
        cost_estimate=pl.CostEstimate(
            flops=count * outer * lanes * 1536, bytes_accessed=count * outer * lanes * 8, transcendentals=0
        ),
        name="filter_transform",
    )(*fixed, taps)


def convolve(tables, mixed, spectrum):
    count, outer, lanes = mixed.shape
    block = block_of(count)
    return pl.pallas_call(
        conv_kernel,
        grid=(count // block,),
        in_specs=[whole(a) for a in tables]
        + [
            pl.BlockSpec((block, outer, lanes), lambda i: (i, 0, 0)),
            pl.BlockSpec((block, outer, 2 * lanes), lambda i: (i, 0, 0)),
        ],
        out_specs=pl.BlockSpec((block, outer, lanes), lambda i: (i, 0, 0)),
        out_shape=jax.ShapeDtypeStruct((count, outer, lanes), bf16),
        cost_estimate=pl.CostEstimate(
            flops=count * outer * lanes * 3072, bytes_accessed=count * outer * lanes * 8, transcendentals=0
        ),
        name="convolve",
    )(*tables, mixed, spectrum)


MESH = pl.DeviceIdType.MESH


def layer_kernel(
    first, last, inner, inner_back, cos_t, sin_t, skip, key, value, gate, kernel, weight,
    output,
    keys, values, taps, tall, wide, long, spectrum, mixed_out, mixed_in, conv_out, conv_in,
    gates, weights, stacked, gated, total, result,
    kv_sem, taps_sem, here_sem, result_sem, ready,
    in_send, in_recv, out_send, out_recv, g_send, g_recv, w_send, w_recv,
):
    chunks, segs, chans, tokens = key.shape
    groups = gates.shape[0]
    share = tokens // groups
    quads = share // lane_width
    features = weight.shape[-1]
    outer = cos_t.shape[0]
    slabs = tokens // lane_width
    step = slabs + 8
    long_step = outer + 8
    block = segs * chans
    depth = groups * block
    cols = result.shape[-1]
    s = lax.axis_index("seg")
    h = lax.axis_index("ch")

    def seg_peer(d):
        return lax.rem(s + d, segs)

    def ch_peer(d):
        return lax.rem(h + d, groups)

    def lanes(j):
        return pl.ds(pl.multiple_of(j * lane_width, lane_width), lane_width)

    barrier = pltpu.get_barrier_semaphore()
    for d in range(1, segs):
        pl.semaphore_signal(barrier, inc=1, device_id=(seg_peer(d), h), device_id_type=MESH)
    for d in range(1, groups):
        pl.semaphore_signal(barrier, inc=1, device_id=(s, ch_peer(d)), device_id_type=MESH)

    def load_kv(k):
        return (
            pltpu.make_async_copy(key.at[k], keys.at[k], kv_sem.at[0, k]),
            pltpu.make_async_copy(value.at[k], values.at[k], kv_sem.at[1, k]),
        )

    for k in range(chunks):
        for copy in load_kv(k):
            copy.start()
    fetch = pltpu.make_async_copy(kernel.at[:, s], taps, taps_sem)
    fetch.start()

    def part_of(peer):
        return pl.ds(pl.multiple_of(peer * share, lane_width), share)

    own_gate = pltpu.make_async_copy(gate.at[:, :, :, part_of(h)], gates.at[h], here_sem.at[0])
    own_weight = pltpu.make_async_copy(weight, weights.at[h], here_sem.at[1])
    own_gate.start()
    own_weight.start()

    def send_in(k, d):
        return pltpu.make_async_remote_copy(
            src_ref=mixed_out.at[k, d], dst_ref=mixed_in.at[k, s],
            send_sem=in_send.at[k, d], recv_sem=in_recv.at[k, d],
            device_id=(seg_peer(d), h), device_id_type=MESH,
        )

    def send_gate(d):
        peer = ch_peer(d)
        return pltpu.make_async_remote_copy(
            src_ref=gate.at[:, :, :, part_of(peer)], dst_ref=gates.at[h],
            send_sem=g_send.at[d], recv_sem=g_recv.at[d],
            device_id=(s, peer), device_id_type=MESH,
        )

    def send_weight(d):
        return pltpu.make_async_remote_copy(
            src_ref=weight, dst_ref=weights.at[h],
            send_sem=w_send.at[d], recv_sem=w_recv.at[d],
            device_id=(s, ch_peer(d)), device_id_type=MESH,
        )

    def out_rows(seg, peer):
        return pl.ds(seg * slabs + peer * quads, quads)

    for k in range(chunks):
        for copy in load_kv(k):
            copy.wait()
        for d in far_first(segs):
            peer = seg_peer(d)

            def mix(j, carry):
                both = keys[k, peer, :, lanes(j)].astype(f32) * values[k, peer, :, lanes(j)].astype(f32)
                wide[pl.ds(j, chans, stride=step), :] = both
                return carry

            lax.fori_loop(0, slabs, mix, 0, unroll=4)
            into = mixed_out.at[k, d] if d else mixed_in.at[k, s]
            for i in range(chans):
                into[i] = wide[i * step : i * step + slabs, :].astype(bf16)
        if k == 0:
            pl.semaphore_wait(barrier, segs + groups - 2)
        for d in far_first(segs):
            if d:
                send_in(k, d).start()
        if k == 0:
            for d in range(1, groups):
                send_gate(d).start()
            for d in range(1, segs):
                pl.semaphore_signal(ready, inc=1, device_id=(seg_peer(d), h), device_id_type=MESH)
    for d in range(1, groups):
        send_weight(d).start()

    fetch.wait()
    for k in range(chunks):

        def spread(j, carry):
            tall[pl.ds(j, chans, stride=long_step), :] = taps[k, :, lanes(j)]
            return carry

        lax.fori_loop(0, outer, spread, 0, unroll=4)
        signal = [tall[i * long_step : i * long_step + outer, :].astype(bf16) for i in range(chans)]
        out = forward(signal, first[...], inner[...], cos_t[...], sin_t[...])
        spectrum[k] = out.astype(bf16).reshape(chans, outer, 2 * lane_width)
    pl.semaphore_wait(ready, segs - 1)

    for k in range(chunks):
        for d in range(1, segs):
            send_in(k, d).wait_recv()
        signal = [mixed_in[k, :, i].reshape(outer, lane_width) for i in range(chans)]
        filt = spectrum[k].reshape(chans * outer, 2 * lane_width)
        tables = (first[...], last[...], inner[...], inner_back[...], cos_t[...], sin_t[...])
        parts = convolve_block(tables, signal, filt)
        for i in range(chans):
            level = skip[(k * segs + s) * chans + i]
            long[i * long_step : i * long_step + outer, :] = parts[i] + level * signal[i].astype(f32)

        def gather(j, carry):
            conv_out[k, j] = long[pl.ds(j, chans, stride=long_step), :].astype(bf16)
            return carry

        lax.fori_loop(0, outer, gather, 0, unroll=8)
        for d in far_first(segs):
            seg = seg_peer(d)

            def send(e, carry):
                peer = ch_peer(e)
                pltpu.make_async_remote_copy(
                    src_ref=conv_out.at[k, out_rows(seg, peer)], dst_ref=conv_in.at[k, h, s],
                    send_sem=out_send.at[k], recv_sem=out_recv.at[k],
                    device_id=(seg, peer), device_id_type=MESH,
                ).start()
                return carry

            lax.fori_loop(0 if d else 1, groups, send, 0)
        for q in range(quads):
            conv_in[k, h, s, q] = conv_out[k, s * slabs + h * quads + q]

    own_gate.wait()
    own_weight.wait()
    for d in range(1, groups):
        send_gate(d).wait()
        send_weight(d).wait()
    for k in range(chunks):

        def restack(g, carry):
            for at in range(0, segs, 2):
                pair = [weights[g, k, at + e].astype(f32) for e in range(2)]
                rows = pl.ds(pl.multiple_of(g * block + at * chans, 2 * chans), 2 * chans)
                stacked[k, rows, :] = jnp.concatenate(pair, axis=0).astype(bf16)
            return carry

        lax.fori_loop(0, groups, restack, 0)

    outs = []
    for k in range(chunks):
        pieces = pltpu.make_async_remote_copy(
            src_ref=conv_out.at[k, pl.ds(0, outer - quads)], dst_ref=conv_out.at[k, pl.ds(0, outer - quads)],
            send_sem=out_send.at[k], recv_sem=out_recv.at[k],
            device_id=(seg_peer(1), h), device_id_type=MESH,
        )
        pieces.wait_recv()

        def combine(g, carry):
            for at in range(0, segs, 2):
                for q in range(quads):
                    both = [
                        conv_in[k, g, at + e, q].astype(f32)
                        * gates[g, k, at + e, :, q * lane_width : (q + 1) * lane_width].astype(f32)
                        for e in range(2)
                    ]
                    rows = pl.ds(pl.multiple_of(g * block + at * chans, 2 * chans), 2 * chans)
                    gated[rows, q * lane_width : (q + 1) * lane_width] = jnp.concatenate(both, axis=0).astype(bf16)
            return carry

        lax.fori_loop(0, groups, combine, 0, unroll=2)
        left = gated[...]
        for n in range(features // cols):
            at = slice(n * cols, (n + 1) * cols)
            prod = lax.dot_general(
                left, stacked[k, :, at], (((0,), (0,)), ((), ())), preferred_element_type=f32
            )
            if k == 0:
                total[:, at] = prod
            elif k < chunks - 1:
                total[:, at] += prod
            else:
                result[n] = (total[:, at] + prod).astype(bf16)
                copy = pltpu.make_async_copy(result.at[n], output.at[:, pl.ds(n * cols, cols)], result_sem.at[n])
                copy.start()
                outs.append(copy)

    for k in range(chunks):
        for d in range(1, segs):
            send_in(k, d).wait_send()
        pltpu.make_async_remote_copy(
            src_ref=conv_out.at[k, pl.ds(0, outer - quads)], dst_ref=conv_out.at[k, pl.ds(0, outer - quads)],
            send_sem=out_send.at[k], recv_sem=out_recv.at[k],
            device_id=(seg_peer(1), h), device_id_type=MESH,
        ).wait_send()
    for copy in outs:
        copy.wait()


def far_first(segs):
    return [d for d in range(segs - 1, 0, -1)] + [0]


def whole_layer(gate_in, key_in, value_in, kernel, skip_gain, out_weight, chans):
    segs, groups = lax.axis_size("seg"), lax.axis_size("ch")
    channels, tokens = key_in.shape
    full_len = kernel.shape[1]
    outer = full_len // lane_width
    slabs = tokens // lane_width
    features = out_weight.shape[1]
    chunks = channels // segs // chans
    share = tokens // groups
    quads = share // lane_width
    tables = make_tables(outer)
    split = (chunks, segs, chans)
    cols = 512 if features % 512 == 0 else features
    args = (
        *tables,
        skip_gain,
        key_in.reshape(*split, tokens),
        value_in.reshape(*split, tokens),
        gate_in.reshape(*split, tokens),
        kernel.reshape(*split, full_len),
        out_weight.reshape(*split, features),
    )
    vmem = pl.BlockSpec(memory_space=pltpu.VMEM)
    hbm = pl.BlockSpec(memory_space=pl.ANY)
    dma = pltpu.SemaphoreType.DMA
    return pl.pallas_call(
        layer_kernel,
        in_specs=[vmem] * 6 + [pl.BlockSpec(memory_space=pltpu.SMEM)] + [hbm] * 5,
        out_specs=hbm,
        out_shape=jax.ShapeDtypeStruct((share, features), bf16),
        scratch_shapes=[
            pltpu.VMEM((*split, tokens), bf16),
            pltpu.VMEM((*split, tokens), bf16),
            pltpu.VMEM((chunks, chans, full_len), f32),
            pltpu.VMEM((chans * (outer + 8), lane_width), f32),
            pltpu.VMEM((chans * (slabs + 8), lane_width), f32),
            pltpu.VMEM((chans * (outer + 8), lane_width), f32),
            pltpu.VMEM((chunks, chans, outer, 2 * lane_width), bf16),
            pltpu.VMEM((chunks, segs, chans, slabs, lane_width), bf16),
            pltpu.VMEM((chunks, segs, chans, slabs, lane_width), bf16),
            pltpu.VMEM((chunks, outer, chans, lane_width), bf16),
            pltpu.VMEM((chunks, groups, segs, quads, chans, lane_width), bf16),
            pltpu.VMEM((groups, *split, share), bf16),
            pltpu.VMEM((groups, *split, features), bf16),
            pltpu.VMEM((chunks, groups * segs * chans, features), bf16),
            pltpu.VMEM((groups * segs * chans, share), bf16),
            pltpu.VMEM((share, features), f32),
            pltpu.VMEM((features // cols, share, cols), bf16),
            dma((2, chunks)), dma, dma((2,)), dma((features // cols,)), pltpu.SemaphoreType.REGULAR,
            dma((chunks, segs)), dma((chunks, segs)), dma((chunks,)), dma((chunks,)),
            dma((groups,)), dma((groups,)), dma((groups,)), dma((groups,)),
        ],
        compiler_params=pltpu.CompilerParams(
            collective_id=0, has_side_effects=True, vmem_limit_bytes=56 * 1024 * 1024
        ),
        name="layer",
    )(*args)


def on_device(gate_in, key_in, value_in, kernel, skip_gain, out_weight):
    seg_count = lax.axis_size("seg")
    seg_index = lax.axis_index("seg")
    channels, tokens = key_in.shape
    full_len = kernel.shape[1]
    outer = full_len // lane_width
    tables = make_tables(outer)
    col_count = channels // seg_count
    sublanes = 8
    if col_count % sublanes == 0 and tokens // lax.axis_size("ch") % lane_width == 0:
        return whole_layer(gate_in, key_in, value_in, kernel, skip_gain, out_weight, sublanes)
    mixed = key_in.astype(f32) * value_in.astype(f32)
    mixed_sent = mixed.astype(bf16).reshape(channels, tokens // lane_width, lane_width)
    col_mixed = lax.all_to_all(mixed_sent, "seg", split_axis=0, concat_axis=1, tiled=True)
    taps = lax.dynamic_slice_in_dim(kernel, seg_index * col_count, col_count, 0)
    spectrum = transform_filter(tables, taps.astype(bf16).reshape(col_count, outer, lane_width))
    col_conv = convolve(tables, col_mixed, spectrum)
    conv = lax.all_to_all(col_conv, "seg", split_axis=1, concat_axis=0, tiled=True)
    conv = conv.reshape(channels, tokens).astype(f32)
    gated = (gate_in.astype(f32) * (conv + skip_gain[:, None] * mixed)).astype(bf16)
    mine = lax.all_to_all(gated, "ch", split_axis=1, concat_axis=0, tiled=True)
    weight = lax.all_gather(out_weight, "ch", axis=0, tiled=True)
    result = lax.dot_general(
        mine, weight, (((0,), (0,)), ((), ())), preferred_element_type=f32
    )
    return result.astype(bf16)


def solution(mesh):
    placed = (P("ch", "seg"), P("ch", "seg"), P("ch", "seg"), P("ch", None), P("ch"), P("ch", None))
    return jax.shard_map(
        on_device, mesh=mesh, in_specs=placed, out_specs=P(("seg", "ch"), None), check_vma=False
    )
```

```python
import functools
import math

import jax
import jax.numpy as jnp
import numpy as np
from jax import lax
from jax.experimental import pallas as pl
from jax.experimental.pallas import tpu as pltpu
from jax.sharding import PartitionSpec as P

lane_width = 128
bf16 = jnp.bfloat16
f32 = jnp.float32


def angles(rows, cols, period):
    theta = (rows[:, None] * cols[None, :] % (4 * period)) * (2.0 * math.pi / (4 * period))
    return np.cos(theta), np.sin(theta)


def make_tables(outer):
    quarter = 4 * np.arange(outer) + 1
    row = np.arange(outer)
    lane = np.arange(lane_width)
    cos_o, sin_o = angles(quarter, row, outer)
    cos_t, sin_t = angles(quarter, lane, outer * lane_width)
    cos_i, sin_i = angles(4 * lane, lane, lane_width)
    first = np.concatenate([cos_o, -sin_o], axis=0)
    last = np.concatenate([cos_o.T, -sin_o.T], axis=1) / (outer * lane_width)
    inner = np.block([[cos_i, -sin_i], [sin_i, cos_i]])
    inner_back = np.block([[cos_i, sin_i], [-sin_i, cos_i]])
    narrow = [jnp.asarray(m.astype(np.float32).astype(bf16)) for m in (first, last, inner, inner_back)]
    return (*narrow, jnp.asarray(cos_t.astype(np.float32)), jnp.asarray(sin_t.astype(np.float32)))


def forward(signal, first, inner, cos_t, sin_t):
    outer = cos_t.shape[0]
    rows = []
    for at in range(0, len(signal), 2):
        pair = signal[at : at + 2]
        wide = jnp.dot(first, jnp.concatenate(pair, axis=1), preferred_element_type=f32)
        for i in range(len(pair)):
            part = wide[:, i * lane_width : (i + 1) * lane_width]
            real, imag = part[:outer], part[outer:]
            rows.append(
                jnp.concatenate(
                    [
                        (real * cos_t + imag * sin_t).astype(bf16),
                        (imag * cos_t - real * sin_t).astype(bf16),
                    ],
                    axis=1,
                )
            )
    return jnp.dot(jnp.concatenate(rows, axis=0), inner, preferred_element_type=f32)


def filter_kernel(first, inner, cos_t, sin_t, taps, spectrum):
    count, outer = taps.shape[0], taps.shape[1]
    signal = [taps[i].astype(bf16) for i in range(count)]
    out = forward(signal, first[...], inner[...], cos_t[...], sin_t[...])
    spectrum[...] = out.astype(bf16).reshape(count, outer, 2 * lane_width)


def convolve_block(tables, signal, filt):
    first, last, inner, inner_back, cos, sin = tables
    outer = cos.shape[0]
    sig = forward(signal, first, inner, cos, sin)
    filt = filt.astype(f32)
    sig_re, sig_im = sig[:, :lane_width], sig[:, lane_width:]
    filt_re, filt_im = filt[:, :lane_width], filt[:, lane_width:]
    prod = jnp.concatenate(
        [
            (filt_re * sig_re - filt_im * sig_im).astype(bf16),
            (filt_re * sig_im + filt_im * sig_re).astype(bf16),
        ],
        axis=1,
    )
    back = jnp.dot(prod, inner_back, preferred_element_type=f32)
    parts = []
    for at in range(0, len(signal), 2):
        cols = []
        for i in range(at, min(at + 2, len(signal))):
            rows = back[i * outer : (i + 1) * outer]
            real, imag = rows[:, :lane_width], rows[:, lane_width:]
            cols.append(
                jnp.concatenate(
                    [
                        (real * cos - imag * sin).astype(bf16),
                        (imag * cos + real * sin).astype(bf16),
                    ],
                    axis=0,
                )
            )
        wide = jnp.dot(last, jnp.concatenate(cols, axis=1), preferred_element_type=f32)
        for i in range(len(cols)):
            parts.append(wide[:, i * lane_width : (i + 1) * lane_width])
    return parts


def conv_kernel(first, last, inner, inner_back, cos_t, sin_t, mixed, spectrum, conv):
    count, outer = mixed.shape[0], mixed.shape[1]
    tables = (first[...], last[...], inner[...], inner_back[...], cos_t[...], sin_t[...])
    filt = spectrum[...].reshape(count * outer, 2 * lane_width)
    parts = convolve_block(tables, [mixed[i] for i in range(count)], filt)
    for i in range(count):
        conv[i] = parts[i].astype(bf16)


def whole(array):
    return pl.BlockSpec(array.shape, lambda i: (0,) * array.ndim)


def block_of(count):
    return max(b for b in range(1, 9) if count % b == 0)


def transform_filter(tables, taps):
    first, last, inner, inner_back, cos_t, sin_t = tables
    count, outer, lanes = taps.shape
    block = block_of(count)
    fixed = (first, inner, cos_t, sin_t)
    return pl.pallas_call(
        filter_kernel,
        grid=(count // block,),
        in_specs=[whole(a) for a in fixed] + [pl.BlockSpec((block, outer, lanes), lambda i: (i, 0, 0))],
        out_specs=pl.BlockSpec((block, outer, 2 * lanes), lambda i: (i, 0, 0)),
        out_shape=jax.ShapeDtypeStruct((count, outer, 2 * lanes), bf16),
        cost_estimate=pl.CostEstimate(
            flops=count * outer * lanes * 1536, bytes_accessed=count * outer * lanes * 8, transcendentals=0
        ),
        name="filter_transform",
    )(*fixed, taps)


def convolve(tables, mixed, spectrum):
    count, outer, lanes = mixed.shape
    block = block_of(count)
    return pl.pallas_call(
        conv_kernel,
        grid=(count // block,),
        in_specs=[whole(a) for a in tables]
        + [
            pl.BlockSpec((block, outer, lanes), lambda i: (i, 0, 0)),
            pl.BlockSpec((block, outer, 2 * lanes), lambda i: (i, 0, 0)),
        ],
        out_specs=pl.BlockSpec((block, outer, lanes), lambda i: (i, 0, 0)),
        out_shape=jax.ShapeDtypeStruct((count, outer, lanes), bf16),
        cost_estimate=pl.CostEstimate(
            flops=count * outer * lanes * 3072, bytes_accessed=count * outer * lanes * 8, transcendentals=0
        ),
        name="convolve",
    )(*tables, mixed, spectrum)


MESH = pl.DeviceIdType.MESH


def layer_kernel(
    first, last, inner, inner_back, cos_t, sin_t, skip, key, value, gate, kernel, weight,
    output,
    keys, values, taps, tall, wide, long, spectrum, mixed_out, mixed_in, conv_out, conv_in,
    gates, weights, stacked, gated, total, result,
    kv_sem, taps_sem, here_sem, result_sem, ready,
    in_send, in_recv, out_send, out_recv, g_send, g_recv, w_send, w_recv,
):
    chunks, segs, chans, tokens = key.shape
    groups = gates.shape[0]
    share = tokens // groups
    quads = share // lane_width
    features = weight.shape[-1]
    outer = cos_t.shape[0]
    slabs = tokens // lane_width
    step = slabs + 8
    long_step = outer + 8
    block = segs * chans
    depth = groups * block
    cols = result.shape[-1]
    direct = [1, 2, 4, 6] if groups == 8 else range(1, groups)
    passed = [2, 4, 6] if groups == 8 else []
    s = lax.axis_index("seg")
    h = lax.axis_index("ch")

    def seg_peer(d):
        return lax.rem(s + d, segs)

    def ch_peer(d):
        return lax.rem(h + d, groups)

    def lanes(j):
        return pl.ds(pl.multiple_of(j * lane_width, lane_width), lane_width)

    barrier = pltpu.get_barrier_semaphore()
    for d in range(1, segs):
        pl.semaphore_signal(barrier, inc=1, device_id=(seg_peer(d), h), device_id_type=MESH)
    for d in range(1, groups):
        pl.semaphore_signal(barrier, inc=1, device_id=(s, ch_peer(d)), device_id_type=MESH)

    def load_kv(k):
        return (
            pltpu.make_async_copy(key.at[k], keys.at[k], kv_sem.at[0, k]),
            pltpu.make_async_copy(value.at[k], values.at[k], kv_sem.at[1, k]),
        )

    for k in range(chunks):
        for copy in load_kv(k):
            copy.start()
    fetch = pltpu.make_async_copy(kernel.at[:, s], taps, taps_sem)
    fetch.start()

    def part_of(peer):
        return pl.ds(pl.multiple_of(peer * share, lane_width), share)

    own_gate = pltpu.make_async_copy(gate.at[:, :, :, part_of(h)], gates.at[h], here_sem.at[0])
    own_weight = pltpu.make_async_copy(weight, weights.at[h], here_sem.at[1])
    own_gate.start()
    own_weight.start()

    def send_in(k, d):
        return pltpu.make_async_remote_copy(
            src_ref=mixed_out.at[k, d], dst_ref=mixed_in.at[k, s],
            send_sem=in_send.at[k, d], recv_sem=in_recv.at[k, d],
            device_id=(seg_peer(d), h), device_id_type=MESH,
        )

    def send_gate(d):
        peer = ch_peer(d)
        return pltpu.make_async_remote_copy(
            src_ref=gate.at[:, :, :, part_of(peer)], dst_ref=gates.at[h],
            send_sem=g_send.at[d], recv_sem=g_recv.at[d],
            device_id=(s, peer), device_id_type=MESH,
        )

    def flipped(at, d):
        for bit in (1, 2, 4):
            if d & bit:
                at = at + bit - 2 * bit * lax.rem(at // bit, 2)
        return at

    def send_weight(d):
        peer = flipped(h, d)
        return pltpu.make_async_remote_copy(
            src_ref=weight, dst_ref=weights.at[h],
            send_sem=w_send.at[d], recv_sem=w_recv.at[d],
            device_id=(s, peer), device_id_type=MESH,
        )

    def pass_weight(d):
        owner = flipped(h, d)
        return pltpu.make_async_remote_copy(
            src_ref=weights.at[owner], dst_ref=weights.at[owner],
            send_sem=w_send.at[d + 1], recv_sem=w_recv.at[d + 1],
            device_id=(s, flipped(h, 1)), device_id_type=MESH,
        )

    def out_rows(seg, peer):
        return pl.ds(seg * slabs + peer * quads, quads)

    for k in range(chunks):
        for copy in load_kv(k):
            copy.wait()
        for d in far_first(segs):
            peer = seg_peer(d)

            def mix(j, carry):
                both = keys[k, peer, :, lanes(j)].astype(f32) * values[k, peer, :, lanes(j)].astype(f32)
                wide[pl.ds(j, chans, stride=step), :] = both
                return carry

            lax.fori_loop(0, slabs, mix, 0, unroll=4)
            into = mixed_out.at[k, d] if d else mixed_in.at[k, s]
            for i in range(chans):
                into[i] = wide[i * step : i * step + slabs, :].astype(bf16)
        if k == 0:
            pl.semaphore_wait(barrier, segs + groups - 2)
        for d in far_first(segs):
            if d:
                send_in(k, d).start()
        if k == 0:
            for d in range(1, groups):
                send_gate(d).start()
            for d in range(1, segs):
                pl.semaphore_signal(ready, inc=1, device_id=(seg_peer(d), h), device_id_type=MESH)
    for d in direct:
        send_weight(d).start()

    fetch.wait()
    for k in range(chunks):

        def spread(j, carry):
            tall[pl.ds(j, chans, stride=long_step), :] = taps[k, :, lanes(j)]
            return carry

        lax.fori_loop(0, outer, spread, 0, unroll=4)
        signal = [tall[i * long_step : i * long_step + outer, :].astype(bf16) for i in range(chans)]
        out = forward(signal, first[...], inner[...], cos_t[...], sin_t[...])
        spectrum[k] = out.astype(bf16).reshape(chans, outer, 2 * lane_width)
    pl.semaphore_wait(ready, segs - 1)

    for k in range(chunks):
        for d in range(1, segs):
            send_in(k, d).wait_recv()
        signal = [mixed_in[k, :, i].reshape(outer, lane_width) for i in range(chans)]
        filt = spectrum[k].reshape(chans * outer, 2 * lane_width)
        tables = (first[...], last[...], inner[...], inner_back[...], cos_t[...], sin_t[...])
        parts = convolve_block(tables, signal, filt)
        for i in range(chans):
            level = skip[(k * segs + s) * chans + i]
            long[i * long_step : i * long_step + outer, :] = parts[i] + level * signal[i].astype(f32)

        def gather(j, carry):
            conv_out[k, j] = long[pl.ds(j, chans, stride=long_step), :].astype(bf16)
            return carry

        lax.fori_loop(0, outer, gather, 0, unroll=8)
        for d in far_first(segs):
            seg = seg_peer(d)

            def send(e, carry):
                peer = ch_peer(e)
                pltpu.make_async_remote_copy(
                    src_ref=conv_out.at[k, out_rows(seg, peer)], dst_ref=conv_in.at[k, h, s],
                    send_sem=out_send.at[k], recv_sem=out_recv.at[k],
                    device_id=(seg, peer), device_id_type=MESH,
                ).start()
                return carry

            lax.fori_loop(0 if d else 1, groups, send, 0)
        for q in range(quads):
            conv_in[k, h, s, q] = conv_out[k, s * slabs + h * quads + q]

    own_gate.wait()
    own_weight.wait()
    for d in passed:
        send_weight(d).wait_recv()
        pass_weight(d).start()
    for d in range(1, groups):
        send_gate(d).wait()
    for d in direct:
        if d in passed:
            send_weight(d).wait_send()
        else:
            send_weight(d).wait()
    for d in passed:
        pass_weight(d).wait()
    for k in range(chunks):

        def restack(g, carry):
            for at in range(0, segs, 2):
                pair = [weights[g, k, at + e].astype(f32) for e in range(2)]
                rows = pl.ds(pl.multiple_of(g * block + at * chans, 2 * chans), 2 * chans)
                stacked[k, rows, :] = jnp.concatenate(pair, axis=0).astype(bf16)
            return carry

        lax.fori_loop(0, groups, restack, 0)

    outs = []
    for k in range(chunks):
        pieces = pltpu.make_async_remote_copy(
            src_ref=conv_out.at[k, pl.ds(0, outer - quads)], dst_ref=conv_out.at[k, pl.ds(0, outer - quads)],
            send_sem=out_send.at[k], recv_sem=out_recv.at[k],
            device_id=(seg_peer(1), h), device_id_type=MESH,
        )
        pieces.wait_recv()

        def combine(g, carry):
            for at in range(0, segs, 2):
                for q in range(quads):
                    both = [
                        conv_in[k, g, at + e, q].astype(f32)
                        * gates[g, k, at + e, :, q * lane_width : (q + 1) * lane_width].astype(f32)
                        for e in range(2)
                    ]
                    rows = pl.ds(pl.multiple_of(g * block + at * chans, 2 * chans), 2 * chans)
                    gated[rows, q * lane_width : (q + 1) * lane_width] = jnp.concatenate(both, axis=0).astype(bf16)
            return carry

        lax.fori_loop(0, groups, combine, 0, unroll=2)
        left = gated[...]
        for n in range(features // cols):
            at = slice(n * cols, (n + 1) * cols)
            prod = lax.dot_general(
                left, stacked[k, :, at], (((0,), (0,)), ((), ())), preferred_element_type=f32
            )
            if k == 0:
                total[:, at] = prod
            elif k < chunks - 1:
                total[:, at] += prod
            else:
                result[n] = (total[:, at] + prod).astype(bf16)
                copy = pltpu.make_async_copy(result.at[n], output.at[:, pl.ds(n * cols, cols)], result_sem.at[n])
                copy.start()
                outs.append(copy)

    for k in range(chunks):
        for d in range(1, segs):
            send_in(k, d).wait_send()
        pltpu.make_async_remote_copy(
            src_ref=conv_out.at[k, pl.ds(0, outer - quads)], dst_ref=conv_out.at[k, pl.ds(0, outer - quads)],
            send_sem=out_send.at[k], recv_sem=out_recv.at[k],
            device_id=(seg_peer(1), h), device_id_type=MESH,
        ).wait_send()
    for copy in outs:
        copy.wait()


def far_first(segs):
    return [d for d in range(segs - 1, 0, -1)] + [0]


def whole_layer(gate_in, key_in, value_in, kernel, skip_gain, out_weight, chans):
    segs, groups = lax.axis_size("seg"), lax.axis_size("ch")
    channels, tokens = key_in.shape
    full_len = kernel.shape[1]
    outer = full_len // lane_width
    slabs = tokens // lane_width
    features = out_weight.shape[1]
    chunks = channels // segs // chans
    share = tokens // groups
    quads = share // lane_width
    tables = make_tables(outer)
    split = (chunks, segs, chans)
    cols = 512 if features % 512 == 0 else features
    args = (
        *tables,
        skip_gain,
        key_in.reshape(*split, tokens),
        value_in.reshape(*split, tokens),
        gate_in.reshape(*split, tokens),
        kernel.reshape(*split, full_len),
        out_weight.reshape(*split, features),
    )
    vmem = pl.BlockSpec(memory_space=pltpu.VMEM)
    hbm = pl.BlockSpec(memory_space=pl.ANY)
    dma = pltpu.SemaphoreType.DMA
    return pl.pallas_call(
        layer_kernel,
        in_specs=[vmem] * 6 + [pl.BlockSpec(memory_space=pltpu.SMEM)] + [hbm] * 5,
        out_specs=hbm,
        out_shape=jax.ShapeDtypeStruct((share, features), bf16),
        scratch_shapes=[
            pltpu.VMEM((*split, tokens), bf16),
            pltpu.VMEM((*split, tokens), bf16),
            pltpu.VMEM((chunks, chans, full_len), f32),
            pltpu.VMEM((chans * (outer + 8), lane_width), f32),
            pltpu.VMEM((chans * (slabs + 8), lane_width), f32),
            pltpu.VMEM((chans * (outer + 8), lane_width), f32),
            pltpu.VMEM((chunks, chans, outer, 2 * lane_width), bf16),
            pltpu.VMEM((chunks, segs, chans, slabs, lane_width), bf16),
            pltpu.VMEM((chunks, segs, chans, slabs, lane_width), bf16),
            pltpu.VMEM((chunks, outer, chans, lane_width), bf16),
            pltpu.VMEM((chunks, groups, segs, quads, chans, lane_width), bf16),
            pltpu.VMEM((groups, *split, share), bf16),
            pltpu.VMEM((groups, *split, features), bf16),
            pltpu.VMEM((chunks, groups * segs * chans, features), bf16),
            pltpu.VMEM((groups * segs * chans, share), bf16),
            pltpu.VMEM((share, features), f32),
            pltpu.VMEM((features // cols, share, cols), bf16),
            dma((2, chunks)), dma, dma((2,)), dma((features // cols,)), pltpu.SemaphoreType.REGULAR,
            dma((chunks, segs)), dma((chunks, segs)), dma((chunks,)), dma((chunks,)),
            dma((groups,)), dma((groups,)), dma((groups,)), dma((groups,)),
        ],
        compiler_params=pltpu.CompilerParams(
            collective_id=0, has_side_effects=True, vmem_limit_bytes=56 * 1024 * 1024
        ),
        name="layer",
    )(*args)


def on_device(gate_in, key_in, value_in, kernel, skip_gain, out_weight):
    seg_count = lax.axis_size("seg")
    seg_index = lax.axis_index("seg")
    channels, tokens = key_in.shape
    full_len = kernel.shape[1]
    outer = full_len // lane_width
    tables = make_tables(outer)
    col_count = channels // seg_count
    sublanes = 8
    if col_count % sublanes == 0 and tokens // lax.axis_size("ch") % lane_width == 0:
        return whole_layer(gate_in, key_in, value_in, kernel, skip_gain, out_weight, sublanes)
    mixed = key_in.astype(f32) * value_in.astype(f32)
    mixed_sent = mixed.astype(bf16).reshape(channels, tokens // lane_width, lane_width)
    col_mixed = lax.all_to_all(mixed_sent, "seg", split_axis=0, concat_axis=1, tiled=True)
    taps = lax.dynamic_slice_in_dim(kernel, seg_index * col_count, col_count, 0)
    spectrum = transform_filter(tables, taps.astype(bf16).reshape(col_count, outer, lane_width))
    col_conv = convolve(tables, col_mixed, spectrum)
    conv = lax.all_to_all(col_conv, "seg", split_axis=1, concat_axis=0, tiled=True)
    conv = conv.reshape(channels, tokens).astype(f32)
    gated = (gate_in.astype(f32) * (conv + skip_gain[:, None] * mixed)).astype(bf16)
    mine = lax.all_to_all(gated, "ch", split_axis=1, concat_axis=0, tiled=True)
    weight = lax.all_gather(out_weight, "ch", axis=0, tiled=True)
    result = lax.dot_general(
        mine, weight, (((0,), (0,)), ((), ())), preferred_element_type=f32
    )
    return result.astype(bf16)


def solution(mesh):
    placed = (P("ch", "seg"), P("ch", "seg"), P("ch", "seg"), P("ch", None), P("ch"), P("ch", None))
    return jax.shard_map(
        on_device, mesh=mesh, in_specs=placed, out_specs=P(("seg", "ch"), None), check_vma=False
    )
```

```python
import functools
import math

import jax
import jax.numpy as jnp
import numpy as np
from jax import lax
from jax.experimental import pallas as pl
from jax.experimental.pallas import tpu as pltpu
from jax.sharding import PartitionSpec as P

lane_width = 128
bf16 = jnp.bfloat16
f32 = jnp.float32


def angles(rows, cols, period):
    theta = (rows[:, None] * cols[None, :] % (4 * period)) * (2.0 * math.pi / (4 * period))
    return np.cos(theta), np.sin(theta)


def make_tables(outer):
    quarter = 4 * np.arange(outer) + 1
    row = np.arange(outer)
    lane = np.arange(lane_width)
    cos_o, sin_o = angles(quarter, row, outer)
    cos_t, sin_t = angles(quarter, lane, outer * lane_width)
    cos_i, sin_i = angles(4 * lane, lane, lane_width)
    first = np.concatenate([cos_o, -sin_o], axis=0)
    last = np.concatenate([cos_o.T, -sin_o.T], axis=1) / (outer * lane_width)
    inner = np.block([[cos_i, -sin_i], [sin_i, cos_i]])
    inner_back = np.block([[cos_i, sin_i], [-sin_i, cos_i]])
    narrow = [jnp.asarray(m.astype(np.float32).astype(bf16)) for m in (first, last, inner, inner_back)]
    return (*narrow, jnp.asarray(cos_t.astype(np.float32)), jnp.asarray(sin_t.astype(np.float32)))


def forward(signal, first, inner, cos_t, sin_t):
    outer = cos_t.shape[0]
    rows = []
    for at in range(0, len(signal), 2):
        pair = signal[at : at + 2]
        wide = jnp.dot(first, jnp.concatenate(pair, axis=1), preferred_element_type=f32)
        for i in range(len(pair)):
            part = wide[:, i * lane_width : (i + 1) * lane_width]
            real, imag = part[:outer], part[outer:]
            rows.append(
                jnp.concatenate(
                    [
                        (real * cos_t + imag * sin_t).astype(bf16),
                        (imag * cos_t - real * sin_t).astype(bf16),
                    ],
                    axis=1,
                )
            )
    return jnp.dot(jnp.concatenate(rows, axis=0), inner, preferred_element_type=f32)


def filter_kernel(first, inner, cos_t, sin_t, taps, spectrum):
    count, outer = taps.shape[0], taps.shape[1]
    signal = [taps[i].astype(bf16) for i in range(count)]
    out = forward(signal, first[...], inner[...], cos_t[...], sin_t[...])
    spectrum[...] = out.astype(bf16).reshape(count, outer, 2 * lane_width)


def convolve_block(tables, signal, filt):
    first, last, inner, inner_back, cos, sin = tables
    outer = cos.shape[0]
    sig = forward(signal, first, inner, cos, sin)
    filt = filt.astype(f32)
    sig_re, sig_im = sig[:, :lane_width], sig[:, lane_width:]
    filt_re, filt_im = filt[:, :lane_width], filt[:, lane_width:]
    prod = jnp.concatenate(
        [
            (filt_re * sig_re - filt_im * sig_im).astype(bf16),
            (filt_re * sig_im + filt_im * sig_re).astype(bf16),
        ],
        axis=1,
    )
    back = jnp.dot(prod, inner_back, preferred_element_type=f32)
    parts = []
    for at in range(0, len(signal), 2):
        cols = []
        for i in range(at, min(at + 2, len(signal))):
            rows = back[i * outer : (i + 1) * outer]
            real, imag = rows[:, :lane_width], rows[:, lane_width:]
            cols.append(
                jnp.concatenate(
                    [
                        (real * cos - imag * sin).astype(bf16),
                        (imag * cos + real * sin).astype(bf16),
                    ],
                    axis=0,
                )
            )
        wide = jnp.dot(last, jnp.concatenate(cols, axis=1), preferred_element_type=f32)
        for i in range(len(cols)):
            parts.append(wide[:, i * lane_width : (i + 1) * lane_width])
    return parts


def conv_kernel(first, last, inner, inner_back, cos_t, sin_t, mixed, spectrum, conv):
    count, outer = mixed.shape[0], mixed.shape[1]
    tables = (first[...], last[...], inner[...], inner_back[...], cos_t[...], sin_t[...])
    filt = spectrum[...].reshape(count * outer, 2 * lane_width)
    parts = convolve_block(tables, [mixed[i] for i in range(count)], filt)
    for i in range(count):
        conv[i] = parts[i].astype(bf16)


def whole(array):
    return pl.BlockSpec(array.shape, lambda i: (0,) * array.ndim)


def block_of(count):
    return max(b for b in range(1, 9) if count % b == 0)


def transform_filter(tables, taps):
    first, last, inner, inner_back, cos_t, sin_t = tables
    count, outer, lanes = taps.shape
    block = block_of(count)
    fixed = (first, inner, cos_t, sin_t)
    return pl.pallas_call(
        filter_kernel,
        grid=(count // block,),
        in_specs=[whole(a) for a in fixed] + [pl.BlockSpec((block, outer, lanes), lambda i: (i, 0, 0))],
        out_specs=pl.BlockSpec((block, outer, 2 * lanes), lambda i: (i, 0, 0)),
        out_shape=jax.ShapeDtypeStruct((count, outer, 2 * lanes), bf16),
        cost_estimate=pl.CostEstimate(
            flops=count * outer * lanes * 1536, bytes_accessed=count * outer * lanes * 8, transcendentals=0
        ),
        name="filter_transform",
    )(*fixed, taps)


def convolve(tables, mixed, spectrum):
    count, outer, lanes = mixed.shape
    block = block_of(count)
    return pl.pallas_call(
        conv_kernel,
        grid=(count // block,),
        in_specs=[whole(a) for a in tables]
        + [
            pl.BlockSpec((block, outer, lanes), lambda i: (i, 0, 0)),
            pl.BlockSpec((block, outer, 2 * lanes), lambda i: (i, 0, 0)),
        ],
        out_specs=pl.BlockSpec((block, outer, lanes), lambda i: (i, 0, 0)),
        out_shape=jax.ShapeDtypeStruct((count, outer, lanes), bf16),
        cost_estimate=pl.CostEstimate(
            flops=count * outer * lanes * 3072, bytes_accessed=count * outer * lanes * 8, transcendentals=0
        ),
        name="convolve",
    )(*tables, mixed, spectrum)


MESH = pl.DeviceIdType.MESH


def layer_kernel(
    first_in, last_in, inner_in, inner_back_in, cos_in, sin_in, skip_in, key, value, gate, kernel, weight,
    output,
    first, last, inner, inner_back, cos_t, sin_t, skip, table_sem, keys, values, taps, tall, wide, long, spectrum, mixed_out, mixed_in, conv_out, conv_in,
    gates, weights, stacked, gated, total,
    kv_sem, taps_sem, here_sem, ready,
    in_send, in_recv, out_send, out_recv, g_send, g_recv, w_send, w_recv,
):
    chunks, segs, chans, tokens = key.shape
    groups = gates.shape[0]
    share = tokens // groups
    quads = share // lane_width
    features = weight.shape[-1]
    outer = cos_t.shape[0]
    slabs = tokens // lane_width
    step = slabs + 8
    long_step = outer + 8
    block = segs * chans
    depth = groups * block
    cols = 512 if features % 512 == 0 else features
    direct = [1, 2, 4, 6] if groups == 8 else range(1, groups)
    passed = [2, 4, 6] if groups == 8 else []
    s = lax.axis_index("seg")
    h = lax.axis_index("ch")

    def seg_peer(d):
        return lax.rem(s + d, segs)

    def ch_peer(d):
        return lax.rem(h + d, groups)

    def lanes(j):
        return pl.ds(pl.multiple_of(j * lane_width, lane_width), lane_width)

    barrier = pltpu.get_barrier_semaphore()
    for d in range(1, segs):
        pl.semaphore_signal(barrier, inc=1, device_id=(seg_peer(d), h), device_id_type=MESH)
    for d in range(1, groups):
        pl.semaphore_signal(barrier, inc=1, device_id=(s, ch_peer(d)), device_id_type=MESH)

    def load_kv(k):
        return (
            pltpu.make_async_copy(key.at[k], keys.at[k], kv_sem.at[0, k]),
            pltpu.make_async_copy(value.at[k], values.at[k], kv_sem.at[1, k]),
        )

    for k in range(chunks):
        for copy in load_kv(k):
            copy.start()
    fetch = pltpu.make_async_copy(kernel.at[:, s], taps, taps_sem)
    fetch.start()
    whole_in = (first_in, last_in, inner_in, inner_back_in, cos_in, sin_in, skip_in)
    whole_here = (first, last, inner, inner_back, cos_t, sin_t, skip)
    loads = [pltpu.make_async_copy(a, b, table_sem.at[i]) for i, (a, b) in enumerate(zip(whole_in, whole_here))]
    for copy in loads:
        copy.start()

    def part_of(peer):
        return pl.ds(pl.multiple_of(peer * share, lane_width), share)

    own_gate = pltpu.make_async_copy(gate.at[:, :, :, part_of(h)], gates.at[h], here_sem.at[0])
    own_weight = pltpu.make_async_copy(weight, weights.at[h], here_sem.at[1])
    own_gate.start()
    own_weight.start()

    def send_in(k, d):
        return pltpu.make_async_remote_copy(
            src_ref=mixed_out.at[k, d], dst_ref=mixed_in.at[k, s],
            send_sem=in_send.at[k, d], recv_sem=in_recv.at[k, d],
            device_id=(seg_peer(d), h), device_id_type=MESH,
        )

    def send_gate(d):
        peer = ch_peer(d)
        return pltpu.make_async_remote_copy(
            src_ref=gate.at[:, :, :, part_of(peer)], dst_ref=gates.at[h],
            send_sem=g_send.at[d], recv_sem=g_recv.at[d],
            device_id=(s, peer), device_id_type=MESH,
        )

    def flipped(at, d):
        for bit in (1, 2, 4):
            if d & bit:
                at = at + bit - 2 * bit * lax.rem(at // bit, 2)
        return at

    def send_weight(d):
        peer = flipped(h, d)
        return pltpu.make_async_remote_copy(
            src_ref=weight, dst_ref=weights.at[h],
            send_sem=w_send.at[d], recv_sem=w_recv.at[d],
            device_id=(s, peer), device_id_type=MESH,
        )

    def pass_weight(d):
        owner = flipped(h, d)
        return pltpu.make_async_remote_copy(
            src_ref=weights.at[owner], dst_ref=weights.at[owner],
            send_sem=w_send.at[d + 1], recv_sem=w_recv.at[d + 1],
            device_id=(s, flipped(h, 1)), device_id_type=MESH,
        )

    def out_rows(seg, peer):
        return pl.ds(seg * slabs + peer * quads, quads)

    for k in range(chunks):
        for copy in load_kv(k):
            copy.wait()
        for d in far_first(segs):
            peer = seg_peer(d)

            def mix(j, carry):
                both = keys[k, peer, :, lanes(j)].astype(f32) * values[k, peer, :, lanes(j)].astype(f32)
                wide[pl.ds(j, chans, stride=step), :] = both
                return carry

            lax.fori_loop(0, slabs, mix, 0, unroll=4)
            into = mixed_out.at[k, d] if d else mixed_in.at[k, s]
            for i in range(chans):
                into[i] = wide[i * step : i * step + slabs, :].astype(bf16)
        if k == 0:
            pl.semaphore_wait(barrier, segs + groups - 2)
        for d in far_first(segs):
            if d:
                send_in(k, d).start()
        if k == 0:
            for d in range(1, groups):
                send_gate(d).start()
            for d in range(1, segs):
                pl.semaphore_signal(ready, inc=1, device_id=(seg_peer(d), h), device_id_type=MESH)
    for d in direct:
        send_weight(d).start()

    fetch.wait()
    for copy in loads:
        copy.wait()
    for k in range(chunks):

        def spread(j, carry):
            tall[pl.ds(j, chans, stride=long_step), :] = taps[k, :, lanes(j)]
            return carry

        lax.fori_loop(0, outer, spread, 0, unroll=4)
        signal = [tall[i * long_step : i * long_step + outer, :].astype(bf16) for i in range(chans)]
        out = forward(signal, first[...], inner[...], cos_t[...], sin_t[...])
        spectrum[k] = out.astype(bf16).reshape(chans, outer, 2 * lane_width)
    pl.semaphore_wait(ready, segs - 1)

    for k in range(chunks):
        for d in range(1, segs):
            send_in(k, d).wait_recv()
        signal = [mixed_in[k, :, i].reshape(outer, lane_width) for i in range(chans)]
        filt = spectrum[k].reshape(chans * outer, 2 * lane_width)
        tables = (first[...], last[...], inner[...], inner_back[...], cos_t[...], sin_t[...])
        parts = convolve_block(tables, signal, filt)
        for i in range(chans):
            level = skip[(k * segs + s) * chans + i]
            long[i * long_step : i * long_step + outer, :] = parts[i] + level * signal[i].astype(f32)

        def gather(j, carry):
            conv_out[k, j] = long[pl.ds(j, chans, stride=long_step), :].astype(bf16)
            return carry

        lax.fori_loop(0, outer, gather, 0, unroll=8)
        for d in far_first(segs):
            seg = seg_peer(d)

            def send(e, carry):
                peer = ch_peer(e)
                pltpu.make_async_remote_copy(
                    src_ref=conv_out.at[k, out_rows(seg, peer)], dst_ref=conv_in.at[k, h, s],
                    send_sem=out_send.at[k], recv_sem=out_recv.at[k],
                    device_id=(seg, peer), device_id_type=MESH,
                ).start()
                return carry

            lax.fori_loop(0 if d else 1, groups, send, 0)
        for q in range(quads):
            conv_in[k, h, s, q] = conv_out[k, s * slabs + h * quads + q]

    own_gate.wait()
    own_weight.wait()
    for d in passed:
        send_weight(d).wait_recv()
        pass_weight(d).start()
    for d in range(1, groups):
        send_gate(d).wait()
    for d in direct:
        if d in passed:
            send_weight(d).wait_send()
        else:
            send_weight(d).wait()
    for d in passed:
        pass_weight(d).wait()
    for k in range(chunks):

        def restack(g, carry):
            for at in range(0, segs, 2):
                pair = [weights[g, k, at + e].astype(f32) for e in range(2)]
                rows = pl.ds(pl.multiple_of(g * block + at * chans, 2 * chans), 2 * chans)
                stacked[k, rows, :] = jnp.concatenate(pair, axis=0).astype(bf16)
            return carry

        lax.fori_loop(0, groups, restack, 0)

    for k in range(chunks):
        pieces = pltpu.make_async_remote_copy(
            src_ref=conv_out.at[k, pl.ds(0, outer - quads)], dst_ref=conv_out.at[k, pl.ds(0, outer - quads)],
            send_sem=out_send.at[k], recv_sem=out_recv.at[k],
            device_id=(seg_peer(1), h), device_id_type=MESH,
        )
        pieces.wait_recv()

        def combine(g, carry):
            for at in range(0, segs, 2):
                for q in range(quads):
                    both = [
                        conv_in[k, g, at + e, q].astype(f32)
                        * gates[g, k, at + e, :, q * lane_width : (q + 1) * lane_width].astype(f32)
                        for e in range(2)
                    ]
                    rows = pl.ds(pl.multiple_of(g * block + at * chans, 2 * chans), 2 * chans)
                    gated[rows, q * lane_width : (q + 1) * lane_width] = jnp.concatenate(both, axis=0).astype(bf16)
            return carry

        lax.fori_loop(0, groups, combine, 0, unroll=2)
        left = gated[...]
        for n in range(features // cols):
            at = slice(n * cols, (n + 1) * cols)
            prod = lax.dot_general(
                left, stacked[k, :, at], (((0,), (0,)), ((), ())), preferred_element_type=f32
            )
            if k == 0:
                total[:, at] = prod
            elif k < chunks - 1:
                total[:, at] += prod
            else:
                output[:, at] = (total[:, at] + prod).astype(bf16)

    for k in range(chunks):
        for d in range(1, segs):
            send_in(k, d).wait_send()
        pltpu.make_async_remote_copy(
            src_ref=conv_out.at[k, pl.ds(0, outer - quads)], dst_ref=conv_out.at[k, pl.ds(0, outer - quads)],
            send_sem=out_send.at[k], recv_sem=out_recv.at[k],
            device_id=(seg_peer(1), h), device_id_type=MESH,
        ).wait_send()


def far_first(segs):
    return [d for d in range(segs - 1, 0, -1)] + [0]


def whole_layer(gate_in, key_in, value_in, kernel, skip_gain, out_weight, chans):
    segs, groups = lax.axis_size("seg"), lax.axis_size("ch")
    channels, tokens = key_in.shape
    full_len = kernel.shape[1]
    outer = full_len // lane_width
    slabs = tokens // lane_width
    features = out_weight.shape[1]
    chunks = channels // segs // chans
    share = tokens // groups
    quads = share // lane_width
    tables = make_tables(outer)
    split = (chunks, segs, chans)
    args = (
        *tables,
        skip_gain,
        key_in.reshape(*split, tokens),
        value_in.reshape(*split, tokens),
        gate_in.reshape(*split, tokens),
        kernel.reshape(*split, full_len),
        out_weight.reshape(*split, features),
    )
    vmem = pl.BlockSpec(memory_space=pltpu.VMEM)
    hbm = pl.BlockSpec(memory_space=pltpu.HBM)
    dma = pltpu.SemaphoreType.DMA
    return pl.pallas_call(
        layer_kernel,
        in_specs=[hbm] * len(args),
        out_specs=vmem,
        out_shape=pltpu.VMEM((share, features), bf16),
        scratch_shapes=[pltpu.VMEM(a.shape, a.dtype) for a in tables] + [
            pltpu.SMEM(skip_gain.shape, f32), dma((len(tables) + 1,)),
            pltpu.VMEM((*split, tokens), bf16),
            pltpu.VMEM((*split, tokens), bf16),
            pltpu.VMEM((chunks, chans, full_len), f32),
            pltpu.VMEM((chans * (outer + 8), lane_width), f32),
            pltpu.VMEM((chans * (slabs + 8), lane_width), f32),
            pltpu.VMEM((chans * (outer + 8), lane_width), f32),
            pltpu.VMEM((chunks, chans, outer, 2 * lane_width), bf16),
            pltpu.VMEM((chunks, segs, chans, slabs, lane_width), bf16),
            pltpu.VMEM((chunks, segs, chans, slabs, lane_width), bf16),
            pltpu.VMEM((chunks, outer, chans, lane_width), bf16),
            pltpu.VMEM((chunks, groups, segs, quads, chans, lane_width), bf16),
            pltpu.VMEM((groups, *split, share), bf16),
            pltpu.VMEM((groups, *split, features), bf16),
            pltpu.VMEM((chunks, groups * segs * chans, features), bf16),
            pltpu.VMEM((groups * segs * chans, share), bf16),
            pltpu.VMEM((share, features), f32),
            dma((2, chunks)), dma, dma((2,)), pltpu.SemaphoreType.REGULAR,
            dma((chunks, segs)), dma((chunks, segs)), dma((chunks,)), dma((chunks,)),
            dma((groups,)), dma((groups,)), dma((groups,)), dma((groups,)),
        ],
        compiler_params=pltpu.CompilerParams(
            collective_id=0, has_side_effects=True, vmem_limit_bytes=56 * 1024 * 1024
        ),
        name="layer",
    )(*args)


def on_device(gate_in, key_in, value_in, kernel, skip_gain, out_weight):
    seg_count = lax.axis_size("seg")
    seg_index = lax.axis_index("seg")
    channels, tokens = key_in.shape
    full_len = kernel.shape[1]
    outer = full_len // lane_width
    tables = make_tables(outer)
    col_count = channels // seg_count
    sublanes = 8
    if col_count % sublanes == 0 and tokens // lax.axis_size("ch") % lane_width == 0:
        return whole_layer(gate_in, key_in, value_in, kernel, skip_gain, out_weight, sublanes)
    mixed = key_in.astype(f32) * value_in.astype(f32)
    mixed_sent = mixed.astype(bf16).reshape(channels, tokens // lane_width, lane_width)
    col_mixed = lax.all_to_all(mixed_sent, "seg", split_axis=0, concat_axis=1, tiled=True)
    taps = lax.dynamic_slice_in_dim(kernel, seg_index * col_count, col_count, 0)
    spectrum = transform_filter(tables, taps.astype(bf16).reshape(col_count, outer, lane_width))
    col_conv = convolve(tables, col_mixed, spectrum)
    conv = lax.all_to_all(col_conv, "seg", split_axis=1, concat_axis=0, tiled=True)
    conv = conv.reshape(channels, tokens).astype(f32)
    gated = (gate_in.astype(f32) * (conv + skip_gain[:, None] * mixed)).astype(bf16)
    mine = lax.all_to_all(gated, "ch", split_axis=1, concat_axis=0, tiled=True)
    weight = lax.all_gather(out_weight, "ch", axis=0, tiled=True)
    result = lax.dot_general(
        mine, weight, (((0,), (0,)), ((), ())), preferred_element_type=f32
    )
    return result.astype(bf16)


def solution(mesh):
    placed = (P("ch", "seg"), P("ch", "seg"), P("ch", "seg"), P("ch", None), P("ch"), P("ch", None))
    return jax.shard_map(
        on_device, mesh=mesh, in_specs=placed, out_specs=P(("seg", "ch"), None), check_vma=False
    )
```

```python
import functools
import math

import jax
import jax.numpy as jnp
import numpy as np
from jax import lax
from jax.experimental import pallas as pl
from jax.experimental.pallas import tpu as pltpu
from jax.sharding import PartitionSpec as P

lane_width = 128
bf16 = jnp.bfloat16
f32 = jnp.float32


def angles(rows, cols, period):
    theta = (rows[:, None] * cols[None, :] % (4 * period)) * (2.0 * math.pi / (4 * period))
    return np.cos(theta), np.sin(theta)


def make_tables(outer):
    quarter = 4 * np.arange(outer) + 1
    row = np.arange(outer)
    lane = np.arange(lane_width)
    cos_o, sin_o = angles(quarter, row, outer)
    cos_t, sin_t = angles(quarter, lane, outer * lane_width)
    cos_i, sin_i = angles(4 * lane, lane, lane_width)
    first = np.concatenate([cos_o, -sin_o], axis=0)
    last = np.concatenate([cos_o.T, -sin_o.T], axis=1) / (outer * lane_width)
    inner = np.block([[cos_i, -sin_i], [sin_i, cos_i]])
    inner_back = np.block([[cos_i, sin_i], [-sin_i, cos_i]])
    narrow = [jnp.asarray(m.astype(np.float32).astype(bf16)) for m in (first, last, inner, inner_back)]
    return (*narrow, jnp.asarray(cos_t.astype(np.float32)), jnp.asarray(sin_t.astype(np.float32)))


def forward(signal, first, inner, cos_t, sin_t):
    outer = cos_t.shape[0]
    rows = []
    for at in range(0, len(signal), 2):
        pair = signal[at : at + 2]
        wide = jnp.dot(first, jnp.concatenate(pair, axis=1), preferred_element_type=f32)
        for i in range(len(pair)):
            part = wide[:, i * lane_width : (i + 1) * lane_width]
            real, imag = part[:outer], part[outer:]
            rows.append(
                jnp.concatenate(
                    [
                        (real * cos_t + imag * sin_t).astype(bf16),
                        (imag * cos_t - real * sin_t).astype(bf16),
                    ],
                    axis=1,
                )
            )
    return jnp.dot(jnp.concatenate(rows, axis=0), inner, preferred_element_type=f32)


def filter_kernel(first, inner, cos_t, sin_t, taps, spectrum):
    count, outer = taps.shape[0], taps.shape[1]
    signal = [taps[i].astype(bf16) for i in range(count)]
    out = forward(signal, first[...], inner[...], cos_t[...], sin_t[...])
    spectrum[...] = out.astype(bf16).reshape(count, outer, 2 * lane_width)


def convolve_block(tables, signal, filt):
    first, last, inner, inner_back, cos, sin = tables
    outer = cos.shape[0]
    sig = forward(signal, first, inner, cos, sin)
    filt = filt.astype(f32)
    sig_re, sig_im = sig[:, :lane_width], sig[:, lane_width:]
    filt_re, filt_im = filt[:, :lane_width], filt[:, lane_width:]
    prod = jnp.concatenate(
        [
            (filt_re * sig_re - filt_im * sig_im).astype(bf16),
            (filt_re * sig_im + filt_im * sig_re).astype(bf16),
        ],
        axis=1,
    )
    back = jnp.dot(prod, inner_back, preferred_element_type=f32)
    parts = []
    for at in range(0, len(signal), 2):
        cols = []
        for i in range(at, min(at + 2, len(signal))):
            rows = back[i * outer : (i + 1) * outer]
            real, imag = rows[:, :lane_width], rows[:, lane_width:]
            cols.append(
                jnp.concatenate(
                    [
                        (real * cos - imag * sin).astype(bf16),
                        (imag * cos + real * sin).astype(bf16),
                    ],
                    axis=0,
                )
            )
        wide = jnp.dot(last, jnp.concatenate(cols, axis=1), preferred_element_type=f32)
        for i in range(len(cols)):
            parts.append(wide[:, i * lane_width : (i + 1) * lane_width])
    return parts


def conv_kernel(first, last, inner, inner_back, cos_t, sin_t, mixed, spectrum, conv):
    count, outer = mixed.shape[0], mixed.shape[1]
    tables = (first[...], last[...], inner[...], inner_back[...], cos_t[...], sin_t[...])
    filt = spectrum[...].reshape(count * outer, 2 * lane_width)
    parts = convolve_block(tables, [mixed[i] for i in range(count)], filt)
    for i in range(count):
        conv[i] = parts[i].astype(bf16)


def whole(array):
    return pl.BlockSpec(array.shape, lambda i: (0,) * array.ndim)


def block_of(count):
    return max(b for b in range(1, 9) if count % b == 0)


def transform_filter(tables, taps):
    first, last, inner, inner_back, cos_t, sin_t = tables
    count, outer, lanes = taps.shape
    block = block_of(count)
    fixed = (first, inner, cos_t, sin_t)
    return pl.pallas_call(
        filter_kernel,
        grid=(count // block,),
        in_specs=[whole(a) for a in fixed] + [pl.BlockSpec((block, outer, lanes), lambda i: (i, 0, 0))],
        out_specs=pl.BlockSpec((block, outer, 2 * lanes), lambda i: (i, 0, 0)),
        out_shape=jax.ShapeDtypeStruct((count, outer, 2 * lanes), bf16),
        cost_estimate=pl.CostEstimate(
            flops=count * outer * lanes * 1536, bytes_accessed=count * outer * lanes * 8, transcendentals=0
        ),
        name="filter_transform",
    )(*fixed, taps)


def convolve(tables, mixed, spectrum):
    count, outer, lanes = mixed.shape
    block = block_of(count)
    return pl.pallas_call(
        conv_kernel,
        grid=(count // block,),
        in_specs=[whole(a) for a in tables]
        + [
            pl.BlockSpec((block, outer, lanes), lambda i: (i, 0, 0)),
            pl.BlockSpec((block, outer, 2 * lanes), lambda i: (i, 0, 0)),
        ],
        out_specs=pl.BlockSpec((block, outer, lanes), lambda i: (i, 0, 0)),
        out_shape=jax.ShapeDtypeStruct((count, outer, lanes), bf16),
        cost_estimate=pl.CostEstimate(
            flops=count * outer * lanes * 3072, bytes_accessed=count * outer * lanes * 8, transcendentals=0
        ),
        name="convolve",
    )(*tables, mixed, spectrum)


MESH = pl.DeviceIdType.MESH


def layer_kernel(
    first_in, last_in, inner_in, inner_back_in, cos_in, sin_in, skip_in, key, value, gate, kernel, weight,
    output,
    first, last, inner, inner_back, cos_t, sin_t, skip, table_sem, keys, values, taps, tall, wide, long,
    spectrum, mixed_out, mixed_in, pair_in, conv_out, pair_out, conv_in, gates, weights, stacked, gated, total,
    kv_sem, taps_sem, here_sem, joined, ready,
    in_send, in_recv, pair_send, pair_recv, out_send, out_recv, g_send, g_recv, w_send, w_recv,
):
    chunks, segs, chans, tokens = key.shape
    groups = gates.shape[0]
    pairs = pair_in.shape[0]
    alone = chunks - pairs
    share = tokens // groups
    quads = share // lane_width
    features = weight.shape[-1]
    cols = 512 if features % 512 == 0 else features
    outer = cos_t.shape[0]
    slabs = tokens // lane_width
    step = slabs + 8
    long_step = outer + 8
    block = segs * chans
    direct = [1, 2, 4, 6]
    passed = [2, 4, 6]
    s = lax.axis_index("seg")
    h = lax.axis_index("ch")
    side = s // 2
    low = lax.rem(s, 2)
    partner = s + 1 - 2 * low
    tail = segs - 1

    def seg_peer(d):
        return lax.rem(s + d, segs)

    def ch_peer(d):
        return lax.rem(h + d, groups)

    def flipped(at, d):
        for bit in (1, 2, 4):
            if d & bit:
                at = at + bit - 2 * bit * lax.rem(at // bit, 2)
        return at

    def lanes(j):
        return pl.ds(pl.multiple_of(j * lane_width, lane_width), lane_width)

    def tell(semaphore, seg, peer):
        pl.semaphore_signal(semaphore, inc=1, device_id=(seg, peer), device_id_type=MESH)

    barrier = pltpu.get_barrier_semaphore()

    @pl.when(side == 0)
    def _():
        tell(barrier, 2, h)
        tell(barrier, 3, h)

    @pl.when(s == 2)
    def _():
        for seg in (1, 0, 3):
            tell(barrier, seg, h)

    for d in range(1, groups):
        tell(barrier, s, ch_peer(d))

    def load_kv(k):
        return (
            pltpu.make_async_copy(key.at[k], keys.at[k], kv_sem.at[0, k]),
            pltpu.make_async_copy(value.at[k], values.at[k], kv_sem.at[1, k]),
        )

    for k in range(chunks):
        for copy in load_kv(k):
            copy.start()
    fetches = [pltpu.make_async_copy(kernel.at[pl.ds(0, alone), s], taps.at[pl.ds(0, alone)], taps_sem.at[0])]
    for p in range(pairs):
        fetches.append(
            pltpu.make_async_copy(
                kernel.at[alone + p, pl.ds(2 * low, 2)], taps.at[pl.ds(alone + 2 * p, 2)], taps_sem.at[1 + p]
            )
        )
    whole_in = (first_in, last_in, inner_in, inner_back_in, cos_in, sin_in, skip_in)
    whole_here = (first, last, inner, inner_back, cos_t, sin_t, skip)
    loads = [pltpu.make_async_copy(a, b, table_sem.at[i]) for i, (a, b) in enumerate(zip(whole_in, whole_here))]
    for copy in fetches + loads:
        copy.start()

    def part_of(peer):
        return pl.ds(pl.multiple_of(peer * share, lane_width), share)

    own_gate = pltpu.make_async_copy(gate.at[:, :, :, part_of(h)], gates.at[h], here_sem.at[0])
    own_weight = pltpu.make_async_copy(weight, weights.at[h], here_sem.at[1])
    own_gate.start()
    own_weight.start()

    def send_in(k, seg):
        return pltpu.make_async_remote_copy(
            src_ref=mixed_out.at[k, seg], dst_ref=mixed_in.at[k, s],
            send_sem=in_send.at[k, seg], recv_sem=in_recv.at[k, s],
            device_id=(seg, h), device_id_type=MESH,
        )

    def came_in(k, seg):
        return pltpu.make_async_remote_copy(
            src_ref=mixed_out.at[k, seg], dst_ref=mixed_in.at[k, seg],
            send_sem=in_send.at[k, seg], recv_sem=in_recv.at[k, seg],
            device_id=(seg, h), device_id_type=MESH,
        )

    def send_pair(p, seg):
        return pltpu.make_async_remote_copy(
            src_ref=mixed_out.at[alone + p, pl.ds(2 * lax.rem(seg, 2), 2)], dst_ref=pair_in.at[p, s],
            send_sem=pair_send.at[p, seg], recv_sem=pair_recv.at[p, s],
            device_id=(seg, h), device_id_type=MESH,
        )

    def came_pair(p, seg):
        return pltpu.make_async_remote_copy(
            src_ref=pair_in.at[p, seg], dst_ref=pair_in.at[p, seg],
            send_sem=pair_send.at[p, seg], recv_sem=pair_recv.at[p, seg],
            device_id=(seg, h), device_id_type=MESH,
        )

    def send_gate(d):
        peer = ch_peer(d)
        return pltpu.make_async_remote_copy(
            src_ref=gate.at[:, :, :, part_of(peer)], dst_ref=gates.at[h],
            send_sem=g_send.at[d], recv_sem=g_recv.at[d],
            device_id=(s, peer), device_id_type=MESH,
        )

    def send_weight(d):
        return pltpu.make_async_remote_copy(
            src_ref=weight, dst_ref=weights.at[h],
            send_sem=w_send.at[d], recv_sem=w_recv.at[d],
            device_id=(s, flipped(h, d)), device_id_type=MESH,
        )

    def pass_weight(d):
        owner = flipped(h, d)
        return pltpu.make_async_remote_copy(
            src_ref=weights.at[owner], dst_ref=weights.at[owner],
            send_sem=w_send.at[d + 1], recv_sem=w_recv.at[d + 1],
            device_id=(s, flipped(h, 1)), device_id_type=MESH,
        )

    def mix_chunk(k):
        for copy in load_kv(k):
            copy.wait()
        for seg in (2, 3, 0, 1):

            def mix(j, carry):
                both = keys[k, seg, :, lanes(j)].astype(f32) * values[k, seg, :, lanes(j)].astype(f32)
                wide[pl.ds(j, chans, stride=step), :] = both
                return carry

            lax.fori_loop(0, slabs, mix, 0, unroll=4)
            for i in range(chans):
                mixed_out[k, seg, i] = wide[i * step : i * step + slabs, :].astype(bf16)

    def cross(k):
        @pl.when(side == 0)
        def _():
            if k < alone:
                send_in(k, 2).start()
            else:
                send_pair(k - alone, 2).start()

        @pl.when(side == 1)
        def _():
            if k < alone:
                send_in(k, 0).start()
                send_in(k, 1).start()

    def spread_rest(k):
        @pl.when(side == 0)
        def _():
            if k < alone:
                send_in(k, 3).start()
            else:
                send_pair(k - alone, 3).start()

        if k < alone:
            send_in(k, partner).start()
        else:
            send_pair(k - alone, partner).start()

    wait_at = min(2, chunks - 1)
    for k in range(chunks):
        mix_chunk(k)
        if k == 0:

            @pl.when(side == 0)
            def _():
                pl.semaphore_wait(barrier, groups)

            @pl.when(s == 2)
            def _():
                pl.semaphore_wait(barrier, groups + 1)

            @pl.when(s == tail)
            def _():
                pl.semaphore_wait(barrier, groups + 2)
                for seg in (2, 1, 0):
                    tell(joined, seg, h)

        cross(k)
        if k == 0:
            for d in range(1, groups):
                send_gate(d).start()
        if k == wait_at:

            @pl.when(s != tail)
            def _():
                pl.semaphore_wait(joined, 1)

            for d in range(1, segs):
                tell(ready, seg_peer(d), h)
            for e in range(k):
                spread_rest(e)
        if k >= wait_at:
            spread_rest(k)
        if k < alone:
            mixed_in[k, s] = mixed_out[k, s]
        else:
            for e in range(2):
                pair_in[k - alone, s, e] = mixed_out[k, 2 * low + e]

            @pl.when(side == 0)
            def _():
                for seg in (2, 3):
                    pair_in[k - alone, seg] = jnp.zeros((2, chans, slabs, lane_width), bf16)

    for d in direct:
        send_weight(d).start()

    for copy in fetches + loads:
        copy.wait()
    for k in range(alone + 2 * pairs):

        def spread(j, carry):
            tall[pl.ds(j, chans, stride=long_step), :] = taps[k, :, lanes(j)]
            return carry

        lax.fori_loop(0, outer, spread, 0, unroll=4)
        signal = [tall[i * long_step : i * long_step + outer, :].astype(bf16) for i in range(chans)]
        out = forward(signal, first[...], inner[...], cos_t[...], sin_t[...])
        spectrum[k] = out.astype(bf16).reshape(chans, outer, 2 * lane_width)
    pl.semaphore_wait(ready, segs - 1)

    def convolve_rows(at, rows_of, row):
        signal = [rows_of(i).reshape(outer, lane_width) for i in range(chans)]
        filt = spectrum[at].reshape(chans * outer, 2 * lane_width)
        tables = (first[...], last[...], inner[...], inner_back[...], cos_t[...], sin_t[...])
        parts = convolve_block(tables, signal, filt)
        for i in range(chans):
            long[i * long_step : i * long_step + outer, :] = parts[i] + skip[row + i] * signal[i].astype(f32)

    for k in range(alone):
        for d in range(1, segs):
            came_in(k, seg_peer(d)).wait_recv()
        convolve_rows(k, lambda i: mixed_in[k, :, i], (k * segs + s) * chans)

        def gather(j, carry):
            conv_out[k, j] = long[pl.ds(j, chans, stride=long_step), :].astype(bf16)
            return carry

        lax.fori_loop(0, outer, gather, 0, unroll=8)
        for d in (2, 3, 1, 0):
            seg = seg_peer(d)

            def send(e, carry):
                peer = ch_peer(groups - 1 - e)
                pltpu.make_async_remote_copy(
                    src_ref=conv_out.at[k, pl.ds(seg * slabs + peer * quads, quads)], dst_ref=conv_in.at[k, h, s],
                    send_sem=out_send.at[k], recv_sem=out_recv.at[k],
                    device_id=(seg, peer), device_id_type=MESH,
                ).start()
                return carry

            lax.fori_loop(0, groups if d else groups - 1, send, 0)
        for q in range(quads):
            conv_in[k, h, s, q] = conv_out[k, s * slabs + h * quads + q]

    for p in range(pairs):
        k = alone + p
        came_pair(p, partner).wait_recv()

        @pl.when(side == 1)
        def _():
            came_pair(p, 0).wait_recv()
            came_pair(p, 1).wait_recv()

        for e in range(2):
            convolve_rows(k + p + e, lambda i: pair_in[p, :, e, i], (k * segs + 2 * low + e) * chans)

            def gather(j, carry):
                from_row = side * (outer // 2) + j
                pair_out[p, e, j] = long[pl.ds(from_row, chans, stride=long_step), :].astype(bf16)
                return carry

            lax.fori_loop(0, outer // 2, gather, 0, unroll=8)
        for d in range(2):
            seg = s if d else partner

            def send(e, carry):
                peer = ch_peer(groups - 1 - e)
                rows = pl.ds(lax.rem(seg, 2) * slabs + peer * quads, quads)
                pltpu.make_async_remote_copy(
                    src_ref=pair_out.at[p, :, rows], dst_ref=conv_in.at[k, h, pl.ds(2 * low, 2)],
                    send_sem=out_send.at[k], recv_sem=out_recv.at[k],
                    device_id=(seg, peer), device_id_type=MESH,
                ).start()
                return carry

            lax.fori_loop(0, groups - d, send, 0)
        for e in range(2):
            for q in range(quads):
                conv_in[k, h, 2 * low + e, q] = pair_out[p, e, low * slabs + h * quads + q]

    own_gate.wait()
    own_weight.wait()
    for d in passed:
        send_weight(d).wait_recv()
        pass_weight(d).start()
    for d in range(1, groups):
        send_gate(d).wait()
    send_weight(1).wait()
    for d in passed:
        send_weight(d).wait_send()
        pass_weight(d).wait()
    for k in range(chunks):

        def restack(g, carry):
            for at in range(0, segs, 2):
                pair = [weights[g, k, at + e].astype(f32) for e in range(2)]
                rows = pl.ds(pl.multiple_of(g * block + at * chans, 2 * chans), 2 * chans)
                stacked[k, rows, :] = jnp.concatenate(pair, axis=0).astype(bf16)
            return carry

        lax.fori_loop(0, groups, restack, 0)

    def all_pieces(k):
        if k < alone:
            ref = conv_out.at[k, pl.ds(0, outer - quads)]
        else:
            ref = pair_out.at[k - alone, :, pl.ds(0, outer // 2 - quads)]
        return pltpu.make_async_remote_copy(
            src_ref=ref, dst_ref=ref, send_sem=out_send.at[k], recv_sem=out_recv.at[k],
            device_id=(partner, h), device_id_type=MESH,
        )

    order = list(range(alone, chunks)) + list(range(alone))
    for k in order:
        all_pieces(k).wait_recv()

        def combine(g, carry):
            for at in range(0, segs, 2):
                for q in range(quads):
                    both = [
                        conv_in[k, g, at + e, q].astype(f32)
                        * gates[g, k, at + e, :, q * lane_width : (q + 1) * lane_width].astype(f32)
                        for e in range(2)
                    ]
                    rows = pl.ds(pl.multiple_of(g * block + at * chans, 2 * chans), 2 * chans)
                    gated[rows, q * lane_width : (q + 1) * lane_width] = jnp.concatenate(both, axis=0).astype(bf16)
            return carry

        lax.fori_loop(0, groups, combine, 0, unroll=2)
        left = gated[...]
        for n in range(features // cols):
            at = slice(n * cols, (n + 1) * cols)
            prod = lax.dot_general(
                left, stacked[k, :, at], (((0,), (0,)), ((), ())), preferred_element_type=f32
            )
            if k == order[0]:
                total[:, at] = prod
            elif k != order[-1]:
                total[:, at] += prod
            else:
                output[:, at] = (total[:, at] + prod).astype(bf16)

    for k in range(alone):
        for d in range(1, segs):
            send_in(k, seg_peer(d)).wait_send()
    for p in range(pairs):
        send_pair(p, partner).wait_send()

        @pl.when(side == 0)
        def _():
            send_pair(p, 2).wait_send()
            send_pair(p, 3).wait_send()

    for k in range(chunks):
        all_pieces(k).wait_send()


def whole_layer(gate_in, key_in, value_in, kernel, skip_gain, out_weight, chans):
    segs, groups = lax.axis_size("seg"), lax.axis_size("ch")
    channels, tokens = key_in.shape
    full_len = kernel.shape[1]
    outer = full_len // lane_width
    slabs = tokens // lane_width
    features = out_weight.shape[1]
    chunks = channels // segs // chans
    pairs = 1
    alone = chunks - pairs
    share = tokens // groups
    quads = share // lane_width
    tables = make_tables(outer)
    split = (chunks, segs, chans)
    args = (
        *tables,
        skip_gain,
        key_in.reshape(*split, tokens),
        value_in.reshape(*split, tokens),
        gate_in.reshape(*split, tokens),
        kernel.reshape(*split, full_len),
        out_weight.reshape(*split, features),
    )
    hbm = pl.BlockSpec(memory_space=pltpu.HBM)
    dma = pltpu.SemaphoreType.DMA
    regular = pltpu.SemaphoreType.REGULAR
    tall = pltpu.VMEM((chans * (outer + 8), lane_width), f32)
    return pl.pallas_call(
        layer_kernel,
        in_specs=[hbm] * len(args),
        out_specs=pl.BlockSpec(memory_space=pltpu.VMEM),
        out_shape=pltpu.VMEM((share, features), bf16),
        scratch_shapes=[pltpu.VMEM(a.shape, a.dtype) for a in tables]
        + [
            pltpu.SMEM(skip_gain.shape, f32),
            dma((len(tables) + 1,)),
            pltpu.VMEM((*split, tokens), bf16),
            pltpu.VMEM((*split, tokens), bf16),
            pltpu.VMEM((alone + 2 * pairs, chans, full_len), f32),
            tall,
            pltpu.VMEM((chans * (slabs + 8), lane_width), f32),
            tall,
            pltpu.VMEM((alone + 2 * pairs, chans, outer, 2 * lane_width), bf16),
            pltpu.VMEM((*split, slabs, lane_width), bf16),
            pltpu.VMEM((alone, segs, chans, slabs, lane_width), bf16),
            pltpu.VMEM((pairs, segs, 2, chans, slabs, lane_width), bf16),
            pltpu.VMEM((alone, outer, chans, lane_width), bf16),
            pltpu.VMEM((pairs, 2, outer // 2, chans, lane_width), bf16),
            pltpu.VMEM((chunks, groups, segs, quads, chans, lane_width), bf16),
            pltpu.VMEM((groups, *split, share), bf16),
            pltpu.VMEM((groups, *split, features), bf16),
            pltpu.VMEM((chunks, groups * segs * chans, features), bf16),
            pltpu.VMEM((groups * segs * chans, share), bf16),
            pltpu.VMEM((share, features), f32),
            dma((2, chunks)), dma((1 + pairs,)), dma((2,)), regular, regular,
            dma((alone, segs)), dma((alone, segs)), dma((pairs, segs)), dma((pairs, segs)),
            dma((chunks,)), dma((chunks,)),
            dma((groups,)), dma((groups,)), dma((groups,)), dma((groups,)),
        ],
        compiler_params=pltpu.CompilerParams(
            collective_id=0, has_side_effects=True, vmem_limit_bytes=56 * 1024 * 1024
        ),
        name="layer",
    )(*args)


def on_device(gate_in, key_in, value_in, kernel, skip_gain, out_weight):
    seg_count = lax.axis_size("seg")
    seg_index = lax.axis_index("seg")
    channels, tokens = key_in.shape
    full_len = kernel.shape[1]
    outer = full_len // lane_width
    tables = make_tables(outer)
    col_count = channels // seg_count
    sublanes = 8
    fits = (seg_count, lax.axis_size("ch")) == (4, 8) and col_count % sublanes == 0 and col_count > sublanes
    if fits and tokens // lax.axis_size("ch") % lane_width == 0:
        return whole_layer(gate_in, key_in, value_in, kernel, skip_gain, out_weight, sublanes)
    mixed = key_in.astype(f32) * value_in.astype(f32)
    mixed_sent = mixed.astype(bf16).reshape(channels, tokens // lane_width, lane_width)
    col_mixed = lax.all_to_all(mixed_sent, "seg", split_axis=0, concat_axis=1, tiled=True)
    taps = lax.dynamic_slice_in_dim(kernel, seg_index * col_count, col_count, 0)
    spectrum = transform_filter(tables, taps.astype(bf16).reshape(col_count, outer, lane_width))
    col_conv = convolve(tables, col_mixed, spectrum)
    conv = lax.all_to_all(col_conv, "seg", split_axis=1, concat_axis=0, tiled=True)
    conv = conv.reshape(channels, tokens).astype(f32)
    gated = (gate_in.astype(f32) * (conv + skip_gain[:, None] * mixed)).astype(bf16)
    mine = lax.all_to_all(gated, "ch", split_axis=1, concat_axis=0, tiled=True)
    weight = lax.all_gather(out_weight, "ch", axis=0, tiled=True)
    result = lax.dot_general(
        mine, weight, (((0,), (0,)), ((), ())), preferred_element_type=f32
    )
    return result.astype(bf16)


def solution(mesh):
    placed = (P("ch", "seg"), P("ch", "seg"), P("ch", "seg"), P("ch", None), P("ch"), P("ch", None))
    return jax.shard_map(
        on_device, mesh=mesh, in_specs=placed, out_specs=P(("seg", "ch"), None), check_vma=False
    )
```

```python
import functools
import math

import jax
import jax.numpy as jnp
import numpy as np
from jax import lax
from jax.experimental import pallas as pl
from jax.experimental.pallas import tpu as pltpu
from jax.sharding import PartitionSpec as P

lane_width = 128
bf16 = jnp.bfloat16
f32 = jnp.float32


def angles(rows, cols, period):
    theta = (rows[:, None] * cols[None, :] % (4 * period)) * (2.0 * math.pi / (4 * period))
    return np.cos(theta), np.sin(theta)


def make_tables(outer):
    quarter = 4 * np.arange(outer) + 1
    row = np.arange(outer)
    lane = np.arange(lane_width)
    cos_o, sin_o = angles(quarter, row, outer)
    cos_t, sin_t = angles(quarter, lane, outer * lane_width)
    cos_i, sin_i = angles(4 * lane, lane, lane_width)
    first = np.concatenate([cos_o, -sin_o], axis=0)
    last = np.concatenate([cos_o.T, -sin_o.T], axis=1) / (outer * lane_width)
    inner = np.block([[cos_i, -sin_i], [sin_i, cos_i]])
    inner_back = np.block([[cos_i, sin_i], [-sin_i, cos_i]])
    narrow = [jnp.asarray(m.astype(np.float32).astype(bf16)) for m in (first, last, inner, inner_back)]
    return (*narrow, jnp.asarray(cos_t.astype(np.float32)), jnp.asarray(sin_t.astype(np.float32)))


def forward(signal, first, inner, cos_t, sin_t):
    outer = cos_t.shape[0]
    rows = []
    for at in range(0, len(signal), 2):
        pair = signal[at : at + 2]
        wide = jnp.dot(first, jnp.concatenate(pair, axis=1), preferred_element_type=f32)
        for i in range(len(pair)):
            part = wide[:, i * lane_width : (i + 1) * lane_width]
            real, imag = part[:outer], part[outer:]
            rows.append(
                jnp.concatenate(
                    [
                        (real * cos_t + imag * sin_t).astype(bf16),
                        (imag * cos_t - real * sin_t).astype(bf16),
                    ],
                    axis=1,
                )
            )
    return jnp.dot(jnp.concatenate(rows, axis=0), inner, preferred_element_type=f32)


def filter_kernel(first, inner, cos_t, sin_t, taps, spectrum):
    count, outer = taps.shape[0], taps.shape[1]
    signal = [taps[i].astype(bf16) for i in range(count)]
    out = forward(signal, first[...], inner[...], cos_t[...], sin_t[...])
    spectrum[...] = out.astype(bf16).reshape(count, outer, 2 * lane_width)


def convolve_block(tables, signal, filt):
    first, last, inner, inner_back, cos, sin = tables
    outer = cos.shape[0]
    sig = forward(signal, first, inner, cos, sin)
    filt = filt.astype(f32)
    sig_re, sig_im = sig[:, :lane_width], sig[:, lane_width:]
    filt_re, filt_im = filt[:, :lane_width], filt[:, lane_width:]
    prod = jnp.concatenate(
        [
            (filt_re * sig_re - filt_im * sig_im).astype(bf16),
            (filt_re * sig_im + filt_im * sig_re).astype(bf16),
        ],
        axis=1,
    )
    back = jnp.dot(prod, inner_back, preferred_element_type=f32)
    parts = []
    for at in range(0, len(signal), 2):
        cols = []
        for i in range(at, min(at + 2, len(signal))):
            rows = back[i * outer : (i + 1) * outer]
            real, imag = rows[:, :lane_width], rows[:, lane_width:]
            cols.append(
                jnp.concatenate(
                    [
                        (real * cos - imag * sin).astype(bf16),
                        (imag * cos + real * sin).astype(bf16),
                    ],
                    axis=0,
                )
            )
        wide = jnp.dot(last, jnp.concatenate(cols, axis=1), preferred_element_type=f32)
        for i in range(len(cols)):
            parts.append(wide[:, i * lane_width : (i + 1) * lane_width])
    return parts


def conv_kernel(first, last, inner, inner_back, cos_t, sin_t, mixed, spectrum, conv):
    count, outer = mixed.shape[0], mixed.shape[1]
    tables = (first[...], last[...], inner[...], inner_back[...], cos_t[...], sin_t[...])
    filt = spectrum[...].reshape(count * outer, 2 * lane_width)
    parts = convolve_block(tables, [mixed[i] for i in range(count)], filt)
    for i in range(count):
        conv[i] = parts[i].astype(bf16)


def whole(array):
    return pl.BlockSpec(array.shape, lambda i: (0,) * array.ndim)


def block_of(count):
    return max(b for b in range(1, 9) if count % b == 0)


def transform_filter(tables, taps):
    first, last, inner, inner_back, cos_t, sin_t = tables
    count, outer, lanes = taps.shape
    block = block_of(count)
    fixed = (first, inner, cos_t, sin_t)
    return pl.pallas_call(
        filter_kernel,
        grid=(count // block,),
        in_specs=[whole(a) for a in fixed] + [pl.BlockSpec((block, outer, lanes), lambda i: (i, 0, 0))],
        out_specs=pl.BlockSpec((block, outer, 2 * lanes), lambda i: (i, 0, 0)),
        out_shape=jax.ShapeDtypeStruct((count, outer, 2 * lanes), bf16),
        cost_estimate=pl.CostEstimate(
            flops=count * outer * lanes * 1536, bytes_accessed=count * outer * lanes * 8, transcendentals=0
        ),
        name="filter_transform",
    )(*fixed, taps)


def convolve(tables, mixed, spectrum):
    count, outer, lanes = mixed.shape
    block = block_of(count)
    return pl.pallas_call(
        conv_kernel,
        grid=(count // block,),
        in_specs=[whole(a) for a in tables]
        + [
            pl.BlockSpec((block, outer, lanes), lambda i: (i, 0, 0)),
            pl.BlockSpec((block, outer, 2 * lanes), lambda i: (i, 0, 0)),
        ],
        out_specs=pl.BlockSpec((block, outer, lanes), lambda i: (i, 0, 0)),
        out_shape=jax.ShapeDtypeStruct((count, outer, lanes), bf16),
        cost_estimate=pl.CostEstimate(
            flops=count * outer * lanes * 3072, bytes_accessed=count * outer * lanes * 8, transcendentals=0
        ),
        name="convolve",
    )(*tables, mixed, spectrum)


MESH = pl.DeviceIdType.MESH


def layer_kernel(
    first_in, last_in, inner_in, inner_back_in, cos_in, sin_in, skip_in, key, value, gate, kernel, weight,
    output,
    first, last, inner, inner_back, cos_t, sin_t, skip, keys, values, taps, tall, wide, long,
    spectrum, mixed_out, mixed_in, pair_in, conv_out, pair_out, conv_in, gates, weights, stacked, gated, total,
    kv_sem, here_sem, joined, ready, sent, in_recv, pair_recv, out_recv, g_recv, w_recv,
):
    chunks, segs, chans, tokens = key.shape
    groups = gates.shape[0]
    pairs = pair_in.shape[0]
    alone = chunks - pairs
    share = tokens // groups
    quads = share // lane_width
    features = weight.shape[-1]
    cols = 512 if features % 512 == 0 else features
    outer = cos_t.shape[0]
    slabs = tokens // lane_width
    step = slabs + 8
    long_step = outer + 8
    block = segs * chans
    direct = [1, 2, 4, 6]
    passed = [2, 4, 6]
    s = lax.axis_index("seg")
    h = lax.axis_index("ch")
    side = s // 2
    low = lax.rem(s, 2)
    partner = s + 1 - 2 * low
    tail = segs - 1

    def seg_peer(d):
        return lax.rem(s + d, segs)

    def ch_peer(d):
        return lax.rem(h + d, groups)

    def flipped(at, d):
        for bit in (1, 2, 4):
            if d & bit:
                at = at + bit - 2 * bit * lax.rem(at // bit, 2)
        return at

    def lanes(j):
        return pl.ds(pl.multiple_of(j * lane_width, lane_width), lane_width)

    def tell(semaphore, seg, peer):
        pl.semaphore_signal(semaphore, inc=1, device_id=(seg, peer), device_id_type=MESH)

    def load_kv(at, size, sem):
        part = pl.ds(at, size)
        return (
            pltpu.make_async_copy(key.at[part], keys.at[part], kv_sem.at[sem]),
            pltpu.make_async_copy(value.at[part], values.at[part], kv_sem.at[sem]),
        )

    for copy in load_kv(0, 1, 0):
        copy.start()
    barrier = pltpu.get_barrier_semaphore()

    @pl.when(side == 0)
    def _():
        tell(barrier, 2, h)
        tell(barrier, 3, h)

    @pl.when(s == 2)
    def _():
        for seg in (1, 0, 3):
            tell(barrier, seg, h)

    for d in range(1, groups):
        tell(barrier, s, ch_peer(d))

    def part_of(peer):
        return pl.ds(pl.multiple_of(peer * share, lane_width), share)

    whole_in = (first_in, last_in, inner_in, inner_back_in, cos_in, sin_in, skip_in)
    whole_here = (first, last, inner, inner_back, cos_t, sin_t, skip)
    moves = list(zip(whole_in, whole_here)) + [
        (kernel.at[pl.ds(0, alone), s], taps.at[pl.ds(0, alone)]),
        (gate.at[:, :, :, part_of(h)], gates.at[h]),
        (weight, weights.at[h]),
    ]
    for p in range(pairs):
        moves.append((kernel.at[alone + p, pl.ds(2 * low, 2)], taps.at[pl.ds(alone + 2 * p, 2)]))
    loads = [pltpu.make_async_copy(a, b, here_sem) for a, b in moves]

    def remote(source, target, recv, seg, peer):
        return pltpu.make_async_remote_copy(
            src_ref=source, dst_ref=target, send_sem=sent, recv_sem=recv,
            device_id=(seg, peer), device_id_type=MESH,
        )

    def bulk(ref, recv):
        return remote(ref, ref, recv, partner, h)

    def send_in(k, seg):
        return remote(mixed_out.at[k, seg], mixed_in.at[k, s], in_recv.at[k], seg, h)

    def send_pair(p, seg):
        source = mixed_out.at[alone + p, pl.ds(2 * lax.rem(seg, 2), 2)]
        return remote(source, pair_in.at[p, s], pair_recv.at[p], seg, h)

    def send_gate(d):
        peer = ch_peer(d)
        return remote(gate.at[:, :, :, part_of(peer)], gates.at[h], g_recv, s, peer)

    def send_weight(d):
        return remote(weight, weights.at[h], w_recv.at[0], s, flipped(h, d))

    def pass_weight(d):
        owner = flipped(h, d)
        return remote(weights.at[owner], weights.at[owner], w_recv.at[1], s, flipped(h, 1))

    def mix_part(k, seg):
        def mix(j, carry):
            both = keys[k, seg, :, lanes(j)].astype(f32) * values[k, seg, :, lanes(j)].astype(f32)
            wide[pl.ds(j, chans, stride=step), :] = both
            return carry

        lax.fori_loop(0, slabs, mix, 0, unroll=4)
        for i in range(chans):
            mixed_out[k, seg, i] = wide[i * step : i * step + slabs, :].astype(bf16)

    def cross(k):
        @pl.when(side == 0)
        def _():
            if k >= alone:
                send_pair(k - alone, 2).start()
            elif k:
                send_in(k, 2).start()

        @pl.when(side == 1)
        def _():
            if k < alone:
                send_in(k, 0).start()
                send_in(k, 1).start()

    def spread_rest(k):
        @pl.when(side == 0)
        def _():
            if k < alone:
                send_in(k, 3).start()
            else:
                send_pair(k - alone, 3).start()

        if k < alone:
            send_in(k, partner).start()
        else:
            send_pair(k - alone, partner).start()

    wait_at = min(2, chunks - 1)
    for k in range(chunks):
        if k < 2:
            for copy in load_kv(k, chunks - 1 if k else 1, k):
                copy.wait()
        mix_part(k, 2)
        if k == 0:

            @pl.when(side == 0)
            def _():
                pl.semaphore_wait(barrier, groups)
                send_in(0, 2).start()

            @pl.when(s == 2)
            def _():
                pl.semaphore_wait(barrier, groups + 1)

            @pl.when(s == tail)
            def _():
                pl.semaphore_wait(barrier, groups + 2)
                for seg in (2, 1, 0):
                    tell(joined, seg, h)

            for copy in [*load_kv(1, chunks - 1, 1), *loads]:
                copy.start()
        for seg in (3, 0, 1):
            mix_part(k, seg)
        cross(k)
        if k == 0:
            for d in range(1, groups):
                send_gate(d).start()
        if k == wait_at:

            @pl.when(s != tail)
            def _():
                pl.semaphore_wait(joined, 1)

            for d in range(1, segs):
                tell(ready, seg_peer(d), h)
            for e in range(k):
                spread_rest(e)
        if k >= wait_at:
            spread_rest(k)
        if k < alone:
            mixed_in[k, s] = mixed_out[k, s]
        else:
            for e in range(2):
                pair_in[k - alone, s, e] = mixed_out[k, 2 * low + e]

            @pl.when(side == 0)
            def _():
                for seg in (2, 3):
                    pair_in[k - alone, seg] = jnp.zeros((2, chans, slabs, lane_width), bf16)

    for d in direct:
        send_weight(d).start()

    for copy in loads:
        copy.wait()
    for k in range(alone + 2 * pairs):

        def spread(j, carry):
            tall[pl.ds(j, chans, stride=long_step), :] = taps[k, :, lanes(j)]
            return carry

        lax.fori_loop(0, outer, spread, 0, unroll=4)
        signal = [tall[i * long_step : i * long_step + outer, :].astype(bf16) for i in range(chans)]
        out = forward(signal, first[...], inner[...], cos_t[...], sin_t[...])
        spectrum[k] = out.astype(bf16).reshape(chans, outer, 2 * lane_width)
    pl.semaphore_wait(ready, segs - 1)

    def slot(k, q):
        return chunks - 1 + q if k == alone - 1 else k if k < alone else k - 1

    def convolve_rows(at, rows_of, row):
        signal = [rows_of(i).reshape(outer, lane_width) for i in range(chans)]
        filt = spectrum[at].reshape(chans * outer, 2 * lane_width)
        tables = (first[...], last[...], inner[...], inner_back[...], cos_t[...], sin_t[...])
        parts = convolve_block(tables, signal, filt)
        for i in range(chans):
            long[i * long_step : i * long_step + outer, :] = parts[i] + skip[row + i] * signal[i].astype(f32)

    for k in range(alone):
        bulk(mixed_in.at[k, pl.ds(0, segs - 1)], in_recv.at[k]).wait_recv()
        convolve_rows(k, lambda i: mixed_in[k, :, i], (k * segs + s) * chans)

        def gather(j, carry):
            conv_out[k, j] = long[pl.ds(j, chans, stride=long_step), :].astype(bf16)
            return carry

        lax.fori_loop(0, outer, gather, 0, unroll=8)
        size = 1 if k == alone - 1 else quads
        for q in range(0, quads, size):
            for d in (2, 3, 1, 0):
                seg = seg_peer(d)

                def send(e, carry):
                    peer = ch_peer(groups - 1 - e)
                    source = conv_out.at[k, pl.ds(seg * slabs + peer * quads + q, size)]
                    target = conv_in.at[k, h, s, pl.ds(q, size)]
                    remote(source, target, out_recv.at[slot(k, q)], seg, peer).start()
                    return carry

                lax.fori_loop(0, groups if d else groups - 1, send, 0)
        for q in range(quads):
            conv_in[k, h, s, q] = conv_out[k, s * slabs + h * quads + q]

    for p in range(pairs):
        k = alone + p

        @pl.when(side == 0)
        def _():
            bulk(pair_in.at[p, 0], pair_recv.at[p]).wait_recv()

        @pl.when(side == 1)
        def _():
            bulk(pair_in.at[p, pl.ds(0, segs - 1)], pair_recv.at[p]).wait_recv()

        for e in range(2):
            convolve_rows(k + p + e, lambda i: pair_in[p, :, e, i], (k * segs + 2 * low + e) * chans)

            def gather(j, carry):
                from_row = side * (outer // 2) + j
                pair_out[p, e, j] = long[pl.ds(from_row, chans, stride=long_step), :].astype(bf16)
                return carry

            lax.fori_loop(0, outer // 2, gather, 0, unroll=8)
        for d in range(2):
            seg = s if d else partner

            def send(e, carry):
                peer = ch_peer(groups - 1 - e)
                rows = pl.ds(lax.rem(seg, 2) * slabs + peer * quads, quads)
                target = conv_in.at[k, h, pl.ds(2 * low, 2)]
                remote(pair_out.at[p, :, rows], target, out_recv.at[slot(k, 0)], seg, peer).start()
                return carry

            lax.fori_loop(0, groups - d, send, 0)
        for e in range(2):
            for q in range(quads):
                conv_in[k, h, 2 * low + e, q] = pair_out[p, e, low * slabs + h * quads + q]

    bulk(weights.at[pl.ds(0, len(direct))], w_recv.at[0]).wait_recv()
    for d in passed:
        pass_weight(d).start()
    bulk(gates.at[pl.ds(0, groups - 1)], g_recv).wait_recv()
    bulk(weights.at[pl.ds(0, len(passed))], w_recv.at[1]).wait_recv()
    for k in range(chunks):

        def restack(g, carry):
            for at in range(0, segs, 2):
                pair = [weights[g, k, at + e].astype(f32) for e in range(2)]
                rows = pl.ds(pl.multiple_of(g * block + at * chans, 2 * chans), 2 * chans)
                stacked[k, rows, :] = jnp.concatenate(pair, axis=0).astype(bf16)
            return carry

        lax.fori_loop(0, groups, restack, 0)

    def all_pieces(k, q, size):
        if k < alone:
            ref = conv_out.at[k, pl.ds(0, (segs * groups - 1) * size)]
        else:
            ref = pair_out.at[k - alone, :, pl.ds(0, outer // 2 - quads)]
        return bulk(ref, out_recv.at[slot(k, q)])

    order = list(range(alone, chunks)) + list(range(alone))
    steps = [(k, 0, quads) for k in order[:-1]] + [(order[-1], q, 1) for q in range(quads)]
    for k, start, size in steps:
        all_pieces(k, start, size).wait_recv()

        def combine(g, carry):
            for at in range(0, segs, 2):
                for q in range(start, start + size):
                    both = [
                        conv_in[k, g, at + e, q].astype(f32)
                        * gates[g, k, at + e, :, q * lane_width : (q + 1) * lane_width].astype(f32)
                        for e in range(2)
                    ]
                    rows = pl.ds(pl.multiple_of(g * block + at * chans, 2 * chans), 2 * chans)
                    gated[rows, q * lane_width : (q + 1) * lane_width] = jnp.concatenate(both, axis=0).astype(bf16)
            return carry

        lax.fori_loop(0, groups, combine, 0, unroll=2)
        tokens_at = slice(start * lane_width, (start + size) * lane_width)
        left = gated[:, tokens_at]
        for n in range(features // cols):
            at = slice(n * cols, (n + 1) * cols)
            prod = lax.dot_general(
                left, stacked[k, :, at], (((0,), (0,)), ((), ())), preferred_element_type=f32
            )
            if k == order[0]:
                total[:, at] = prod
            elif k != order[-1]:
                total[:, at] += prod
            else:
                output[tokens_at, at] = (total[tokens_at, at] + prod).astype(bf16)

    bulk(mixed_in.at[:, pl.ds(0, segs - 1)], g_recv).wait_send()
    for p in range(pairs):

        @pl.when(side == 0)
        def _():
            bulk(pair_in.at[p, pl.ds(0, segs - 1)], g_recv).wait_send()

        @pl.when(side == 1)
        def _():
            bulk(pair_in.at[p, 0], g_recv).wait_send()

    bulk(gates.at[pl.ds(0, groups - 1)], g_recv).wait_send()
    bulk(weights.at[pl.ds(0, groups - 1)], g_recv).wait_send()
    for k, start, size in steps:
        all_pieces(k, start, size).wait_send()


def whole_layer(gate_in, key_in, value_in, kernel, skip_gain, out_weight, chans):
    segs, groups = lax.axis_size("seg"), lax.axis_size("ch")
    channels, tokens = key_in.shape
    full_len = kernel.shape[1]
    outer = full_len // lane_width
    slabs = tokens // lane_width
    features = out_weight.shape[1]
    chunks = channels // segs // chans
    pairs = 1
    alone = chunks - pairs
    share = tokens // groups
    quads = share // lane_width
    tables = make_tables(outer)
    split = (chunks, segs, chans)
    args = (
        *tables,
        skip_gain,
        key_in.reshape(*split, tokens),
        value_in.reshape(*split, tokens),
        gate_in.reshape(*split, tokens),
        kernel.reshape(*split, full_len),
        out_weight.reshape(*split, features),
    )
    hbm = pl.BlockSpec(memory_space=pltpu.HBM)
    dma = pltpu.SemaphoreType.DMA
    regular = pltpu.SemaphoreType.REGULAR
    tall = pltpu.VMEM((chans * (outer + 8), lane_width), f32)
    return pl.pallas_call(
        layer_kernel,
        in_specs=[hbm] * len(args),
        out_specs=pl.BlockSpec(memory_space=pltpu.VMEM),
        out_shape=pltpu.VMEM((share, features), bf16),
        scratch_shapes=[pltpu.VMEM(a.shape, a.dtype) for a in tables]
        + [
            pltpu.SMEM(skip_gain.shape, f32),
            pltpu.VMEM((*split, tokens), bf16),
            pltpu.VMEM((*split, tokens), bf16),
            pltpu.VMEM((alone + 2 * pairs, chans, full_len), f32),
            tall,
            pltpu.VMEM((chans * (slabs + 8), lane_width), f32),
            tall,
            pltpu.VMEM((alone + 2 * pairs, chans, outer, 2 * lane_width), bf16),
            pltpu.VMEM((*split, slabs, lane_width), bf16),
            pltpu.VMEM((alone, segs, chans, slabs, lane_width), bf16),
            pltpu.VMEM((pairs, segs, 2, chans, slabs, lane_width), bf16),
            pltpu.VMEM((alone, outer, chans, lane_width), bf16),
            pltpu.VMEM((pairs, 2, outer // 2, chans, lane_width), bf16),
            pltpu.VMEM((chunks, groups, segs, quads, chans, lane_width), bf16),
            pltpu.VMEM((groups, *split, share), bf16),
            pltpu.VMEM((groups, *split, features), bf16),
            pltpu.VMEM((chunks, groups * segs * chans, features), bf16),
            pltpu.VMEM((groups * segs * chans, share), bf16),
            pltpu.VMEM((share, features), f32),
            dma((2,)), dma, regular, regular, dma, dma((alone,)), dma((pairs,)), dma((chunks - 1 + quads,)), dma, dma((2,)),
        ],
        compiler_params=pltpu.CompilerParams(
            collective_id=0, has_side_effects=True, vmem_limit_bytes=56 * 1024 * 1024
        ),
        name="layer",
    )(*args)


def on_device(gate_in, key_in, value_in, kernel, skip_gain, out_weight):
    seg_count = lax.axis_size("seg")
    seg_index = lax.axis_index("seg")
    channels, tokens = key_in.shape
    full_len = kernel.shape[1]
    outer = full_len // lane_width
    tables = make_tables(outer)
    col_count = channels // seg_count
    sublanes = 8
    fits = (seg_count, lax.axis_size("ch")) == (4, 8) and col_count % sublanes == 0 and col_count > sublanes
    if fits and tokens // lax.axis_size("ch") % lane_width == 0:
        return whole_layer(gate_in, key_in, value_in, kernel, skip_gain, out_weight, sublanes)
    mixed = key_in.astype(f32) * value_in.astype(f32)
    mixed_sent = mixed.astype(bf16).reshape(channels, tokens // lane_width, lane_width)
    col_mixed = lax.all_to_all(mixed_sent, "seg", split_axis=0, concat_axis=1, tiled=True)
    taps = lax.dynamic_slice_in_dim(kernel, seg_index * col_count, col_count, 0)
    spectrum = transform_filter(tables, taps.astype(bf16).reshape(col_count, outer, lane_width))
    col_conv = convolve(tables, col_mixed, spectrum)
    conv = lax.all_to_all(col_conv, "seg", split_axis=1, concat_axis=0, tiled=True)
    conv = conv.reshape(channels, tokens).astype(f32)
    gated = (gate_in.astype(f32) * (conv + skip_gain[:, None] * mixed)).astype(bf16)
    mine = lax.all_to_all(gated, "ch", split_axis=1, concat_axis=0, tiled=True)
    weight = lax.all_gather(out_weight, "ch", axis=0, tiled=True)
    result = lax.dot_general(
        mine, weight, (((0,), (0,)), ((), ())), preferred_element_type=f32
    )
    return result.astype(bf16)


def solution(mesh):
    placed = (P("ch", "seg"), P("ch", "seg"), P("ch", "seg"), P("ch", None), P("ch"), P("ch", None))
    return jax.shard_map(
        on_device, mesh=mesh, in_specs=placed, out_specs=P(("seg", "ch"), None), check_vma=False
    )
```

```python
import functools
import math

import jax
import jax.numpy as jnp
import numpy as np
from jax import lax
from jax.experimental import pallas as pl
from jax.experimental.pallas import tpu as pltpu
from jax.sharding import PartitionSpec as P

lane_width = 128
bf16 = jnp.bfloat16
f32 = jnp.float32


def angles(rows, cols, period):
    theta = (rows[:, None] * cols[None, :] % (4 * period)) * (2.0 * math.pi / (4 * period))
    return np.cos(theta), np.sin(theta)


def make_tables(outer):
    quarter = 4 * np.arange(outer) + 1
    row = np.arange(outer)
    lane = np.arange(lane_width)
    cos_o, sin_o = angles(quarter, row, outer)
    cos_t, sin_t = angles(quarter, lane, outer * lane_width)
    cos_i, sin_i = angles(4 * lane, lane, lane_width)
    first = np.concatenate([cos_o, -sin_o], axis=0)
    last = np.concatenate([cos_o.T, -sin_o.T], axis=1) / (outer * lane_width)
    inner = np.block([[cos_i, -sin_i], [sin_i, cos_i]])
    inner_back = np.block([[cos_i, sin_i], [-sin_i, cos_i]])
    narrow = [jnp.asarray(m.astype(np.float32).astype(bf16)) for m in (first, last, inner, inner_back)]
    return (*narrow, jnp.asarray(cos_t.astype(np.float32)), jnp.asarray(sin_t.astype(np.float32)))


def forward(signal, first, inner, cos_t, sin_t):
    outer = cos_t.shape[0]
    rows = []
    for at in range(0, len(signal), 2):
        pair = signal[at : at + 2]
        wide = jnp.dot(first, jnp.concatenate(pair, axis=1), preferred_element_type=f32)
        for i in range(len(pair)):
            part = wide[:, i * lane_width : (i + 1) * lane_width]
            real, imag = part[:outer], part[outer:]
            rows.append(
                jnp.concatenate(
                    [
                        (real * cos_t + imag * sin_t).astype(bf16),
                        (imag * cos_t - real * sin_t).astype(bf16),
                    ],
                    axis=1,
                )
            )
    return jnp.dot(jnp.concatenate(rows, axis=0), inner, preferred_element_type=f32)


def filter_kernel(first, inner, cos_t, sin_t, taps, spectrum):
    count, outer = taps.shape[0], taps.shape[1]
    signal = [taps[i].astype(bf16) for i in range(count)]
    out = forward(signal, first[...], inner[...], cos_t[...], sin_t[...])
    spectrum[...] = out.astype(bf16).reshape(count, outer, 2 * lane_width)


def convolve_block(tables, signal, filt):
    first, last, inner, inner_back, cos, sin = tables
    outer = cos.shape[0]
    sig = forward(signal, first, inner, cos, sin)
    filt = filt.astype(f32)
    sig_re, sig_im = sig[:, :lane_width], sig[:, lane_width:]
    filt_re, filt_im = filt[:, :lane_width], filt[:, lane_width:]
    prod = jnp.concatenate(
        [
            (filt_re * sig_re - filt_im * sig_im).astype(bf16),
            (filt_re * sig_im + filt_im * sig_re).astype(bf16),
        ],
        axis=1,
    )
    back = jnp.dot(prod, inner_back, preferred_element_type=f32)
    parts = []
    for at in range(0, len(signal), 2):
        cols = []
        for i in range(at, min(at + 2, len(signal))):
            rows = back[i * outer : (i + 1) * outer]
            real, imag = rows[:, :lane_width], rows[:, lane_width:]
            cols.append(
                jnp.concatenate(
                    [
                        (real * cos - imag * sin).astype(bf16),
                        (imag * cos + real * sin).astype(bf16),
                    ],
                    axis=0,
                )
            )
        wide = jnp.dot(last, jnp.concatenate(cols, axis=1), preferred_element_type=f32)
        for i in range(len(cols)):
            parts.append(wide[:, i * lane_width : (i + 1) * lane_width])
    return parts


def conv_kernel(first, last, inner, inner_back, cos_t, sin_t, mixed, spectrum, conv):
    count, outer = mixed.shape[0], mixed.shape[1]
    tables = (first[...], last[...], inner[...], inner_back[...], cos_t[...], sin_t[...])
    filt = spectrum[...].reshape(count * outer, 2 * lane_width)
    parts = convolve_block(tables, [mixed[i] for i in range(count)], filt)
    for i in range(count):
        conv[i] = parts[i].astype(bf16)


def whole(array):
    return pl.BlockSpec(array.shape, lambda i: (0,) * array.ndim)


def block_of(count):
    return max(b for b in range(1, 9) if count % b == 0)


def transform_filter(tables, taps):
    first, last, inner, inner_back, cos_t, sin_t = tables
    count, outer, lanes = taps.shape
    block = block_of(count)
    fixed = (first, inner, cos_t, sin_t)
    return pl.pallas_call(
        filter_kernel,
        grid=(count // block,),
        in_specs=[whole(a) for a in fixed] + [pl.BlockSpec((block, outer, lanes), lambda i: (i, 0, 0))],
        out_specs=pl.BlockSpec((block, outer, 2 * lanes), lambda i: (i, 0, 0)),
        out_shape=jax.ShapeDtypeStruct((count, outer, 2 * lanes), bf16),
        cost_estimate=pl.CostEstimate(
            flops=count * outer * lanes * 1536, bytes_accessed=count * outer * lanes * 8, transcendentals=0
        ),
        name="filter_transform",
    )(*fixed, taps)


def convolve(tables, mixed, spectrum):
    count, outer, lanes = mixed.shape
    block = block_of(count)
    return pl.pallas_call(
        conv_kernel,
        grid=(count // block,),
        in_specs=[whole(a) for a in tables]
        + [
            pl.BlockSpec((block, outer, lanes), lambda i: (i, 0, 0)),
            pl.BlockSpec((block, outer, 2 * lanes), lambda i: (i, 0, 0)),
        ],
        out_specs=pl.BlockSpec((block, outer, lanes), lambda i: (i, 0, 0)),
        out_shape=jax.ShapeDtypeStruct((count, outer, lanes), bf16),
        cost_estimate=pl.CostEstimate(
            flops=count * outer * lanes * 3072, bytes_accessed=count * outer * lanes * 8, transcendentals=0
        ),
        name="convolve",
    )(*tables, mixed, spectrum)


MESH = pl.DeviceIdType.MESH


def layer_kernel(
    first_in, last_in, inner_in, inner_back_in, cos_in, sin_in, skip_in, key, value, gate, kernel, weight,
    output,
    first, last, inner, inner_back, cos_t, sin_t, skip, keys, values, taps, tall, wide, long,
    spectrum, mixed_out, mixed_in, pair_in, conv_out, pair_out, conv_in, gates, weights, stacked, gated, total,
    kv_sem, here_sem, joined, ready, sent, in_recv, pair_recv, out_recv, g_recv, w_recv,
):
    chunks, segs, chans, tokens = key.shape
    groups = gates.shape[0]
    pairs = pair_in.shape[0]
    alone = chunks - pairs
    share = tokens // groups
    quads = share // lane_width
    features = weight.shape[-1]
    cols = 512 if features % 512 == 0 else features
    outer = cos_t.shape[0]
    slabs = tokens // lane_width
    step = slabs + 8
    long_step = outer + 8
    block = segs * chans
    direct = [1, 2, 4, 6]
    passed = [2, 4, 6]
    s = lax.axis_index("seg")
    h = lax.axis_index("ch")
    side = s // 2
    low = lax.rem(s, 2)
    partner = s + 1 - 2 * low
    tail = segs - 1

    def seg_peer(d):
        return lax.rem(s + d, segs)

    def ch_peer(d):
        return lax.rem(h + d, groups)

    def flipped(at, d):
        for bit in (1, 2, 4):
            if d & bit:
                at = at + bit - 2 * bit * lax.rem(at // bit, 2)
        return at

    def lanes(j):
        return pl.ds(pl.multiple_of(j * lane_width, lane_width), lane_width)

    def tell(semaphore, seg, peer):
        pl.semaphore_signal(semaphore, inc=1, device_id=(seg, peer), device_id_type=MESH)

    def load_kv(at, size, sem):
        part = pl.ds(at, size)
        return (
            pltpu.make_async_copy(key.at[part], keys.at[part], kv_sem.at[sem]),
            pltpu.make_async_copy(value.at[part], values.at[part], kv_sem.at[sem]),
        )

    seq = list(range(alone, chunks)) + list(range(alone))
    stages = [(seq[0], 1, 0), (0, 1, 1), (1, alone - 1, 2)]
    for copy in [*load_kv(*stages[0]), *load_kv(*stages[1])]:
        copy.start()
    barrier = pltpu.get_barrier_semaphore()

    @pl.when(side == 0)
    def _():
        tell(barrier, 2, h)
        tell(barrier, 3, h)

    @pl.when(s == 2)
    def _():
        for seg in (1, 0, 3):
            tell(barrier, seg, h)

    for d in range(1, groups):
        tell(barrier, s, ch_peer(d))

    def part_of(peer):
        return pl.ds(pl.multiple_of(peer * share, lane_width), share)

    whole_in = (first_in, last_in, inner_in, inner_back_in, cos_in, sin_in, skip_in)
    whole_here = (first, last, inner, inner_back, cos_t, sin_t, skip)
    moves = list(zip(whole_in, whole_here)) + [
        (kernel.at[pl.ds(0, alone), s], taps.at[pl.ds(0, alone)]),
        (gate.at[:, :, :, part_of(h)], gates.at[h]),
        (weight, weights.at[h]),
    ]
    for p in range(pairs):
        moves.append((kernel.at[alone + p, pl.ds(2 * low, 2)], taps.at[pl.ds(alone + 2 * p, 2)]))
    loads = [pltpu.make_async_copy(a, b, here_sem) for a, b in moves]

    def remote(source, target, recv, seg, peer):
        return pltpu.make_async_remote_copy(
            src_ref=source, dst_ref=target, send_sem=sent, recv_sem=recv,
            device_id=(seg, peer), device_id_type=MESH,
        )

    def bulk(ref, recv):
        return remote(ref, ref, recv, partner, h)

    def send_in(k, seg):
        return remote(mixed_out.at[k, seg], mixed_in.at[k, s], in_recv.at[k], seg, h)

    def send_pair(p, seg):
        source = mixed_out.at[alone + p, pl.ds(2 * lax.rem(seg, 2), 2)]
        return remote(source, pair_in.at[p, s], pair_recv.at[p], seg, h)

    def send_gate(d):
        peer = ch_peer(d)
        return remote(gate.at[:, :, :, part_of(peer)], gates.at[h], g_recv, s, peer)

    def send_weight(d):
        return remote(weight, weights.at[h], w_recv.at[0], s, flipped(h, d))

    def pass_weight(d):
        owner = flipped(h, d)
        return remote(weights.at[owner], weights.at[owner], w_recv.at[1], s, flipped(h, 1))

    def mix_part(k, seg):
        def mix(j, carry):
            both = keys[k, seg, :, lanes(j)].astype(f32) * values[k, seg, :, lanes(j)].astype(f32)
            wide[pl.ds(j, chans, stride=step), :] = both
            return carry

        lax.fori_loop(0, slabs, mix, 0, unroll=4)
        for i in range(chans):
            mixed_out[k, seg, i] = wide[i * step : i * step + slabs, :].astype(bf16)

    def cross(k):
        @pl.when(side == 0)
        def _():
            if k >= alone:
                send_pair(k - alone, 2).start()
            else:
                send_in(k, 2).start()

        @pl.when(side == 1)
        def _():
            if k < alone:
                send_in(k, 0).start()
                send_in(k, 1).start()

    def spread_rest(k):
        @pl.when(side == 0)
        def _():
            if k < alone:
                send_in(k, 3).start()
            else:
                send_pair(k - alone, 3).start()

        if k < alone:
            send_in(k, partner).start()
        else:
            send_pair(k - alone, partner).start()

    for n, k in enumerate(seq):
        if n < len(stages):
            for copy in load_kv(*stages[n]):
                copy.wait()
        if n == 0:
            mix_part(k, 0)
            mix_part(k, 1)

            @pl.when(side == 0)
            def _():
                pl.semaphore_wait(barrier, groups)
                send_pair(0, 2).start()

            @pl.when(s == 2)
            def _():
                pl.semaphore_wait(barrier, groups + 1)

            @pl.when(s == tail)
            def _():
                pl.semaphore_wait(barrier, groups + 2)
                for seg in (2, 1, 0):
                    tell(joined, seg, h)

            for copy in load_kv(*stages[2]):
                copy.start()
            mix_part(k, 2)
            mix_part(k, 3)
            for d in range(1, groups):
                send_gate(d).start()
        else:
            for seg in (2, 3, 0, 1):
                mix_part(k, seg)
            cross(k)
        if n == 1:
            for copy in loads:
                copy.start()
        if n == 2:

            @pl.when(s != tail)
            def _():
                pl.semaphore_wait(joined, 1)

            for d in range(1, segs):
                tell(ready, seg_peer(d), h)
            for e in seq[:n]:
                spread_rest(e)
        if n >= 2:
            spread_rest(k)
        if k < alone:
            mixed_in[k, s] = mixed_out[k, s]
        else:
            for e in range(2):
                pair_in[k - alone, s, e] = mixed_out[k, 2 * low + e]

            @pl.when(side == 0)
            def _():
                for seg in (2, 3):
                    pair_in[k - alone, seg] = jnp.zeros((2, chans, slabs, lane_width), bf16)

    for d in direct:
        send_weight(d).start()

    for copy in loads:
        copy.wait()
    for k in [*range(alone, alone + 2 * pairs), *range(alone)]:

        def spread(j, carry):
            tall[pl.ds(j, chans, stride=long_step), :] = taps[k, :, lanes(j)]
            return carry

        lax.fori_loop(0, outer, spread, 0, unroll=4)
        signal = [tall[i * long_step : i * long_step + outer, :].astype(bf16) for i in range(chans)]
        out = forward(signal, first[...], inner[...], cos_t[...], sin_t[...])
        spectrum[k] = out.astype(bf16).reshape(chans, outer, 2 * lane_width)
    pl.semaphore_wait(ready, segs - 1)

    def slot(k, q):
        return chunks - 1 + q if k == alone - 1 else k if k < alone else k - 1

    def convolve_rows(at, rows_of, row):
        signal = [rows_of(i).reshape(outer, lane_width) for i in range(chans)]
        filt = spectrum[at].reshape(chans * outer, 2 * lane_width)
        tables = (first[...], last[...], inner[...], inner_back[...], cos_t[...], sin_t[...])
        parts = convolve_block(tables, signal, filt)
        for i in range(chans):
            long[i * long_step : i * long_step + outer, :] = parts[i] + skip[row + i] * signal[i].astype(f32)

    for p in range(pairs):
        k = alone + p

        @pl.when(side == 0)
        def _():
            bulk(pair_in.at[p, 0], pair_recv.at[p]).wait_recv()

        @pl.when(side == 1)
        def _():
            bulk(pair_in.at[p, pl.ds(0, segs - 1)], pair_recv.at[p]).wait_recv()

        for e in range(2):
            convolve_rows(k + p + e, lambda i: pair_in[p, :, e, i], (k * segs + 2 * low + e) * chans)

            def gather(j, carry):
                from_row = side * (outer // 2) + j
                pair_out[p, e, j] = long[pl.ds(from_row, chans, stride=long_step), :].astype(bf16)
                return carry

            lax.fori_loop(0, outer // 2, gather, 0, unroll=8)
        for d in range(2):
            seg = s if d else partner

            def send(e, carry):
                peer = ch_peer(groups - 1 - e)
                rows = pl.ds(lax.rem(seg, 2) * slabs + peer * quads, quads)
                target = conv_in.at[k, h, pl.ds(2 * low, 2)]
                remote(pair_out.at[p, :, rows], target, out_recv.at[slot(k, 0)], seg, peer).start()
                return carry

            lax.fori_loop(0, groups - d, send, 0)
        for e in range(2):
            for q in range(quads):
                conv_in[k, h, 2 * low + e, q] = pair_out[p, e, low * slabs + h * quads + q]

    for k in range(alone):
        bulk(mixed_in.at[k, pl.ds(0, segs - 1)], in_recv.at[k]).wait_recv()
        convolve_rows(k, lambda i: mixed_in[k, :, i], (k * segs + s) * chans)

        def gather(j, carry):
            conv_out[k, j] = long[pl.ds(j, chans, stride=long_step), :].astype(bf16)
            return carry

        lax.fori_loop(0, outer, gather, 0, unroll=8)
        size = 1 if k == alone - 1 else quads
        for q in range(0, quads, size):
            for d in (2, 3, 1, 0):
                seg = seg_peer(d)

                def send(e, carry):
                    peer = ch_peer(groups - 1 - e)
                    source = conv_out.at[k, pl.ds(seg * slabs + peer * quads + q, size)]
                    target = conv_in.at[k, h, s, pl.ds(q, size)]
                    remote(source, target, out_recv.at[slot(k, q)], seg, peer).start()
                    return carry

                lax.fori_loop(0, groups if d else groups - 1, send, 0)
        for q in range(quads):
            conv_in[k, h, s, q] = conv_out[k, s * slabs + h * quads + q]

    bulk(weights.at[pl.ds(0, len(direct))], w_recv.at[0]).wait_recv()
    for d in passed:
        pass_weight(d).start()
    bulk(gates.at[pl.ds(0, groups - 1)], g_recv).wait_recv()
    bulk(weights.at[pl.ds(0, len(passed))], w_recv.at[1]).wait_recv()
    for k in range(chunks):

        def restack(g, carry):
            for at in range(0, segs, 2):
                pair = [weights[g, k, at + e].astype(f32) for e in range(2)]
                rows = pl.ds(pl.multiple_of(g * block + at * chans, 2 * chans), 2 * chans)
                stacked[k, rows, :] = jnp.concatenate(pair, axis=0).astype(bf16)
            return carry

        lax.fori_loop(0, groups, restack, 0)

    def all_pieces(k, q, size):
        if k < alone:
            ref = conv_out.at[k, pl.ds(0, (segs * groups - 1) * size)]
        else:
            ref = pair_out.at[k - alone, :, pl.ds(0, outer // 2 - quads)]
        return bulk(ref, out_recv.at[slot(k, q)])

    order = list(range(alone, chunks)) + list(range(alone))
    steps = [(k, 0, quads) for k in order[:-1]] + [(order[-1], q, 1) for q in range(quads)]
    for k, start, size in steps:
        all_pieces(k, start, size).wait_recv()

        def combine(g, carry):
            for at in range(0, segs, 2):
                for q in range(start, start + size):
                    both = [
                        conv_in[k, g, at + e, q].astype(f32)
                        * gates[g, k, at + e, :, q * lane_width : (q + 1) * lane_width].astype(f32)
                        for e in range(2)
                    ]
                    rows = pl.ds(pl.multiple_of(g * block + at * chans, 2 * chans), 2 * chans)
                    gated[rows, q * lane_width : (q + 1) * lane_width] = jnp.concatenate(both, axis=0).astype(bf16)
            return carry

        lax.fori_loop(0, groups, combine, 0, unroll=2)
        tokens_at = slice(start * lane_width, (start + size) * lane_width)
        left = gated[:, tokens_at]
        for n in range(features // cols):
            at = slice(n * cols, (n + 1) * cols)
            prod = lax.dot_general(
                left, stacked[k, :, at], (((0,), (0,)), ((), ())), preferred_element_type=f32
            )
            if k == order[0]:
                total[:, at] = prod
            elif k != order[-1]:
                total[:, at] += prod
            else:
                output[tokens_at, at] = (total[tokens_at, at] + prod).astype(bf16)

    bulk(mixed_in.at[:, pl.ds(0, segs - 1)], g_recv).wait_send()
    for p in range(pairs):

        @pl.when(side == 0)
        def _():
            bulk(pair_in.at[p, pl.ds(0, segs - 1)], g_recv).wait_send()

        @pl.when(side == 1)
        def _():
            bulk(pair_in.at[p, 0], g_recv).wait_send()

    bulk(gates.at[pl.ds(0, groups - 1)], g_recv).wait_send()
    bulk(weights.at[pl.ds(0, groups - 1)], g_recv).wait_send()
    for k, start, size in steps:
        all_pieces(k, start, size).wait_send()


def whole_layer(gate_in, key_in, value_in, kernel, skip_gain, out_weight, chans):
    segs, groups = lax.axis_size("seg"), lax.axis_size("ch")
    channels, tokens = key_in.shape
    full_len = kernel.shape[1]
    outer = full_len // lane_width
    slabs = tokens // lane_width
    features = out_weight.shape[1]
    chunks = channels // segs // chans
    pairs = 1
    alone = chunks - pairs
    share = tokens // groups
    quads = share // lane_width
    tables = make_tables(outer)
    split = (chunks, segs, chans)
    args = (
        *tables,
        skip_gain,
        key_in.reshape(*split, tokens),
        value_in.reshape(*split, tokens),
        gate_in.reshape(*split, tokens),
        kernel.reshape(*split, full_len),
        out_weight.reshape(*split, features),
    )
    hbm = pl.BlockSpec(memory_space=pltpu.HBM)
    dma = pltpu.SemaphoreType.DMA
    regular = pltpu.SemaphoreType.REGULAR
    tall = pltpu.VMEM((chans * (outer + 8), lane_width), f32)
    return pl.pallas_call(
        layer_kernel,
        in_specs=[hbm] * len(args),
        out_specs=pl.BlockSpec(memory_space=pltpu.VMEM),
        out_shape=pltpu.VMEM((share, features), bf16),
        scratch_shapes=[pltpu.VMEM(a.shape, a.dtype) for a in tables]
        + [
            pltpu.SMEM(skip_gain.shape, f32),
            pltpu.VMEM((*split, tokens), bf16),
            pltpu.VMEM((*split, tokens), bf16),
            pltpu.VMEM((alone + 2 * pairs, chans, full_len), f32),
            tall,
            pltpu.VMEM((chans * (slabs + 8), lane_width), f32),
            tall,
            pltpu.VMEM((alone + 2 * pairs, chans, outer, 2 * lane_width), bf16),
            pltpu.VMEM((*split, slabs, lane_width), bf16),
            pltpu.VMEM((alone, segs, chans, slabs, lane_width), bf16),
            pltpu.VMEM((pairs, segs, 2, chans, slabs, lane_width), bf16),
            pltpu.VMEM((alone, outer, chans, lane_width), bf16),
            pltpu.VMEM((pairs, 2, outer // 2, chans, lane_width), bf16),
            pltpu.VMEM((chunks, groups, segs, quads, chans, lane_width), bf16),
            pltpu.VMEM((groups, *split, share), bf16),
            pltpu.VMEM((groups, *split, features), bf16),
            pltpu.VMEM((chunks, groups * segs * chans, features), bf16),
            pltpu.VMEM((groups * segs * chans, share), bf16),
            pltpu.VMEM((share, features), f32),
            dma((3,)), dma, regular, regular, dma, dma((alone,)), dma((pairs,)), dma((chunks - 1 + quads,)), dma, dma((2,)),
        ],
        compiler_params=pltpu.CompilerParams(
            collective_id=0, has_side_effects=True, vmem_limit_bytes=56 * 1024 * 1024
        ),
        name="layer",
    )(*args)


def on_device(gate_in, key_in, value_in, kernel, skip_gain, out_weight):
    seg_count = lax.axis_size("seg")
    seg_index = lax.axis_index("seg")
    channels, tokens = key_in.shape
    full_len = kernel.shape[1]
    outer = full_len // lane_width
    tables = make_tables(outer)
    col_count = channels // seg_count
    sublanes = 8
    fits = (seg_count, lax.axis_size("ch")) == (4, 8) and col_count % sublanes == 0 and col_count > sublanes
    if fits and tokens // lax.axis_size("ch") % lane_width == 0:
        return whole_layer(gate_in, key_in, value_in, kernel, skip_gain, out_weight, sublanes)
    mixed = key_in.astype(f32) * value_in.astype(f32)
    mixed_sent = mixed.astype(bf16).reshape(channels, tokens // lane_width, lane_width)
    col_mixed = lax.all_to_all(mixed_sent, "seg", split_axis=0, concat_axis=1, tiled=True)
    taps = lax.dynamic_slice_in_dim(kernel, seg_index * col_count, col_count, 0)
    spectrum = transform_filter(tables, taps.astype(bf16).reshape(col_count, outer, lane_width))
    col_conv = convolve(tables, col_mixed, spectrum)
    conv = lax.all_to_all(col_conv, "seg", split_axis=1, concat_axis=0, tiled=True)
    conv = conv.reshape(channels, tokens).astype(f32)
    gated = (gate_in.astype(f32) * (conv + skip_gain[:, None] * mixed)).astype(bf16)
    mine = lax.all_to_all(gated, "ch", split_axis=1, concat_axis=0, tiled=True)
    weight = lax.all_gather(out_weight, "ch", axis=0, tiled=True)
    result = lax.dot_general(
        mine, weight, (((0,), (0,)), ((), ())), preferred_element_type=f32
    )
    return result.astype(bf16)


def solution(mesh):
    placed = (P("ch", "seg"), P("ch", "seg"), P("ch", "seg"), P("ch", None), P("ch"), P("ch", None))
    return jax.shard_map(
        on_device, mesh=mesh, in_specs=placed, out_specs=P(("seg", "ch"), None), check_vma=False
    )
```

```python
import functools
import math

import jax
import jax.numpy as jnp
import numpy as np
from jax import lax
from jax.experimental import pallas as pl
from jax.experimental.pallas import tpu as pltpu
from jax.sharding import PartitionSpec as P

lane_width = 128
bf16 = jnp.bfloat16
f32 = jnp.float32


def angles(rows, cols, period):
    theta = (rows[:, None] * cols[None, :] % (4 * period)) * (2.0 * math.pi / (4 * period))
    return np.cos(theta), np.sin(theta)


def make_tables(outer):
    quarter = 4 * np.arange(outer) + 1
    row = np.arange(outer)
    lane = np.arange(lane_width)
    cos_o, sin_o = angles(quarter, row, outer)
    cos_t, sin_t = angles(quarter, lane, outer * lane_width)
    cos_i, sin_i = angles(4 * lane, lane, lane_width)
    first = np.concatenate([cos_o, -sin_o], axis=0)
    last = np.concatenate([cos_o.T, -sin_o.T], axis=1) / (outer * lane_width)
    inner = np.block([[cos_i, -sin_i], [sin_i, cos_i]])
    inner_back = np.block([[cos_i, sin_i], [-sin_i, cos_i]])
    narrow = [jnp.asarray(m.astype(np.float32).astype(bf16)) for m in (first, last, inner, inner_back)]
    return (*narrow, jnp.asarray(cos_t.astype(np.float32)), jnp.asarray(sin_t.astype(np.float32)))


def forward(signal, first, inner, cos_t, sin_t):
    outer = cos_t.shape[0]
    rows = []
    for at in range(0, len(signal), 2):
        pair = signal[at : at + 2]
        wide = jnp.dot(first, jnp.concatenate(pair, axis=1), preferred_element_type=f32)
        for i in range(len(pair)):
            part = wide[:, i * lane_width : (i + 1) * lane_width]
            real, imag = part[:outer], part[outer:]
            rows.append(
                jnp.concatenate(
                    [
                        (real * cos_t + imag * sin_t).astype(bf16),
                        (imag * cos_t - real * sin_t).astype(bf16),
                    ],
                    axis=1,
                )
            )
    return jnp.dot(jnp.concatenate(rows, axis=0), inner, preferred_element_type=f32)


def filter_kernel(first, inner, cos_t, sin_t, taps, spectrum):
    count, outer = taps.shape[0], taps.shape[1]
    signal = [taps[i].astype(bf16) for i in range(count)]
    out = forward(signal, first[...], inner[...], cos_t[...], sin_t[...])
    spectrum[...] = out.astype(bf16).reshape(count, outer, 2 * lane_width)


def convolve_block(tables, signal, filt):
    first, last, inner, inner_back, cos, sin = tables
    outer = cos.shape[0]
    sig = forward(signal, first, inner, cos, sin)
    filt = filt.astype(f32)
    sig_re, sig_im = sig[:, :lane_width], sig[:, lane_width:]
    filt_re, filt_im = filt[:, :lane_width], filt[:, lane_width:]
    prod = jnp.concatenate(
        [
            (filt_re * sig_re - filt_im * sig_im).astype(bf16),
            (filt_re * sig_im + filt_im * sig_re).astype(bf16),
        ],
        axis=1,
    )
    back = jnp.dot(prod, inner_back, preferred_element_type=f32)
    parts = []
    for at in range(0, len(signal), 2):
        cols = []
        for i in range(at, min(at + 2, len(signal))):
            rows = back[i * outer : (i + 1) * outer]
            real, imag = rows[:, :lane_width], rows[:, lane_width:]
            cols.append(
                jnp.concatenate(
                    [
                        (real * cos - imag * sin).astype(bf16),
                        (imag * cos + real * sin).astype(bf16),
                    ],
                    axis=0,
                )
            )
        wide = jnp.dot(last, jnp.concatenate(cols, axis=1), preferred_element_type=f32)
        for i in range(len(cols)):
            parts.append(wide[:, i * lane_width : (i + 1) * lane_width])
    return parts


def conv_kernel(first, last, inner, inner_back, cos_t, sin_t, mixed, spectrum, conv):
    count, outer = mixed.shape[0], mixed.shape[1]
    tables = (first[...], last[...], inner[...], inner_back[...], cos_t[...], sin_t[...])
    filt = spectrum[...].reshape(count * outer, 2 * lane_width)
    parts = convolve_block(tables, [mixed[i] for i in range(count)], filt)
    for i in range(count):
        conv[i] = parts[i].astype(bf16)


def whole(array):
    return pl.BlockSpec(array.shape, lambda i: (0,) * array.ndim)


def block_of(count):
    return max(b for b in range(1, 9) if count % b == 0)


def transform_filter(tables, taps):
    first, last, inner, inner_back, cos_t, sin_t = tables
    count, outer, lanes = taps.shape
    block = block_of(count)
    fixed = (first, inner, cos_t, sin_t)
    return pl.pallas_call(
        filter_kernel,
        grid=(count // block,),
        in_specs=[whole(a) for a in fixed] + [pl.BlockSpec((block, outer, lanes), lambda i: (i, 0, 0))],
        out_specs=pl.BlockSpec((block, outer, 2 * lanes), lambda i: (i, 0, 0)),
        out_shape=jax.ShapeDtypeStruct((count, outer, 2 * lanes), bf16),
        cost_estimate=pl.CostEstimate(
            flops=count * outer * lanes * 1536, bytes_accessed=count * outer * lanes * 8, transcendentals=0
        ),
        name="filter_transform",
    )(*fixed, taps)


def convolve(tables, mixed, spectrum):
    count, outer, lanes = mixed.shape
    block = block_of(count)
    return pl.pallas_call(
        conv_kernel,
        grid=(count // block,),
        in_specs=[whole(a) for a in tables]
        + [
            pl.BlockSpec((block, outer, lanes), lambda i: (i, 0, 0)),
            pl.BlockSpec((block, outer, 2 * lanes), lambda i: (i, 0, 0)),
        ],
        out_specs=pl.BlockSpec((block, outer, lanes), lambda i: (i, 0, 0)),
        out_shape=jax.ShapeDtypeStruct((count, outer, lanes), bf16),
        cost_estimate=pl.CostEstimate(
            flops=count * outer * lanes * 3072, bytes_accessed=count * outer * lanes * 8, transcendentals=0
        ),
        name="convolve",
    )(*tables, mixed, spectrum)


MESH = pl.DeviceIdType.MESH


def layer_kernel(
    first_in, last_in, inner_in, inner_back_in, cos_in, sin_in, skip_in, key, value, gate, kernel, weight,
    result, rest, ending, ending_weight,
    first, last, inner, inner_back, cos_t, sin_t, skip, keys, values, taps, tall, wide, long,
    spectrum, mixed_out, mixed_in, pair_in, conv_out, pair_out, conv_in, gates, weights, stacked, gated, total,
    kv_sem, here_sem, joined, ready, plane, released, sent, in_recv, pair_recv, out_recv, g_recv, w_recv,
):
    chunks, segs, chans, tokens = key.shape
    groups = gates.shape[0]
    pairs = pair_in.shape[0]
    alone = chunks - pairs
    share = tokens // groups
    quads = share // lane_width
    features = weight.shape[-1]
    cols = 512 if features % 512 == 0 else features
    outer = cos_t.shape[0]
    slabs = tokens // lane_width
    step = slabs + 8
    long_step = outer + 8
    block = segs * chans
    direct = [1, 2, 4, 6]
    passed = [2, 4, 6]
    s = lax.axis_index("seg")
    h = lax.axis_index("ch")
    side = s // 2
    low = lax.rem(s, 2)
    partner = s + 1 - 2 * low
    tail = segs - 1

    def seg_peer(d):
        return lax.rem(s + d, segs)

    def ch_peer(d):
        return lax.rem(h + d, groups)

    def flipped(at, d):
        for bit in (1, 2, 4):
            if d & bit:
                at = at + bit - 2 * bit * lax.rem(at // bit, 2)
        return at

    def lanes(j):
        return pl.ds(pl.multiple_of(j * lane_width, lane_width), lane_width)

    def tell(semaphore, seg, peer):
        pl.semaphore_signal(semaphore, inc=1, device_id=(seg, peer), device_id_type=MESH)

    def load_kv(at, size, sem):
        part = pl.ds(at, size)
        return (
            pltpu.make_async_copy(key.at[part], keys.at[part], kv_sem.at[sem]),
            pltpu.make_async_copy(value.at[part], values.at[part], kv_sem.at[sem]),
        )

    seq = list(range(alone, chunks)) + list(range(alone))
    stages = [(seq[0], 1, 0), (0, 1, 1), (1, alone - 1, 2)]
    barrier = pltpu.get_barrier_semaphore()

    @pl.when(s == 2)
    def _():
        for seg in (1, 0, 3):
            tell(barrier, seg, h)

    for copy in [*load_kv(*stages[0]), *load_kv(*stages[1])]:
        copy.start()

    @pl.when(side == 0)
    def _():
        tell(barrier, 2, h)
        tell(barrier, 3, h)

    @pl.when(s == 1)
    def _():
        tell(barrier, 0, h)

    @pl.when(s != 1)
    def _():
        for d in range(1, groups):
            tell(barrier, s, ch_peer(d))

    def part_of(peer):
        return pl.ds(pl.multiple_of(peer * share, lane_width), share)

    whole_in = (first_in, last_in, inner_in, inner_back_in, cos_in, sin_in, skip_in)
    whole_here = (first, last, inner, inner_back, cos_t, sin_t, skip)
    moves = list(zip(whole_in, whole_here)) + [
        (kernel.at[pl.ds(0, alone), s], taps.at[pl.ds(0, alone)]),
        (gate.at[:, :, :, part_of(h)], gates.at[h]),
        (weight, weights.at[h]),
    ]
    for p in range(pairs):
        moves.append((kernel.at[alone + p, pl.ds(2 * low, 2)], taps.at[pl.ds(alone + 2 * p, 2)]))
    loads = [pltpu.make_async_copy(a, b, here_sem) for a, b in moves]

    def remote(source, target, recv, seg, peer):
        return pltpu.make_async_remote_copy(
            src_ref=source, dst_ref=target, send_sem=sent, recv_sem=recv,
            device_id=(seg, peer), device_id_type=MESH,
        )

    def bulk(ref, recv):
        return remote(ref, ref, recv, partner, h)

    def send_in(k, seg):
        return remote(mixed_out.at[k, seg], mixed_in.at[k, s], in_recv.at[k], seg, h)

    def send_pair(p, seg):
        source = mixed_out.at[alone + p, pl.ds(2 * lax.rem(seg, 2), 2)]
        return remote(source, pair_in.at[p, s], pair_recv.at[p], seg, h)

    def send_gate(d):
        peer = ch_peer(d)
        return remote(gate.at[:, :, :, part_of(peer)], gates.at[h], g_recv, s, peer)

    def send_weight(d):
        return remote(weight, weights.at[h], w_recv.at[0], s, flipped(h, d))

    def pass_weight(d):
        owner = flipped(h, d)
        return remote(weights.at[owner], weights.at[owner], w_recv.at[1], s, flipped(h, 1))

    def mix_part(k, seg):
        def mix(j, carry):
            both = keys[k, seg, :, lanes(j)].astype(f32) * values[k, seg, :, lanes(j)].astype(f32)
            wide[pl.ds(j, chans, stride=step), :] = both
            return carry

        lax.fori_loop(0, slabs, mix, 0, unroll=4)
        for i in range(chans):
            mixed_out[k, seg, i] = wide[i * step : i * step + slabs, :].astype(bf16)

    def cross(k):
        @pl.when(side == 0)
        def _():
            if k >= alone:
                send_pair(k - alone, 2).start()
            else:
                send_in(k, 2).start()

        @pl.when(side == 1)
        def _():
            if k < alone:
                send_in(k, 0).start()
                send_in(k, 1).start()

    def spread_rest(k):
        @pl.when(side == 0)
        def _():
            if k < alone:
                send_in(k, 3).start()
            else:
                send_pair(k - alone, 3).start()

        if k < alone:
            send_in(k, partner).start()
        else:
            send_pair(k - alone, partner).start()

    for n, k in enumerate(seq):
        if n < len(stages):
            for copy in load_kv(*stages[n]):
                copy.wait()
        if n == 0:
            mix_part(k, 0)
            mix_part(k, 1)

            @pl.when(s == 1)
            def _():
                pl.semaphore_wait(barrier, 1)
                send_pair(0, 2).start()

            @pl.when(s == 0)
            def _():
                pl.semaphore_wait(barrier, groups + 1)
                send_pair(0, 2).start()
                for d in range(1, groups):
                    tell(plane, s, ch_peer(d))

            @pl.when(s == 2)
            def _():
                pl.semaphore_wait(barrier, groups + 1)

            @pl.when(s == tail)
            def _():
                pl.semaphore_wait(barrier, groups + 2)
                for seg in (2, 1, 0):
                    tell(joined, seg, h)

            for copy in load_kv(*stages[2]):
                copy.start()
            mix_part(k, 2)
            mix_part(k, 3)

            @pl.when(s != 1)
            def _():
                for d in range(1, groups):
                    send_gate(d).start()
        else:
            for seg in (2, 3, 0, 1):
                mix_part(k, seg)
            cross(k)
        if n == 1:
            for copy in loads:
                copy.start()
        if n == 2:

            @pl.when(s == 0)
            def _():
                pl.semaphore_wait(plane, groups - 1)
                tell(released, 1, h)

            @pl.when(s != tail)
            def _():
                pl.semaphore_wait(joined, 1)

            @pl.when(s != 1)
            def _():
                for d in range(1, segs):
                    tell(ready, seg_peer(d), h)

            for e in seq[:n]:
                spread_rest(e)
        if n >= 2:
            spread_rest(k)
        if n == 3:

            @pl.when(s == 1)
            def _():
                pl.semaphore_wait(released, 1)
                for d in range(1, segs):
                    tell(ready, seg_peer(d), h)
                for d in range(1, groups):
                    send_gate(d).start()

        if k < alone:
            mixed_in[k, s] = mixed_out[k, s]
        else:
            for e in range(2):
                pair_in[k - alone, s, e] = mixed_out[k, 2 * low + e]

            @pl.when(side == 0)
            def _():
                for seg in (2, 3):
                    pair_in[k - alone, seg] = jnp.zeros((2, chans, slabs, lane_width), bf16)

    for d in direct:
        send_weight(d).start()

    for copy in loads:
        copy.wait()
    for k in [*range(alone, alone + 2 * pairs), *range(alone)]:

        def spread(j, carry):
            tall[pl.ds(j, chans, stride=long_step), :] = taps[k, :, lanes(j)]
            return carry

        lax.fori_loop(0, outer, spread, 0, unroll=4)
        signal = [tall[i * long_step : i * long_step + outer, :].astype(bf16) for i in range(chans)]
        out = forward(signal, first[...], inner[...], cos_t[...], sin_t[...])
        spectrum[k] = out.astype(bf16).reshape(chans, outer, 2 * lane_width)
    pl.semaphore_wait(ready, segs - 1)

    def slot(k, q):
        return chunks - 1 + q if k == alone - 1 else k if k < alone else k - 1

    def convolve_rows(at, rows_of, row):
        signal = [rows_of(i).reshape(outer, lane_width) for i in range(chans)]
        filt = spectrum[at].reshape(chans * outer, 2 * lane_width)
        tables = (first[...], last[...], inner[...], inner_back[...], cos_t[...], sin_t[...])
        parts = convolve_block(tables, signal, filt)
        for i in range(chans):
            long[i * long_step : i * long_step + outer, :] = parts[i] + skip[row + i] * signal[i].astype(f32)

    for p in range(pairs):
        k = alone + p

        @pl.when(side == 0)
        def _():
            bulk(pair_in.at[p, 0], pair_recv.at[p]).wait_recv()

        @pl.when(side == 1)
        def _():
            bulk(pair_in.at[p, pl.ds(0, segs - 1)], pair_recv.at[p]).wait_recv()

        for e in range(2):
            convolve_rows(k + p + e, lambda i: pair_in[p, :, e, i], (k * segs + 2 * low + e) * chans)

            def gather(j, carry):
                from_row = side * (outer // 2) + j
                pair_out[p, e, j] = long[pl.ds(from_row, chans, stride=long_step), :].astype(bf16)
                return carry

            lax.fori_loop(0, outer // 2, gather, 0, unroll=8)
        for d in range(2):
            seg = s if d else partner

            def send(e, carry):
                peer = ch_peer(groups - 1 - e)
                rows = pl.ds(lax.rem(seg, 2) * slabs + peer * quads, quads)
                target = conv_in.at[k, h, pl.ds(2 * low, 2)]
                remote(pair_out.at[p, :, rows], target, out_recv.at[slot(k, 0)], seg, peer).start()
                return carry

            lax.fori_loop(0, groups - d, send, 0)
        for e in range(2):
            for q in range(quads):
                conv_in[k, h, 2 * low + e, q] = pair_out[p, e, low * slabs + h * quads + q]

    for k in range(alone):
        bulk(mixed_in.at[k, pl.ds(0, segs - 1)], in_recv.at[k]).wait_recv()
        convolve_rows(k, lambda i: mixed_in[k, :, i], (k * segs + s) * chans)

        def gather(j, carry):
            conv_out[k, j] = long[pl.ds(j, chans, stride=long_step), :].astype(bf16)
            return carry

        lax.fori_loop(0, outer, gather, 0, unroll=8)
        size = 1 if k == alone - 1 else quads
        for q in range(0, quads, size):
            for d in (2, 3, 1, 0):
                seg = seg_peer(d)

                def send(e, carry):
                    peer = ch_peer(groups - 1 - e)
                    source = conv_out.at[k, pl.ds(seg * slabs + peer * quads + q, size)]
                    target = conv_in.at[k, h, s, pl.ds(q, size)]
                    remote(source, target, out_recv.at[slot(k, q)], seg, peer).start()
                    return carry

                lax.fori_loop(0, groups if d else groups - 1, send, 0)
        for q in range(quads):
            conv_in[k, h, s, q] = conv_out[k, s * slabs + h * quads + q]

    bulk(weights.at[pl.ds(0, len(direct))], w_recv.at[0]).wait_recv()
    for d in passed:
        pass_weight(d).start()
    bulk(gates.at[pl.ds(0, groups - 1)], g_recv).wait_recv()
    bulk(weights.at[pl.ds(0, len(passed))], w_recv.at[1]).wait_recv()
    order = list(range(alone, chunks)) + list(range(alone))
    for at, k in enumerate(order):
        into = ending_weight if k == order[-1] else stacked.at[at]

        def restack(g, carry):
            for at in range(0, segs, 2):
                pair = [weights[g, k, at + e].astype(f32) for e in range(2)]
                rows = pl.ds(pl.multiple_of(g * block + at * chans, 2 * chans), 2 * chans)
                into[rows, :] = jnp.concatenate(pair, axis=0).astype(bf16)
            return carry

        lax.fori_loop(0, groups, restack, 0)

    def all_pieces(k, q, size):
        if k < alone:
            ref = conv_out.at[k, pl.ds(0, (segs * groups - 1) * size)]
        else:
            ref = pair_out.at[k - alone, :, pl.ds(0, outer // 2 - quads)]
        return bulk(ref, out_recv.at[slot(k, q)])

    steps = [(k, 0, quads) for k in order[:-1]] + [(order[-1], q, 1) for q in range(quads)]
    for n, (k, start, size) in enumerate(steps):
        all_pieces(k, start, size).wait_recv()
        ends = n == len(steps) - 1
        into = ending if ends else gated
        shift = start if ends else 0
        weight_of = ending_weight if k == order[-1] else stacked.at[n]

        def combine(g, carry):
            for at in range(0, segs, 2):
                for q in range(start, start + size):
                    both = [
                        conv_in[k, g, at + e, q].astype(f32)
                        * gates[g, k, at + e, :, q * lane_width : (q + 1) * lane_width].astype(f32)
                        for e in range(2)
                    ]
                    rows = pl.ds(pl.multiple_of(g * block + at * chans, 2 * chans), 2 * chans)
                    at_q = slice((q - shift) * lane_width, (q - shift + 1) * lane_width)
                    into[rows, at_q] = jnp.concatenate(both, axis=0).astype(bf16)
            return carry

        lax.fori_loop(0, groups, combine, 0, unroll=2)
        if ends:
            continue
        tokens_at = slice(start * lane_width, (start + size) * lane_width)
        left = gated[:, tokens_at]
        for c in range(features // cols):
            at = slice(c * cols, (c + 1) * cols)
            prod = lax.dot_general(
                left, weight_of[:, at], (((0,), (0,)), ((), ())), preferred_element_type=f32
            )
            if k == order[0]:
                total[:, at] = prod
            elif k == order[-1]:
                result[tokens_at, at] = (total[tokens_at, at] + prod).astype(bf16)
            elif k != order[-2]:
                total[:, at] += prod
            else:
                early = result.shape[0]
                total[:, at] += prod
                rest[:, at] = total[early:, at]

    bulk(mixed_in.at[:, pl.ds(0, segs - 1)], g_recv).wait_send()
    for p in range(pairs):

        @pl.when(side == 0)
        def _():
            bulk(pair_in.at[p, pl.ds(0, segs - 1)], g_recv).wait_send()

        @pl.when(side == 1)
        def _():
            bulk(pair_in.at[p, 0], g_recv).wait_send()

    bulk(gates.at[pl.ds(0, groups - 1)], g_recv).wait_send()
    bulk(weights.at[pl.ds(0, groups - 1)], g_recv).wait_send()
    for k, start, size in steps:
        all_pieces(k, start, size).wait_send()


def finish_kernel(result, rest, ending, ending_weight, output, final, sem):
    early = result.shape[0]
    copies = [pltpu.make_async_copy(result, output.at[pl.ds(0, early)], sem.at[0])]
    copies[0].start()
    prod = lax.dot_general(
        ending[...], ending_weight[...], (((0,), (0,)), ((), ())), preferred_element_type=f32
    )
    final[...] = (rest[...] + prod).astype(bf16)
    copies.append(pltpu.make_async_copy(final, output.at[pl.ds(early, final.shape[0])], sem.at[1]))
    copies[1].start()
    for copy in copies:
        copy.wait()


def whole_layer(gate_in, key_in, value_in, kernel, skip_gain, out_weight, chans):
    segs, groups = lax.axis_size("seg"), lax.axis_size("ch")
    channels, tokens = key_in.shape
    full_len = kernel.shape[1]
    outer = full_len // lane_width
    slabs = tokens // lane_width
    features = out_weight.shape[1]
    chunks = channels // segs // chans
    pairs = 1
    alone = chunks - pairs
    share = tokens // groups
    quads = share // lane_width
    tables = make_tables(outer)
    split = (chunks, segs, chans)
    args = (
        *tables,
        skip_gain,
        key_in.reshape(*split, tokens),
        value_in.reshape(*split, tokens),
        gate_in.reshape(*split, tokens),
        kernel.reshape(*split, full_len),
        out_weight.reshape(*split, features),
    )
    hbm = pl.BlockSpec(memory_space=pltpu.HBM)
    dma = pltpu.SemaphoreType.DMA
    regular = pltpu.SemaphoreType.REGULAR
    tall = pltpu.VMEM((chans * (outer + 8), lane_width), f32)
    early = share - lane_width
    vmem = pl.BlockSpec(memory_space=pltpu.VMEM)
    parts = pl.pallas_call(
        layer_kernel,
        in_specs=[hbm] * len(args),
        out_specs=[vmem] * 4,
        out_shape=[
            pltpu.VMEM((early, features), bf16),
            pltpu.VMEM((lane_width, features), f32),
            pltpu.VMEM((groups * segs * chans, lane_width), bf16),
            pltpu.VMEM((groups * segs * chans, features), bf16),
        ],
        scratch_shapes=[pltpu.VMEM(a.shape, a.dtype) for a in tables]
        + [
            pltpu.SMEM(skip_gain.shape, f32),
            pltpu.VMEM((*split, tokens), bf16),
            pltpu.VMEM((*split, tokens), bf16),
            pltpu.VMEM((alone + 2 * pairs, chans, full_len), f32),
            tall,
            pltpu.VMEM((chans * (slabs + 8), lane_width), f32),
            tall,
            pltpu.VMEM((alone + 2 * pairs, chans, outer, 2 * lane_width), bf16),
            pltpu.VMEM((*split, slabs, lane_width), bf16),
            pltpu.VMEM((alone, segs, chans, slabs, lane_width), bf16),
            pltpu.VMEM((pairs, segs, 2, chans, slabs, lane_width), bf16),
            pltpu.VMEM((alone, outer, chans, lane_width), bf16),
            pltpu.VMEM((pairs, 2, outer // 2, chans, lane_width), bf16),
            pltpu.VMEM((chunks, groups, segs, quads, chans, lane_width), bf16),
            pltpu.VMEM((groups, *split, share), bf16),
            pltpu.VMEM((groups, *split, features), bf16),
            pltpu.VMEM((chunks - 1, groups * segs * chans, features), bf16),
            pltpu.VMEM((groups * segs * chans, share), bf16),
            pltpu.VMEM((share, features), f32),
            dma((3,)), dma, regular, regular, regular, regular, dma, dma((alone,)), dma((pairs,)), dma((chunks - 1 + quads,)), dma, dma((2,)),
        ],
        compiler_params=pltpu.CompilerParams(
            collective_id=0, has_side_effects=True, vmem_limit_bytes=56 * 1024 * 1024
        ),
        name="layer",
    )(*args)
    return pl.pallas_call(
        finish_kernel,
        in_specs=[vmem] * 4,
        out_specs=hbm,
        out_shape=jax.ShapeDtypeStruct((share, features), bf16),
        scratch_shapes=[pltpu.VMEM((lane_width, features), bf16), dma((2,))],
        compiler_params=pltpu.CompilerParams(vmem_limit_bytes=4 * 1024 * 1024),
        name="finish",
    )(*parts)


def on_device(gate_in, key_in, value_in, kernel, skip_gain, out_weight):
    seg_count = lax.axis_size("seg")
    seg_index = lax.axis_index("seg")
    channels, tokens = key_in.shape
    full_len = kernel.shape[1]
    outer = full_len // lane_width
    tables = make_tables(outer)
    col_count = channels // seg_count
    sublanes = 8
    fits = (seg_count, lax.axis_size("ch")) == (4, 8) and col_count % sublanes == 0 and col_count > sublanes
    if fits and tokens // lax.axis_size("ch") % lane_width == 0:
        return whole_layer(gate_in, key_in, value_in, kernel, skip_gain, out_weight, sublanes)
    mixed = key_in.astype(f32) * value_in.astype(f32)
    mixed_sent = mixed.astype(bf16).reshape(channels, tokens // lane_width, lane_width)
    col_mixed = lax.all_to_all(mixed_sent, "seg", split_axis=0, concat_axis=1, tiled=True)
    taps = lax.dynamic_slice_in_dim(kernel, seg_index * col_count, col_count, 0)
    spectrum = transform_filter(tables, taps.astype(bf16).reshape(col_count, outer, lane_width))
    col_conv = convolve(tables, col_mixed, spectrum)
    conv = lax.all_to_all(col_conv, "seg", split_axis=1, concat_axis=0, tiled=True)
    conv = conv.reshape(channels, tokens).astype(f32)
    gated = (gate_in.astype(f32) * (conv + skip_gain[:, None] * mixed)).astype(bf16)
    mine = lax.all_to_all(gated, "ch", split_axis=1, concat_axis=0, tiled=True)
    weight = lax.all_gather(out_weight, "ch", axis=0, tiled=True)
    result = lax.dot_general(
        mine, weight, (((0,), (0,)), ((), ())), preferred_element_type=f32
    )
    return result.astype(bf16)


def solution(mesh):
    placed = (P("ch", "seg"), P("ch", "seg"), P("ch", "seg"), P("ch", None), P("ch"), P("ch", None))
    return jax.shard_map(
        on_device, mesh=mesh, in_specs=placed, out_specs=P(("seg", "ch"), None), check_vma=False
    )
```

```python
import functools
import math

import jax
import jax.numpy as jnp
import numpy as np
from jax import lax
from jax.experimental import pallas as pl
from jax.experimental.pallas import tpu as pltpu
from jax.sharding import PartitionSpec as P

lane_width = 128
bf16 = jnp.bfloat16
f32 = jnp.float32


def angles(rows, cols, period):
    theta = (rows[:, None] * cols[None, :] % (4 * period)) * (2.0 * math.pi / (4 * period))
    return np.cos(theta), np.sin(theta)


def make_tables(outer):
    quarter = 4 * np.arange(outer) + 1
    row = np.arange(outer)
    lane = np.arange(lane_width)
    cos_o, sin_o = angles(quarter, row, outer)
    cos_t, sin_t = angles(quarter, lane, outer * lane_width)
    cos_i, sin_i = angles(4 * lane, lane, lane_width)
    first = np.concatenate([cos_o, -sin_o], axis=0)
    last = np.concatenate([cos_o.T, -sin_o.T], axis=1) / (outer * lane_width)
    inner = np.block([[cos_i, -sin_i], [sin_i, cos_i]])
    inner_back = np.block([[cos_i, sin_i], [-sin_i, cos_i]])
    narrow = [jnp.asarray(m.astype(np.float32).astype(bf16)) for m in (first, last, inner, inner_back)]
    return (*narrow, jnp.asarray(cos_t.astype(np.float32)), jnp.asarray(sin_t.astype(np.float32)))


def forward(signal, first, inner, cos_t, sin_t):
    outer = cos_t.shape[0]
    rows = []
    for at in range(0, len(signal), 2):
        pair = signal[at : at + 2]
        wide = jnp.dot(first, jnp.concatenate(pair, axis=1), preferred_element_type=f32)
        for i in range(len(pair)):
            part = wide[:, i * lane_width : (i + 1) * lane_width]
            real, imag = part[:outer], part[outer:]
            rows.append(
                jnp.concatenate(
                    [
                        (real * cos_t + imag * sin_t).astype(bf16),
                        (imag * cos_t - real * sin_t).astype(bf16),
                    ],
                    axis=1,
                )
            )
    return jnp.dot(jnp.concatenate(rows, axis=0), inner, preferred_element_type=f32)


def filter_kernel(first, inner, cos_t, sin_t, taps, spectrum):
    count, outer = taps.shape[0], taps.shape[1]
    signal = [taps[i].astype(bf16) for i in range(count)]
    out = forward(signal, first[...], inner[...], cos_t[...], sin_t[...])
    spectrum[...] = out.astype(bf16).reshape(count, outer, 2 * lane_width)


def convolve_block(tables, signal, filt):
    first, last, inner, inner_back, cos, sin = tables
    outer = cos.shape[0]
    sig = forward(signal, first, inner, cos, sin)
    filt = filt.astype(f32)
    sig_re, sig_im = sig[:, :lane_width], sig[:, lane_width:]
    filt_re, filt_im = filt[:, :lane_width], filt[:, lane_width:]
    prod = jnp.concatenate(
        [
            (filt_re * sig_re - filt_im * sig_im).astype(bf16),
            (filt_re * sig_im + filt_im * sig_re).astype(bf16),
        ],
        axis=1,
    )
    back = jnp.dot(prod, inner_back, preferred_element_type=f32)
    parts = []
    for at in range(0, len(signal), 2):
        cols = []
        for i in range(at, min(at + 2, len(signal))):
            rows = back[i * outer : (i + 1) * outer]
            real, imag = rows[:, :lane_width], rows[:, lane_width:]
            cols.append(
                jnp.concatenate(
                    [
                        (real * cos - imag * sin).astype(bf16),
                        (imag * cos + real * sin).astype(bf16),
                    ],
                    axis=0,
                )
            )
        wide = jnp.dot(last, jnp.concatenate(cols, axis=1), preferred_element_type=f32)
        for i in range(len(cols)):
            parts.append(wide[:, i * lane_width : (i + 1) * lane_width])
    return parts


def conv_kernel(first, last, inner, inner_back, cos_t, sin_t, mixed, spectrum, conv):
    count, outer = mixed.shape[0], mixed.shape[1]
    tables = (first[...], last[...], inner[...], inner_back[...], cos_t[...], sin_t[...])
    filt = spectrum[...].reshape(count * outer, 2 * lane_width)
    parts = convolve_block(tables, [mixed[i] for i in range(count)], filt)
    for i in range(count):
        conv[i] = parts[i].astype(bf16)


def whole(array):
    return pl.BlockSpec(array.shape, lambda i: (0,) * array.ndim)


def block_of(count):
    return max(b for b in range(1, 9) if count % b == 0)


def transform_filter(tables, taps):
    first, last, inner, inner_back, cos_t, sin_t = tables
    count, outer, lanes = taps.shape
    block = block_of(count)
    fixed = (first, inner, cos_t, sin_t)
    return pl.pallas_call(
        filter_kernel,
        grid=(count // block,),
        in_specs=[whole(a) for a in fixed] + [pl.BlockSpec((block, outer, lanes), lambda i: (i, 0, 0))],
        out_specs=pl.BlockSpec((block, outer, 2 * lanes), lambda i: (i, 0, 0)),
        out_shape=jax.ShapeDtypeStruct((count, outer, 2 * lanes), bf16),
        cost_estimate=pl.CostEstimate(
            flops=count * outer * lanes * 1536, bytes_accessed=count * outer * lanes * 8, transcendentals=0
        ),
        name="filter_transform",
    )(*fixed, taps)


def convolve(tables, mixed, spectrum):
    count, outer, lanes = mixed.shape
    block = block_of(count)
    return pl.pallas_call(
        conv_kernel,
        grid=(count // block,),
        in_specs=[whole(a) for a in tables]
        + [
            pl.BlockSpec((block, outer, lanes), lambda i: (i, 0, 0)),
            pl.BlockSpec((block, outer, 2 * lanes), lambda i: (i, 0, 0)),
        ],
        out_specs=pl.BlockSpec((block, outer, lanes), lambda i: (i, 0, 0)),
        out_shape=jax.ShapeDtypeStruct((count, outer, lanes), bf16),
        cost_estimate=pl.CostEstimate(
            flops=count * outer * lanes * 3072, bytes_accessed=count * outer * lanes * 8, transcendentals=0
        ),
        name="convolve",
    )(*tables, mixed, spectrum)


MESH = pl.DeviceIdType.MESH


def layer_kernel(
    first_in, last_in, inner_in, inner_back_in, cos_in, sin_in, skip_in, key, value, gate, kernel, weight,
    result, rest, ending, ending_weight,
    first, last, inner, inner_back, cos_t, sin_t, skip, keys, values, taps, tall, wide, long,
    spectrum, mixed_out, mixed_in, pair_in, conv_out, pair_out, conv_in, gates, weights, stacked, gated, total,
    kv_sem, here_sem, joined, ready, plane, released, sent, in_recv, pair_recv, out_recv, g_recv, w_recv,
):
    chunks, segs, chans, tokens = key.shape
    groups = gates.shape[0]
    pairs = pair_in.shape[0]
    alone = chunks - pairs
    share = tokens // groups
    quads = share // lane_width
    features = weight.shape[-1]
    cols = 512 if features % 512 == 0 else features
    outer = cos_t.shape[0]
    slabs = tokens // lane_width
    step = slabs + 8
    long_step = outer + 8
    block = segs * chans
    direct = [1, 2, 4, 6]
    passed = [2, 4, 6]
    s = lax.axis_index("seg")
    h = lax.axis_index("ch")
    side = s // 2
    low = lax.rem(s, 2)
    partner = s + 1 - 2 * low
    tail = segs - 1

    def seg_peer(d):
        return lax.rem(s + d, segs)

    def ch_peer(d):
        return lax.rem(h + d, groups)

    def flipped(at, d):
        for bit in (1, 2, 4):
            if d & bit:
                at = at + bit - 2 * bit * lax.rem(at // bit, 2)
        return at

    def lanes(j):
        return pl.ds(pl.multiple_of(j * lane_width, lane_width), lane_width)

    def tell(semaphore, seg, peer):
        pl.semaphore_signal(semaphore, inc=1, device_id=(seg, peer), device_id_type=MESH)

    def load_kv(at, size, sem):
        part = pl.ds(at, size)
        return (
            pltpu.make_async_copy(key.at[part], keys.at[part], kv_sem.at[sem]),
            pltpu.make_async_copy(value.at[part], values.at[part], kv_sem.at[sem]),
        )

    seq = list(range(alone, chunks)) + list(range(alone))
    stages = [(seq[0], 1, 0), (0, 1, 1), (1, alone - 1, 2)]
    barrier = pltpu.get_barrier_semaphore()

    @pl.when(s == 2)
    def _():
        for seg in (1, 0, 3):
            tell(barrier, seg, h)

    for copy in [*load_kv(*stages[0]), *load_kv(*stages[1])]:
        copy.start()

    @pl.when(side == 0)
    def _():
        tell(barrier, 2, h)
        tell(barrier, 3, h)

    @pl.when(s == 1)
    def _():
        tell(barrier, 0, h)

    @pl.when(s != 1)
    def _():
        for d in range(1, groups):
            tell(barrier, s, ch_peer(d))

    def part_of(peer):
        return pl.ds(pl.multiple_of(peer * share, lane_width), share)

    whole_in = (first_in, last_in, inner_in, inner_back_in, cos_in, sin_in, skip_in)
    whole_here = (first, last, inner, inner_back, cos_t, sin_t, skip)
    moves = list(zip(whole_in, whole_here)) + [
        (kernel.at[pl.ds(0, alone), s], taps.at[pl.ds(0, alone)]),
        (gate.at[:, :, :, part_of(h)], gates.at[h]),
        (weight, weights.at[h]),
    ]
    for p in range(pairs):
        moves.append((kernel.at[alone + p, pl.ds(2 * low, 2)], taps.at[pl.ds(alone + 2 * p, 2)]))
    loads = [pltpu.make_async_copy(a, b, here_sem) for a, b in moves]

    def remote(source, target, recv, seg, peer):
        return pltpu.make_async_remote_copy(
            src_ref=source, dst_ref=target, send_sem=sent, recv_sem=recv,
            device_id=(seg, peer), device_id_type=MESH,
        )

    def bulk(ref, recv):
        return remote(ref, ref, recv, partner, h)

    def send_in(k, seg):
        return remote(mixed_out.at[k, seg], mixed_in.at[k, s], in_recv.at[k], seg, h)

    def send_pair(p, seg):
        source = mixed_out.at[alone + p, pl.ds(2 * lax.rem(seg, 2), 2)]
        return remote(source, pair_in.at[p, s], pair_recv.at[p], seg, h)

    def send_gate(d):
        peer = ch_peer(d)
        return remote(gate.at[:, :, :, part_of(peer)], gates.at[h], g_recv, s, peer)

    def send_weight(d):
        return remote(weight, weights.at[h], w_recv.at[0], s, flipped(h, d))

    def pass_weight(d):
        owner = flipped(h, d)
        return remote(weights.at[owner], weights.at[owner], w_recv.at[1], s, flipped(h, 1))

    def mix_part(k, seg):
        def mix(j, carry):
            both = keys[k, seg, :, lanes(j)].astype(f32) * values[k, seg, :, lanes(j)].astype(f32)
            wide[pl.ds(j, chans, stride=step), :] = both
            return carry

        lax.fori_loop(0, slabs, mix, 0, unroll=4)
        for i in range(chans):
            mixed_out[k, seg, i] = wide[i * step : i * step + slabs, :].astype(bf16)

    def cross(k):
        @pl.when(side == 0)
        def _():
            if k >= alone:
                send_pair(k - alone, 2).start()
            else:
                send_in(k, 2).start()

        @pl.when(side == 1)
        def _():
            if k < alone:
                send_in(k, 0).start()
                send_in(k, 1).start()

    def spread_rest(k):
        @pl.when(side == 0)
        def _():
            if k < alone:
                send_in(k, 3).start()
            else:
                send_pair(k - alone, 3).start()

        if k < alone:
            send_in(k, partner).start()
        else:
            send_pair(k - alone, partner).start()

    for n, k in enumerate(seq):
        if n < len(stages):
            for copy in load_kv(*stages[n]):
                copy.wait()
        if n == 0:
            mix_part(k, 0)
            mix_part(k, 1)

            @pl.when(s == 1)
            def _():
                pl.semaphore_wait(barrier, 1)
                send_pair(0, 2).start()

            @pl.when(s == 0)
            def _():
                pl.semaphore_wait(barrier, groups + 1)
                send_pair(0, 2).start()
                for d in range(1, groups):
                    tell(plane, s, ch_peer(d))

            @pl.when(s == 2)
            def _():
                pl.semaphore_wait(barrier, groups + 1)

            @pl.when(s == tail)
            def _():
                pl.semaphore_wait(barrier, groups + 2)
                for seg in (2, 1, 0):
                    tell(joined, seg, h)

            for copy in load_kv(*stages[2]):
                copy.start()
            mix_part(k, 2)
            mix_part(k, 3)

            @pl.when(s != 1)
            def _():
                for d in range(1, groups):
                    send_gate(d).start()
        else:
            for seg in (2, 3, 0, 1):
                mix_part(k, seg)
            cross(k)
        if n == 1:
            for copy in loads:
                copy.start()
        if n == 2:

            @pl.when(s == 0)
            def _():
                pl.semaphore_wait(plane, groups - 1)
                tell(released, 1, h)

            @pl.when(s != tail)
            def _():
                pl.semaphore_wait(joined, 1)

            @pl.when(s != 1)
            def _():
                for d in range(1, segs):
                    tell(ready, seg_peer(d), h)

            for e in seq[:n]:
                spread_rest(e)
        if n >= 2:
            spread_rest(k)
        if n == 3:

            @pl.when(s == 1)
            def _():
                pl.semaphore_wait(released, 1)
                for d in range(1, segs):
                    tell(ready, seg_peer(d), h)
                for d in range(1, groups):
                    send_gate(d).start()

        if k < alone:
            mixed_in[k, s] = mixed_out[k, s]
        else:
            for e in range(2):
                pair_in[k - alone, s, e] = mixed_out[k, 2 * low + e]

            @pl.when(side == 0)
            def _():
                for seg in (2, 3):
                    pair_in[k - alone, seg] = jnp.zeros((2, chans, slabs, lane_width), bf16)

    for d in direct:
        send_weight(d).start()

    for copy in loads:
        copy.wait()
    for k in [*range(alone, alone + 2 * pairs), *range(alone)]:

        def spread(j, carry):
            tall[pl.ds(j, chans, stride=long_step), :] = taps[k, :, lanes(j)]
            return carry

        lax.fori_loop(0, outer, spread, 0, unroll=4)
        signal = [tall[i * long_step : i * long_step + outer, :].astype(bf16) for i in range(chans)]
        out = forward(signal, first[...], inner[...], cos_t[...], sin_t[...])
        spectrum[k] = out.astype(bf16).reshape(chans, outer, 2 * lane_width)
    pl.semaphore_wait(ready, segs - 1)

    def slot(k, q):
        return chunks - 1 + q if k == alone - 1 else k if k < alone else k - 1

    def convolve_rows(at, rows_of, row):
        signal = [rows_of(i).reshape(outer, lane_width) for i in range(chans)]
        filt = spectrum[at].reshape(chans * outer, 2 * lane_width)
        tables = (first[...], last[...], inner[...], inner_back[...], cos_t[...], sin_t[...])
        parts = convolve_block(tables, signal, filt)
        for i in range(chans):
            long[i * long_step : i * long_step + outer, :] = parts[i] + skip[row + i] * signal[i].astype(f32)

    for p in range(pairs):
        k = alone + p

        @pl.when(side == 0)
        def _():
            bulk(pair_in.at[p, 0], pair_recv.at[p]).wait_recv()

        @pl.when(side == 1)
        def _():
            bulk(pair_in.at[p, pl.ds(0, segs - 1)], pair_recv.at[p]).wait_recv()

        for e in range(2):
            convolve_rows(k + p + e, lambda i: pair_in[p, :, e, i], (k * segs + 2 * low + e) * chans)

            def gather(j, carry):
                from_row = side * (outer // 2) + j
                pair_out[p, e, j] = long[pl.ds(from_row, chans, stride=long_step), :].astype(bf16)
                return carry

            lax.fori_loop(0, outer // 2, gather, 0, unroll=8)
        for d in range(2):
            seg = s if d else partner

            def send(e, carry):
                peer = ch_peer(groups - 1 - e)
                rows = pl.ds(lax.rem(seg, 2) * slabs + peer * quads, quads)
                target = conv_in.at[k, h, pl.ds(2 * low, 2)]
                remote(pair_out.at[p, :, rows], target, out_recv.at[slot(k, 0)], seg, peer).start()
                return carry

            lax.fori_loop(0, groups - d, send, 0)
        for e in range(2):
            for q in range(quads):
                conv_in[k, h, 2 * low + e, q] = pair_out[p, e, low * slabs + h * quads + q]

    for k in range(alone):
        bulk(mixed_in.at[k, pl.ds(0, segs - 1)], in_recv.at[k]).wait_recv()
        convolve_rows(k, lambda i: mixed_in[k, :, i], (k * segs + s) * chans)

        def gather(j, carry):
            conv_out[k, j] = long[pl.ds(j, chans, stride=long_step), :].astype(bf16)
            return carry

        lax.fori_loop(0, outer, gather, 0, unroll=8)
        if k < alone - 1:
            batches = [(0, quads, 0, groups)]
        else:
            batches = [(q, 1, 0, 2) for q in range(quads)] + [(q, 1, 2, groups) for q in range(quads)]
        for q, size, low_peer, high_peer in batches:
            for d in (2, 3, 1, 0):
                seg = seg_peer(d)

                def send(e, carry):
                    peer = low_peer + lax.rem(h + e, high_peer - low_peer) if k == alone - 1 else ch_peer(groups - 1 - e)

                    def go():
                        source = conv_out.at[k, pl.ds(seg * slabs + peer * quads + q, size)]
                        target = conv_in.at[k, h, s, pl.ds(q, size)]
                        remote(source, target, out_recv.at[slot(k, q)], seg, peer).start()

                    if d:
                        go()
                    else:
                        pl.when(peer != h)(go)
                    return carry

                lax.fori_loop(0, high_peer - low_peer, send, 0)
        for q in range(quads):
            conv_in[k, h, s, q] = conv_out[k, s * slabs + h * quads + q]

    def restack(owner):
        def move(k, into):
            for at in range(0, segs, 2):
                pair = [weights[owner, k, at + e].astype(f32) for e in range(2)]
                rows = pl.ds(pl.multiple_of(owner * block + at * chans, 2 * chans), 2 * chans)
                into[rows, :] = jnp.concatenate(pair, axis=0).astype(bf16)

        def step_of(n, carry):
            move(lax.rem(n + alone, chunks), stacked.at[n])
            return carry

        lax.fori_loop(0, chunks - 1, step_of, 0)
        move(alone - 1, ending_weight)

    order = list(range(alone, chunks)) + list(range(alone))
    bulk(weights.at[pl.ds(0, len(direct))], w_recv.at[0]).wait_recv()
    for d in passed:
        pass_weight(d).start()
    for d in [0] + direct:
        restack(flipped(h, d))
    bulk(gates.at[pl.ds(0, groups - 1)], g_recv).wait_recv()
    bulk(weights.at[pl.ds(0, len(passed))], w_recv.at[1]).wait_recv()
    for d in passed:
        restack(flipped(h, d + 1))

    def all_pieces(k, q, size):
        if k < alone:
            ref = conv_out.at[k, pl.ds(0, (segs * groups - 1) * size)]
        else:
            ref = pair_out.at[k - alone, :, pl.ds(0, outer // 2 - quads)]
        return bulk(ref, out_recv.at[slot(k, q)])

    steps = [(k, 0, quads) for k in order[:-1]] + [(order[-1], q, 1) for q in range(quads)]
    for n, (k, start, size) in enumerate(steps):
        all_pieces(k, start, size).wait_recv()
        ends = n == len(steps) - 1
        into = ending if ends else gated
        shift = start if ends else 0
        weight_of = ending_weight if k == order[-1] else stacked.at[n]

        def combine(g, carry):
            for at in range(0, segs, 2):
                for q in range(start, start + size):
                    both = [
                        conv_in[k, g, at + e, q].astype(f32)
                        * gates[g, k, at + e, :, q * lane_width : (q + 1) * lane_width].astype(f32)
                        for e in range(2)
                    ]
                    rows = pl.ds(pl.multiple_of(g * block + at * chans, 2 * chans), 2 * chans)
                    at_q = slice((q - shift) * lane_width, (q - shift + 1) * lane_width)
                    into[rows, at_q] = jnp.concatenate(both, axis=0).astype(bf16)
            return carry

        lax.fori_loop(0, groups, combine, 0, unroll=2)
        if ends:
            continue
        tokens_at = slice(start * lane_width, (start + size) * lane_width)
        left = gated[:, tokens_at]
        for c in range(features // cols):
            at = slice(c * cols, (c + 1) * cols)
            prod = lax.dot_general(
                left, weight_of[:, at], (((0,), (0,)), ((), ())), preferred_element_type=f32
            )
            if k == order[0]:
                total[:, at] = prod
            elif k == order[-1]:
                result[tokens_at, at] = (total[tokens_at, at] + prod).astype(bf16)
            elif k != order[-2]:
                total[:, at] += prod
            else:
                early = result.shape[0]
                total[:, at] += prod
                rest[:, at] = total[early:, at]

    bulk(mixed_in.at[:, pl.ds(0, segs - 1)], g_recv).wait_send()
    for p in range(pairs):

        @pl.when(side == 0)
        def _():
            bulk(pair_in.at[p, pl.ds(0, segs - 1)], g_recv).wait_send()

        @pl.when(side == 1)
        def _():
            bulk(pair_in.at[p, 0], g_recv).wait_send()

    bulk(gates.at[pl.ds(0, groups - 1)], g_recv).wait_send()
    bulk(weights.at[pl.ds(0, groups - 1)], g_recv).wait_send()
    for k, start, size in steps:
        all_pieces(k, start, size).wait_send()


def finish_kernel(result, rest, ending, ending_weight, output, final, sem):
    early = result.shape[0]
    copies = [pltpu.make_async_copy(result, output.at[pl.ds(0, early)], sem.at[0])]
    copies[0].start()
    prod = lax.dot_general(
        ending[...], ending_weight[...], (((0,), (0,)), ((), ())), preferred_element_type=f32
    )
    final[...] = (rest[...] + prod).astype(bf16)
    copies.append(pltpu.make_async_copy(final, output.at[pl.ds(early, final.shape[0])], sem.at[1]))
    copies[1].start()
    for copy in copies:
        copy.wait()


def whole_layer(gate_in, key_in, value_in, kernel, skip_gain, out_weight, chans):
    segs, groups = lax.axis_size("seg"), lax.axis_size("ch")
    channels, tokens = key_in.shape
    full_len = kernel.shape[1]
    outer = full_len // lane_width
    slabs = tokens // lane_width
    features = out_weight.shape[1]
    chunks = channels // segs // chans
    pairs = 1
    alone = chunks - pairs
    share = tokens // groups
    quads = share // lane_width
    tables = make_tables(outer)
    split = (chunks, segs, chans)
    args = (
        *tables,
        skip_gain,
        key_in.reshape(*split, tokens),
        value_in.reshape(*split, tokens),
        gate_in.reshape(*split, tokens),
        kernel.reshape(*split, full_len),
        out_weight.reshape(*split, features),
    )
    hbm = pl.BlockSpec(memory_space=pltpu.HBM)
    dma = pltpu.SemaphoreType.DMA
    regular = pltpu.SemaphoreType.REGULAR
    tall = pltpu.VMEM((chans * (outer + 8), lane_width), f32)
    early = share - lane_width
    vmem = pl.BlockSpec(memory_space=pltpu.VMEM)
    parts = pl.pallas_call(
        layer_kernel,
        in_specs=[hbm] * len(args),
        out_specs=[vmem] * 4,
        out_shape=[
            pltpu.VMEM((early, features), bf16),
            pltpu.VMEM((lane_width, features), f32),
            pltpu.VMEM((groups * segs * chans, lane_width), bf16),
            pltpu.VMEM((groups * segs * chans, features), bf16),
        ],
        scratch_shapes=[pltpu.VMEM(a.shape, a.dtype) for a in tables]
        + [
            pltpu.SMEM(skip_gain.shape, f32),
            pltpu.VMEM((*split, tokens), bf16),
            pltpu.VMEM((*split, tokens), bf16),
            pltpu.VMEM((alone + 2 * pairs, chans, full_len), f32),
            tall,
            pltpu.VMEM((chans * (slabs + 8), lane_width), f32),
            tall,
            pltpu.VMEM((alone + 2 * pairs, chans, outer, 2 * lane_width), bf16),
            pltpu.VMEM((*split, slabs, lane_width), bf16),
            pltpu.VMEM((alone, segs, chans, slabs, lane_width), bf16),
            pltpu.VMEM((pairs, segs, 2, chans, slabs, lane_width), bf16),
            pltpu.VMEM((alone, outer, chans, lane_width), bf16),
            pltpu.VMEM((pairs, 2, outer // 2, chans, lane_width), bf16),
            pltpu.VMEM((chunks, groups, segs, quads, chans, lane_width), bf16),
            pltpu.VMEM((groups, *split, share), bf16),
            pltpu.VMEM((groups, *split, features), bf16),
            pltpu.VMEM((chunks - 1, groups * segs * chans, features), bf16),
            pltpu.VMEM((groups * segs * chans, share), bf16),
            pltpu.VMEM((share, features), f32),
            dma((3,)), dma, regular, regular, regular, regular, dma, dma((alone,)), dma((pairs,)), dma((chunks - 1 + quads,)), dma, dma((2,)),
        ],
        compiler_params=pltpu.CompilerParams(
            collective_id=0, has_side_effects=True, vmem_limit_bytes=56 * 1024 * 1024
        ),
        name="layer",
    )(*args)
    return pl.pallas_call(
        finish_kernel,
        in_specs=[vmem] * 4,
        out_specs=hbm,
        out_shape=jax.ShapeDtypeStruct((share, features), bf16),
        scratch_shapes=[pltpu.VMEM((lane_width, features), bf16), dma((2,))],
        compiler_params=pltpu.CompilerParams(vmem_limit_bytes=4 * 1024 * 1024),
        name="finish",
    )(*parts)


def on_device(gate_in, key_in, value_in, kernel, skip_gain, out_weight):
    seg_count = lax.axis_size("seg")
    seg_index = lax.axis_index("seg")
    channels, tokens = key_in.shape
    full_len = kernel.shape[1]
    outer = full_len // lane_width
    tables = make_tables(outer)
    col_count = channels // seg_count
    sublanes = 8
    fits = (seg_count, lax.axis_size("ch")) == (4, 8) and col_count % sublanes == 0 and col_count > sublanes
    if fits and tokens // lax.axis_size("ch") % lane_width == 0:
        return whole_layer(gate_in, key_in, value_in, kernel, skip_gain, out_weight, sublanes)
    mixed = key_in.astype(f32) * value_in.astype(f32)
    mixed_sent = mixed.astype(bf16).reshape(channels, tokens // lane_width, lane_width)
    col_mixed = lax.all_to_all(mixed_sent, "seg", split_axis=0, concat_axis=1, tiled=True)
    taps = lax.dynamic_slice_in_dim(kernel, seg_index * col_count, col_count, 0)
    spectrum = transform_filter(tables, taps.astype(bf16).reshape(col_count, outer, lane_width))
    col_conv = convolve(tables, col_mixed, spectrum)
    conv = lax.all_to_all(col_conv, "seg", split_axis=1, concat_axis=0, tiled=True)
    conv = conv.reshape(channels, tokens).astype(f32)
    gated = (gate_in.astype(f32) * (conv + skip_gain[:, None] * mixed)).astype(bf16)
    mine = lax.all_to_all(gated, "ch", split_axis=1, concat_axis=0, tiled=True)
    weight = lax.all_gather(out_weight, "ch", axis=0, tiled=True)
    result = lax.dot_general(
        mine, weight, (((0,), (0,)), ((), ())), preferred_element_type=f32
    )
    return result.astype(bf16)


def solution(mesh):
    placed = (P("ch", "seg"), P("ch", "seg"), P("ch", "seg"), P("ch", None), P("ch"), P("ch", None))
    return jax.shard_map(
        on_device, mesh=mesh, in_specs=placed, out_specs=P(("seg", "ch"), None), check_vma=False
    )
```

```python
import functools
import math

import jax
import jax.numpy as jnp
import numpy as np
from jax import lax
from jax.experimental import pallas as pl
from jax.experimental.pallas import tpu as pltpu
from jax.sharding import PartitionSpec as P

lane_width = 128
bf16 = jnp.bfloat16
f32 = jnp.float32


def angles(rows, cols, period):
    theta = (rows[:, None] * cols[None, :] % (4 * period)) * (2.0 * math.pi / (4 * period))
    return np.cos(theta), np.sin(theta)


def make_tables(outer):
    quarter = 4 * np.arange(outer) + 1
    row = np.arange(outer)
    lane = np.arange(lane_width)
    cos_o, sin_o = angles(quarter, row, outer)
    cos_t, sin_t = angles(quarter, lane, outer * lane_width)
    cos_i, sin_i = angles(4 * lane, lane, lane_width)
    first = np.concatenate([cos_o, -sin_o], axis=0)
    last = np.concatenate([cos_o.T, -sin_o.T], axis=1) / (outer * lane_width)
    inner = np.block([[cos_i, -sin_i], [sin_i, cos_i]])
    inner_back = np.block([[cos_i, sin_i], [-sin_i, cos_i]])
    narrow = [jnp.asarray(m.astype(np.float32).astype(bf16)) for m in (first, last, inner, inner_back)]
    return (*narrow, jnp.asarray(cos_t.astype(np.float32)), jnp.asarray(sin_t.astype(np.float32)))


def forward(signal, first, inner, cos_t, sin_t):
    outer = cos_t.shape[0]
    rows = []
    for at in range(0, len(signal), 2):
        pair = signal[at : at + 2]
        wide = jnp.dot(first, jnp.concatenate(pair, axis=1), preferred_element_type=f32)
        for i in range(len(pair)):
            part = wide[:, i * lane_width : (i + 1) * lane_width]
            real, imag = part[:outer], part[outer:]
            rows.append(
                jnp.concatenate(
                    [
                        (real * cos_t + imag * sin_t).astype(bf16),
                        (imag * cos_t - real * sin_t).astype(bf16),
                    ],
                    axis=1,
                )
            )
    return jnp.dot(jnp.concatenate(rows, axis=0), inner, preferred_element_type=f32)


def filter_kernel(first, inner, cos_t, sin_t, taps, spectrum):
    count, outer = taps.shape[0], taps.shape[1]
    signal = [taps[i].astype(bf16) for i in range(count)]
    out = forward(signal, first[...], inner[...], cos_t[...], sin_t[...])
    spectrum[...] = out.astype(bf16).reshape(count, outer, 2 * lane_width)


def convolve_block(tables, signal, filt):
    first, last, inner, inner_back, cos, sin = tables
    outer = cos.shape[0]
    sig = forward(signal, first, inner, cos, sin)
    filt = filt.astype(f32)
    sig_re, sig_im = sig[:, :lane_width], sig[:, lane_width:]
    filt_re, filt_im = filt[:, :lane_width], filt[:, lane_width:]
    prod = jnp.concatenate(
        [
            (filt_re * sig_re - filt_im * sig_im).astype(bf16),
            (filt_re * sig_im + filt_im * sig_re).astype(bf16),
        ],
        axis=1,
    )
    back = jnp.dot(prod, inner_back, preferred_element_type=f32)
    parts = []
    for at in range(0, len(signal), 2):
        cols = []
        for i in range(at, min(at + 2, len(signal))):
            rows = back[i * outer : (i + 1) * outer]
            real, imag = rows[:, :lane_width], rows[:, lane_width:]
            cols.append(
                jnp.concatenate(
                    [
                        (real * cos - imag * sin).astype(bf16),
                        (imag * cos + real * sin).astype(bf16),
                    ],
                    axis=0,
                )
            )
        wide = jnp.dot(last, jnp.concatenate(cols, axis=1), preferred_element_type=f32)
        for i in range(len(cols)):
            parts.append(wide[:, i * lane_width : (i + 1) * lane_width])
    return parts


def conv_kernel(first, last, inner, inner_back, cos_t, sin_t, mixed, spectrum, conv):
    count, outer = mixed.shape[0], mixed.shape[1]
    tables = (first[...], last[...], inner[...], inner_back[...], cos_t[...], sin_t[...])
    filt = spectrum[...].reshape(count * outer, 2 * lane_width)
    parts = convolve_block(tables, [mixed[i] for i in range(count)], filt)
    for i in range(count):
        conv[i] = parts[i].astype(bf16)


def whole(array):
    return pl.BlockSpec(array.shape, lambda i: (0,) * array.ndim)


def block_of(count):
    return max(b for b in range(1, 9) if count % b == 0)


def transform_filter(tables, taps):
    first, last, inner, inner_back, cos_t, sin_t = tables
    count, outer, lanes = taps.shape
    block = block_of(count)
    fixed = (first, inner, cos_t, sin_t)
    return pl.pallas_call(
        filter_kernel,
        grid=(count // block,),
        in_specs=[whole(a) for a in fixed] + [pl.BlockSpec((block, outer, lanes), lambda i: (i, 0, 0))],
        out_specs=pl.BlockSpec((block, outer, 2 * lanes), lambda i: (i, 0, 0)),
        out_shape=jax.ShapeDtypeStruct((count, outer, 2 * lanes), bf16),
        cost_estimate=pl.CostEstimate(
            flops=count * outer * lanes * 1536, bytes_accessed=count * outer * lanes * 8, transcendentals=0
        ),
        name="filter_transform",
    )(*fixed, taps)


def convolve(tables, mixed, spectrum):
    count, outer, lanes = mixed.shape
    block = block_of(count)
    return pl.pallas_call(
        conv_kernel,
        grid=(count // block,),
        in_specs=[whole(a) for a in tables]
        + [
            pl.BlockSpec((block, outer, lanes), lambda i: (i, 0, 0)),
            pl.BlockSpec((block, outer, 2 * lanes), lambda i: (i, 0, 0)),
        ],
        out_specs=pl.BlockSpec((block, outer, lanes), lambda i: (i, 0, 0)),
        out_shape=jax.ShapeDtypeStruct((count, outer, lanes), bf16),
        cost_estimate=pl.CostEstimate(
            flops=count * outer * lanes * 3072, bytes_accessed=count * outer * lanes * 8, transcendentals=0
        ),
        name="convolve",
    )(*tables, mixed, spectrum)


MESH = pl.DeviceIdType.MESH


def layer_kernel(
    first_in, last_in, inner_in, inner_back_in, cos_in, sin_in, skip_in, key, value, gate, kernel, weight,
    result, rest, ending, ending_weight,
    first, last, inner, inner_back, cos_t, sin_t, skip, keys, values, taps, tall, wide, long,
    spectrum, mixed_out, mixed_in, pair_in, conv_out, pair_out, conv_in, gates, weights, stacked, gated, total,
    kv_sem, here_sem, joined, ready, plane, released, sent, in_recv, pair_recv, out_recv, g_recv, w_recv,
):
    chunks, segs, chans, tokens = key.shape
    groups = gates.shape[0]
    pairs = pair_in.shape[0]
    alone = chunks - pairs
    share = tokens // groups
    quads = share // lane_width
    features = weight.shape[-1]
    cols = 512 if features % 512 == 0 else features
    outer = cos_t.shape[0]
    slabs = tokens // lane_width
    step = slabs + 8
    long_step = outer + 8
    block = segs * chans
    direct = [1, 2, 4, 6]
    passed = [2, 4, 6]
    s = lax.axis_index("seg")
    h = lax.axis_index("ch")
    side = s // 2
    low = lax.rem(s, 2)
    partner = s + 1 - 2 * low
    tail = segs - 1

    def seg_peer(d):
        return lax.rem(s + d, segs)

    def ch_peer(d):
        return lax.rem(h + d, groups)

    def flipped(at, d):
        for bit in (1, 2, 4):
            if d & bit:
                at = at + bit - 2 * bit * lax.rem(at // bit, 2)
        return at

    def lanes(j):
        return pl.ds(pl.multiple_of(j * lane_width, lane_width), lane_width)

    def tell(semaphore, seg, peer):
        pl.semaphore_signal(semaphore, inc=1, device_id=(seg, peer), device_id_type=MESH)

    def load_kv(at, size, sem):
        part = pl.ds(at, size)
        return (
            pltpu.make_async_copy(key.at[part], keys.at[part], kv_sem.at[sem]),
            pltpu.make_async_copy(value.at[part], values.at[part], kv_sem.at[sem]),
        )

    seq = list(range(alone, chunks)) + list(range(alone))
    stages = [(seq[0], 1, 0), (0, 1, 1), (1, alone - 1, 2)]
    barrier = pltpu.get_barrier_semaphore()

    @pl.when(s == 2)
    def _():
        for seg in (1, 0, 3):
            tell(barrier, seg, h)

    for copy in [*load_kv(*stages[0]), *load_kv(*stages[1])]:
        copy.start()

    @pl.when(side == 0)
    def _():
        tell(barrier, 2, h)
        tell(barrier, 3, h)

    @pl.when(s == 1)
    def _():
        tell(barrier, 0, h)

    @pl.when(s != 1)
    def _():
        for d in range(1, groups):
            tell(barrier, s, ch_peer(d))

    def part_of(peer):
        return pl.ds(pl.multiple_of(peer * share, lane_width), share)

    whole_in = (first_in, last_in, inner_in, inner_back_in, cos_in, sin_in, skip_in)
    whole_here = (first, last, inner, inner_back, cos_t, sin_t, skip)
    moves = list(zip(whole_in, whole_here)) + [
        (kernel.at[pl.ds(0, alone), s], taps.at[pl.ds(0, alone)]),
        (gate.at[:, :, :, part_of(h)], gates.at[h]),
        (weight, weights.at[h]),
    ]
    for p in range(pairs):
        moves.append((kernel.at[alone + p, pl.ds(2 * low, 2)], taps.at[pl.ds(alone + 2 * p, 2)]))
    loads = [pltpu.make_async_copy(a, b, here_sem) for a, b in moves]

    def remote(source, target, recv, seg, peer):
        return pltpu.make_async_remote_copy(
            src_ref=source, dst_ref=target, send_sem=sent, recv_sem=recv,
            device_id=(seg, peer), device_id_type=MESH,
        )

    def bulk(ref, recv):
        return remote(ref, ref, recv, partner, h)

    def send_in(k, seg):
        return remote(mixed_out.at[k, seg], mixed_in.at[k, s], in_recv.at[k], seg, h)

    def send_pair(p, seg):
        source = mixed_out.at[alone + p, pl.ds(2 * lax.rem(seg, 2), 2)]
        return remote(source, pair_in.at[p, s], pair_recv.at[p], seg, h)

    def send_gate(d):
        peer = ch_peer(d)
        return remote(gate.at[:, :, :, part_of(peer)], gates.at[h], g_recv, s, peer)

    def send_weight(d):
        return remote(weight, weights.at[h], w_recv.at[0], s, flipped(h, d))

    def pass_weight(d):
        owner = flipped(h, d)
        return remote(weights.at[owner], weights.at[owner], w_recv.at[1], s, flipped(h, 1))

    def mix_part(k, seg):
        def mix(j, carry):
            both = keys[k, seg, :, lanes(j)].astype(f32) * values[k, seg, :, lanes(j)].astype(f32)
            wide[pl.ds(j, chans, stride=step), :] = both
            return carry

        lax.fori_loop(0, slabs, mix, 0, unroll=4)
        for i in range(chans):
            mixed_out[k, seg, i] = wide[i * step : i * step + slabs, :].astype(bf16)

    def cross(k):
        @pl.when(side == 0)
        def _():
            if k >= alone:
                send_pair(k - alone, 2).start()
            else:
                send_in(k, 2).start()

        @pl.when(side == 1)
        def _():
            if k < alone:
                send_in(k, 0).start()
                send_in(k, 1).start()

    def spread_rest(k):
        @pl.when(side == 0)
        def _():
            if k < alone:
                send_in(k, 3).start()
            else:
                send_pair(k - alone, 3).start()

        if k < alone:
            send_in(k, partner).start()
        else:
            send_pair(k - alone, partner).start()

    for n, k in enumerate(seq):
        if n < len(stages):
            for copy in load_kv(*stages[n]):
                copy.wait()
        if n == 0:
            mix_part(k, 0)
            mix_part(k, 1)

            @pl.when(s == 1)
            def _():
                pl.semaphore_wait(barrier, 1)
                send_pair(0, 2).start()

            @pl.when(s == 0)
            def _():
                pl.semaphore_wait(barrier, groups + 1)
                send_pair(0, 2).start()
                for d in range(1, groups):
                    tell(plane, s, ch_peer(d))

            @pl.when(s == 2)
            def _():
                pl.semaphore_wait(barrier, groups + 1)

            @pl.when(s == tail)
            def _():
                pl.semaphore_wait(barrier, groups + 2)
                for seg in (2, 1, 0):
                    tell(joined, seg, h)

            for copy in load_kv(*stages[2]):
                copy.start()
            mix_part(k, 2)
            mix_part(k, 3)

            @pl.when(s != 1)
            def _():
                for d in direct:
                    send_weight(d).start()
        else:
            for seg in (2, 3, 0, 1):
                mix_part(k, seg)
            cross(k)
        if n == 1:
            for copy in loads:
                copy.start()
        if n == 2:

            @pl.when(s == 0)
            def _():
                pl.semaphore_wait(plane, groups - 1)
                tell(released, 1, h)

            @pl.when(s != tail)
            def _():
                pl.semaphore_wait(joined, 1)

            @pl.when(s != 1)
            def _():
                for d in range(1, segs):
                    tell(ready, seg_peer(d), h)

            for e in seq[:n]:
                spread_rest(e)
        if n >= 2:
            spread_rest(k)
        if n == 3:

            @pl.when(s == 1)
            def _():
                pl.semaphore_wait(released, 1)
                for d in range(1, segs):
                    tell(ready, seg_peer(d), h)
                for d in direct:
                    send_weight(d).start()

        if k < alone:
            mixed_in[k, s] = mixed_out[k, s]
        else:
            for e in range(2):
                pair_in[k - alone, s, e] = mixed_out[k, 2 * low + e]

            @pl.when(side == 0)
            def _():
                for seg in (2, 3):
                    pair_in[k - alone, seg] = jnp.zeros((2, chans, slabs, lane_width), bf16)

    for d in range(1, groups):
        send_gate(d).start()

    for copy in loads:
        copy.wait()
    for k in [*range(alone, alone + 2 * pairs), *range(alone)]:

        def spread(j, carry):
            tall[pl.ds(j, chans, stride=long_step), :] = taps[k, :, lanes(j)]
            return carry

        lax.fori_loop(0, outer, spread, 0, unroll=4)
        signal = [tall[i * long_step : i * long_step + outer, :].astype(bf16) for i in range(chans)]
        out = forward(signal, first[...], inner[...], cos_t[...], sin_t[...])
        spectrum[k] = out.astype(bf16).reshape(chans, outer, 2 * lane_width)
    pl.semaphore_wait(ready, segs - 1)

    def slot(k, q):
        return chunks - 1 + q if k == alone - 1 else k if k < alone else k - 1

    def convolve_rows(at, rows_of, row):
        signal = [rows_of(i).reshape(outer, lane_width) for i in range(chans)]
        filt = spectrum[at].reshape(chans * outer, 2 * lane_width)
        tables = (first[...], last[...], inner[...], inner_back[...], cos_t[...], sin_t[...])
        parts = convolve_block(tables, signal, filt)
        for i in range(chans):
            long[i * long_step : i * long_step + outer, :] = parts[i] + skip[row + i] * signal[i].astype(f32)

    for p in range(pairs):
        k = alone + p

        @pl.when(side == 0)
        def _():
            bulk(pair_in.at[p, 0], pair_recv.at[p]).wait_recv()

        @pl.when(side == 1)
        def _():
            bulk(pair_in.at[p, pl.ds(0, segs - 1)], pair_recv.at[p]).wait_recv()

        for e in range(2):
            convolve_rows(k + p + e, lambda i: pair_in[p, :, e, i], (k * segs + 2 * low + e) * chans)

            def gather(j, carry):
                from_row = side * (outer // 2) + j
                pair_out[p, e, j] = long[pl.ds(from_row, chans, stride=long_step), :].astype(bf16)
                return carry

            lax.fori_loop(0, outer // 2, gather, 0, unroll=8)
        for d in range(2):
            seg = s if d else partner

            def send(e, carry):
                peer = ch_peer(groups - 1 - e)
                rows = pl.ds(lax.rem(seg, 2) * slabs + peer * quads, quads)
                target = conv_in.at[k, h, pl.ds(2 * low, 2)]
                remote(pair_out.at[p, :, rows], target, out_recv.at[slot(k, 0)], seg, peer).start()
                return carry

            lax.fori_loop(0, groups - d, send, 0)
        for e in range(2):
            for q in range(quads):
                conv_in[k, h, 2 * low + e, q] = pair_out[p, e, low * slabs + h * quads + q]

    for k in range(alone):
        bulk(mixed_in.at[k, pl.ds(0, segs - 1)], in_recv.at[k]).wait_recv()
        convolve_rows(k, lambda i: mixed_in[k, :, i], (k * segs + s) * chans)

        def gather(j, carry):
            conv_out[k, j] = long[pl.ds(j, chans, stride=long_step), :].astype(bf16)
            return carry

        lax.fori_loop(0, outer, gather, 0, unroll=8)
        if k < alone - 1:
            batches = [(0, quads, 0, groups)]
        else:
            batches = [(q, 1, 0, 2) for q in range(quads)] + [(q, 1, 2, groups) for q in range(quads)]
        for q, size, low_peer, high_peer in batches:
            for d in (2, 3, 1, 0):
                seg = seg_peer(d)

                def send(e, carry):
                    peer = low_peer + lax.rem(h + e, high_peer - low_peer) if k == alone - 1 else ch_peer(groups - 1 - e)

                    def go():
                        source = conv_out.at[k, pl.ds(seg * slabs + peer * quads + q, size)]
                        target = conv_in.at[k, h, s, pl.ds(q, size)]
                        remote(source, target, out_recv.at[slot(k, q)], seg, peer).start()

                    if d:
                        go()
                    else:
                        pl.when(peer != h)(go)
                    return carry

                lax.fori_loop(0, high_peer - low_peer, send, 0)
        for q in range(quads):
            conv_in[k, h, s, q] = conv_out[k, s * slabs + h * quads + q]

    def restack(owner):
        def move(k, into):
            for at in range(0, segs, 2):
                pair = [weights[owner, k, at + e].astype(f32) for e in range(2)]
                rows = pl.ds(pl.multiple_of(owner * block + at * chans, 2 * chans), 2 * chans)
                into[rows, :] = jnp.concatenate(pair, axis=0).astype(bf16)

        def step_of(n, carry):
            move(lax.rem(n + alone, chunks), stacked.at[n])
            return carry

        lax.fori_loop(0, chunks - 1, step_of, 0)
        move(alone - 1, ending_weight)

    order = list(range(alone, chunks)) + list(range(alone))
    bulk(weights.at[pl.ds(0, len(direct))], w_recv.at[0]).wait_recv()
    for d in passed:
        pass_weight(d).start()
    for d in [0] + direct:
        restack(flipped(h, d))
    bulk(gates.at[pl.ds(0, groups - 1)], g_recv).wait_recv()
    bulk(weights.at[pl.ds(0, len(passed))], w_recv.at[1]).wait_recv()
    for d in passed:
        restack(flipped(h, d + 1))

    def all_pieces(k, q, size):
        if k < alone:
            ref = conv_out.at[k, pl.ds(0, (segs * groups - 1) * size)]
        else:
            ref = pair_out.at[k - alone, :, pl.ds(0, outer // 2 - quads)]
        return bulk(ref, out_recv.at[slot(k, q)])

    steps = [(k, 0, quads) for k in order[:-1]] + [(order[-1], q, 1) for q in range(quads)]
    for n, (k, start, size) in enumerate(steps):
        all_pieces(k, start, size).wait_recv()
        ends = n == len(steps) - 1
        into = ending if ends else gated
        shift = start if ends else 0
        weight_of = ending_weight if k == order[-1] else stacked.at[n]

        def combine(g, carry):
            for at in range(0, segs, 2):
                for q in range(start, start + size):
                    both = [
                        conv_in[k, g, at + e, q].astype(f32)
                        * gates[g, k, at + e, :, q * lane_width : (q + 1) * lane_width].astype(f32)
                        for e in range(2)
                    ]
                    rows = pl.ds(pl.multiple_of(g * block + at * chans, 2 * chans), 2 * chans)
                    at_q = slice((q - shift) * lane_width, (q - shift + 1) * lane_width)
                    into[rows, at_q] = jnp.concatenate(both, axis=0).astype(bf16)
            return carry

        lax.fori_loop(0, groups, combine, 0, unroll=2)
        if ends:
            continue
        tokens_at = slice(start * lane_width, (start + size) * lane_width)
        left = gated[:, tokens_at]
        for c in range(features // cols):
            at = slice(c * cols, (c + 1) * cols)
            prod = lax.dot_general(
                left, weight_of[:, at], (((0,), (0,)), ((), ())), preferred_element_type=f32
            )
            if k == order[0]:
                total[:, at] = prod
            elif k == order[-1]:
                result[tokens_at, at] = (total[tokens_at, at] + prod).astype(bf16)
            elif k != order[-2]:
                total[:, at] += prod
            else:
                early = result.shape[0]
                total[:, at] += prod
                rest[:, at] = total[early:, at]

    bulk(mixed_in.at[:, pl.ds(0, segs - 1)], g_recv).wait_send()
    for p in range(pairs):

        @pl.when(side == 0)
        def _():
            bulk(pair_in.at[p, pl.ds(0, segs - 1)], g_recv).wait_send()

        @pl.when(side == 1)
        def _():
            bulk(pair_in.at[p, 0], g_recv).wait_send()

    bulk(gates.at[pl.ds(0, groups - 1)], g_recv).wait_send()
    bulk(weights.at[pl.ds(0, groups - 1)], g_recv).wait_send()
    for k, start, size in steps:
        all_pieces(k, start, size).wait_send()


def finish_kernel(result, rest, ending, ending_weight, output, final, sem):
    early = result.shape[0]
    copies = [pltpu.make_async_copy(result, output.at[pl.ds(0, early)], sem.at[0])]
    copies[0].start()
    prod = lax.dot_general(
        ending[...], ending_weight[...], (((0,), (0,)), ((), ())), preferred_element_type=f32
    )
    final[...] = (rest[...] + prod).astype(bf16)
    copies.append(pltpu.make_async_copy(final, output.at[pl.ds(early, final.shape[0])], sem.at[1]))
    copies[1].start()
    for copy in copies:
        copy.wait()


def whole_layer(gate_in, key_in, value_in, kernel, skip_gain, out_weight, chans):
    segs, groups = lax.axis_size("seg"), lax.axis_size("ch")
    channels, tokens = key_in.shape
    full_len = kernel.shape[1]
    outer = full_len // lane_width
    slabs = tokens // lane_width
    features = out_weight.shape[1]
    chunks = channels // segs // chans
    pairs = 1
    alone = chunks - pairs
    share = tokens // groups
    quads = share // lane_width
    tables = make_tables(outer)
    split = (chunks, segs, chans)
    args = (
        *tables,
        skip_gain,
        key_in.reshape(*split, tokens),
        value_in.reshape(*split, tokens),
        gate_in.reshape(*split, tokens),
        kernel.reshape(*split, full_len),
        out_weight.reshape(*split, features),
    )
    hbm = pl.BlockSpec(memory_space=pltpu.HBM)
    dma = pltpu.SemaphoreType.DMA
    regular = pltpu.SemaphoreType.REGULAR
    tall = pltpu.VMEM((chans * (outer + 8), lane_width), f32)
    early = share - lane_width
    vmem = pl.BlockSpec(memory_space=pltpu.VMEM)
    parts = pl.pallas_call(
        layer_kernel,
        in_specs=[hbm] * len(args),
        out_specs=[vmem] * 4,
        out_shape=[
            pltpu.VMEM((early, features), bf16),
            pltpu.VMEM((lane_width, features), f32),
            pltpu.VMEM((groups * segs * chans, lane_width), bf16),
            pltpu.VMEM((groups * segs * chans, features), bf16),
        ],
        scratch_shapes=[pltpu.VMEM(a.shape, a.dtype) for a in tables]
        + [
            pltpu.SMEM(skip_gain.shape, f32),
            pltpu.VMEM((*split, tokens), bf16),
            pltpu.VMEM((*split, tokens), bf16),
            pltpu.VMEM((alone + 2 * pairs, chans, full_len), f32),
            tall,
            pltpu.VMEM((chans * (slabs + 8), lane_width), f32),
            tall,
            pltpu.VMEM((alone + 2 * pairs, chans, outer, 2 * lane_width), bf16),
            pltpu.VMEM((*split, slabs, lane_width), bf16),
            pltpu.VMEM((alone, segs, chans, slabs, lane_width), bf16),
            pltpu.VMEM((pairs, segs, 2, chans, slabs, lane_width), bf16),
            pltpu.VMEM((alone, outer, chans, lane_width), bf16),
            pltpu.VMEM((pairs, 2, outer // 2, chans, lane_width), bf16),
            pltpu.VMEM((chunks, groups, segs, quads, chans, lane_width), bf16),
            pltpu.VMEM((groups, *split, share), bf16),
            pltpu.VMEM((groups, *split, features), bf16),
            pltpu.VMEM((chunks - 1, groups * segs * chans, features), bf16),
            pltpu.VMEM((groups * segs * chans, share), bf16),
            pltpu.VMEM((share, features), f32),
            dma((3,)), dma, regular, regular, regular, regular, dma, dma((alone,)), dma((pairs,)), dma((chunks - 1 + quads,)), dma, dma((2,)),
        ],
        compiler_params=pltpu.CompilerParams(
            collective_id=0, has_side_effects=True, vmem_limit_bytes=56 * 1024 * 1024
        ),
        name="layer",
    )(*args)
    return pl.pallas_call(
        finish_kernel,
        in_specs=[vmem] * 4,
        out_specs=hbm,
        out_shape=jax.ShapeDtypeStruct((share, features), bf16),
        scratch_shapes=[pltpu.VMEM((lane_width, features), bf16), dma((2,))],
        compiler_params=pltpu.CompilerParams(vmem_limit_bytes=4 * 1024 * 1024),
        name="finish",
    )(*parts)


def on_device(gate_in, key_in, value_in, kernel, skip_gain, out_weight):
    seg_count = lax.axis_size("seg")
    seg_index = lax.axis_index("seg")
    channels, tokens = key_in.shape
    full_len = kernel.shape[1]
    outer = full_len // lane_width
    tables = make_tables(outer)
    col_count = channels // seg_count
    sublanes = 8
    fits = (seg_count, lax.axis_size("ch")) == (4, 8) and col_count % sublanes == 0 and col_count > sublanes
    if fits and tokens // lax.axis_size("ch") % lane_width == 0:
        return whole_layer(gate_in, key_in, value_in, kernel, skip_gain, out_weight, sublanes)
    mixed = key_in.astype(f32) * value_in.astype(f32)
    mixed_sent = mixed.astype(bf16).reshape(channels, tokens // lane_width, lane_width)
    col_mixed = lax.all_to_all(mixed_sent, "seg", split_axis=0, concat_axis=1, tiled=True)
    taps = lax.dynamic_slice_in_dim(kernel, seg_index * col_count, col_count, 0)
    spectrum = transform_filter(tables, taps.astype(bf16).reshape(col_count, outer, lane_width))
    col_conv = convolve(tables, col_mixed, spectrum)
    conv = lax.all_to_all(col_conv, "seg", split_axis=1, concat_axis=0, tiled=True)
    conv = conv.reshape(channels, tokens).astype(f32)
    gated = (gate_in.astype(f32) * (conv + skip_gain[:, None] * mixed)).astype(bf16)
    mine = lax.all_to_all(gated, "ch", split_axis=1, concat_axis=0, tiled=True)
    weight = lax.all_gather(out_weight, "ch", axis=0, tiled=True)
    result = lax.dot_general(
        mine, weight, (((0,), (0,)), ((), ())), preferred_element_type=f32
    )
    return result.astype(bf16)


def solution(mesh):
    placed = (P("ch", "seg"), P("ch", "seg"), P("ch", "seg"), P("ch", None), P("ch"), P("ch", None))
    return jax.shard_map(
        on_device, mesh=mesh, in_specs=placed, out_specs=P(("seg", "ch"), None), check_vma=False
    )
```

```python
import functools
import math

import jax
import jax.numpy as jnp
import numpy as np
from jax import lax
from jax.experimental import pallas as pl
from jax.experimental.pallas import tpu as pltpu
from jax.sharding import PartitionSpec as P

lane_width = 128
bf16 = jnp.bfloat16
f32 = jnp.float32


def angles(rows, cols, period):
    theta = (rows[:, None] * cols[None, :] % (4 * period)) * (2.0 * math.pi / (4 * period))
    return np.cos(theta), np.sin(theta)


def make_tables(outer):
    quarter = 4 * np.arange(outer) + 1
    row = np.arange(outer)
    lane = np.arange(lane_width)
    cos_o, sin_o = angles(quarter, row, outer)
    cos_t, sin_t = angles(quarter, lane, outer * lane_width)
    cos_i, sin_i = angles(4 * lane, lane, lane_width)
    first = np.concatenate([cos_o, -sin_o], axis=0)
    last = np.concatenate([cos_o.T, -sin_o.T], axis=1) / (outer * lane_width)
    inner = np.block([[cos_i, -sin_i], [sin_i, cos_i]])
    inner_back = np.block([[cos_i, sin_i], [-sin_i, cos_i]])
    narrow = [jnp.asarray(m.astype(np.float32).astype(bf16)) for m in (first, last, inner, inner_back)]
    return (*narrow, jnp.asarray(cos_t.astype(np.float32)), jnp.asarray(sin_t.astype(np.float32)))


def forward(signal, first, inner, cos_t, sin_t):
    outer = cos_t.shape[0]
    rows = []
    for at in range(0, len(signal), 2):
        pair = signal[at : at + 2]
        wide = jnp.dot(first, jnp.concatenate(pair, axis=1), preferred_element_type=f32)
        for i in range(len(pair)):
            part = wide[:, i * lane_width : (i + 1) * lane_width]
            real, imag = part[:outer], part[outer:]
            rows.append(
                jnp.concatenate(
                    [
                        (real * cos_t + imag * sin_t).astype(bf16),
                        (imag * cos_t - real * sin_t).astype(bf16),
                    ],
                    axis=1,
                )
            )
    return jnp.dot(jnp.concatenate(rows, axis=0), inner, preferred_element_type=f32)


def filter_kernel(first, inner, cos_t, sin_t, taps, spectrum):
    count, outer = taps.shape[0], taps.shape[1]
    signal = [taps[i].astype(bf16) for i in range(count)]
    out = forward(signal, first[...], inner[...], cos_t[...], sin_t[...])
    spectrum[...] = out.astype(bf16).reshape(count, outer, 2 * lane_width)


def convolve_block(tables, signal, filt):
    first, last, inner, inner_back, cos, sin = tables
    outer = cos.shape[0]
    sig = forward(signal, first, inner, cos, sin)
    filt = filt.astype(f32)
    sig_re, sig_im = sig[:, :lane_width], sig[:, lane_width:]
    filt_re, filt_im = filt[:, :lane_width], filt[:, lane_width:]
    prod = jnp.concatenate(
        [
            (filt_re * sig_re - filt_im * sig_im).astype(bf16),
            (filt_re * sig_im + filt_im * sig_re).astype(bf16),
        ],
        axis=1,
    )
    back = jnp.dot(prod, inner_back, preferred_element_type=f32)
    parts = []
    for at in range(0, len(signal), 2):
        cols = []
        for i in range(at, min(at + 2, len(signal))):
            rows = back[i * outer : (i + 1) * outer]
            real, imag = rows[:, :lane_width], rows[:, lane_width:]
            cols.append(
                jnp.concatenate(
                    [
                        (real * cos - imag * sin).astype(bf16),
                        (imag * cos + real * sin).astype(bf16),
                    ],
                    axis=0,
                )
            )
        wide = jnp.dot(last, jnp.concatenate(cols, axis=1), preferred_element_type=f32)
        for i in range(len(cols)):
            parts.append(wide[:, i * lane_width : (i + 1) * lane_width])
    return parts


def conv_kernel(first, last, inner, inner_back, cos_t, sin_t, mixed, spectrum, conv):
    count, outer = mixed.shape[0], mixed.shape[1]
    tables = (first[...], last[...], inner[...], inner_back[...], cos_t[...], sin_t[...])
    filt = spectrum[...].reshape(count * outer, 2 * lane_width)
    parts = convolve_block(tables, [mixed[i] for i in range(count)], filt)
    for i in range(count):
        conv[i] = parts[i].astype(bf16)


def whole(array):
    return pl.BlockSpec(array.shape, lambda i: (0,) * array.ndim)


def block_of(count):
    return max(b for b in range(1, 9) if count % b == 0)


def transform_filter(tables, taps):
    first, last, inner, inner_back, cos_t, sin_t = tables
    count, outer, lanes = taps.shape
    block = block_of(count)
    fixed = (first, inner, cos_t, sin_t)
    return pl.pallas_call(
        filter_kernel,
        grid=(count // block,),
        in_specs=[whole(a) for a in fixed] + [pl.BlockSpec((block, outer, lanes), lambda i: (i, 0, 0))],
        out_specs=pl.BlockSpec((block, outer, 2 * lanes), lambda i: (i, 0, 0)),
        out_shape=jax.ShapeDtypeStruct((count, outer, 2 * lanes), bf16),
        cost_estimate=pl.CostEstimate(
            flops=count * outer * lanes * 1536, bytes_accessed=count * outer * lanes * 8, transcendentals=0
        ),
        name="filter_transform",
    )(*fixed, taps)


def convolve(tables, mixed, spectrum):
    count, outer, lanes = mixed.shape
    block = block_of(count)
    return pl.pallas_call(
        conv_kernel,
        grid=(count // block,),
        in_specs=[whole(a) for a in tables]
        + [
            pl.BlockSpec((block, outer, lanes), lambda i: (i, 0, 0)),
            pl.BlockSpec((block, outer, 2 * lanes), lambda i: (i, 0, 0)),
        ],
        out_specs=pl.BlockSpec((block, outer, lanes), lambda i: (i, 0, 0)),
        out_shape=jax.ShapeDtypeStruct((count, outer, lanes), bf16),
        cost_estimate=pl.CostEstimate(
            flops=count * outer * lanes * 3072, bytes_accessed=count * outer * lanes * 8, transcendentals=0
        ),
        name="convolve",
    )(*tables, mixed, spectrum)


MESH = pl.DeviceIdType.MESH


def layer_kernel(
    first_in, last_in, inner_in, inner_back_in, cos_in, sin_in, skip_in, key, value, gate, kernel, weight,
    result, rest, ending, ending_weight,
    first, last, inner, inner_back, cos_t, sin_t, skip, keys, values, taps, tall, wide, long,
    spectrum, mixed_out, mixed_in, pair_in, conv_out, pair_out, conv_in, gates, weights, stacked, gated, total,
    kv_sem, here_sem, joined, ready, plane, released, sent, in_recv, pair_recv, out_recv, g_recv, w_recv,
):
    chunks, segs, chans, tokens = key.shape
    groups = gates.shape[0]
    pairs = pair_in.shape[0]
    alone = chunks - pairs
    share = tokens // groups
    quads = share // lane_width
    features = weight.shape[-1]
    cols = 512 if features % 512 == 0 else features
    outer = cos_t.shape[0]
    slabs = tokens // lane_width
    step = slabs + 8
    long_step = outer + 8
    block = segs * chans
    direct = [1, 2, 4, 6]
    passed = [2, 4, 6]
    s = lax.axis_index("seg")
    h = lax.axis_index("ch")
    side = s // 2
    low = lax.rem(s, 2)
    partner = s + 1 - 2 * low
    tail = segs - 1

    def seg_peer(d):
        return lax.rem(s + d, segs)

    def ch_peer(d):
        return lax.rem(h + d, groups)

    def flipped(at, d):
        for bit in (1, 2, 4):
            if d & bit:
                at = at + bit - 2 * bit * lax.rem(at // bit, 2)
        return at

    def lanes(j):
        return pl.ds(pl.multiple_of(j * lane_width, lane_width), lane_width)

    def tell(semaphore, seg, peer):
        pl.semaphore_signal(semaphore, inc=1, device_id=(seg, peer), device_id_type=MESH)

    def load_kv(at, size, sem):
        part = pl.ds(at, size)
        return (
            pltpu.make_async_copy(key.at[part], keys.at[part], kv_sem.at[sem]),
            pltpu.make_async_copy(value.at[part], values.at[part], kv_sem.at[sem]),
        )

    seq = list(range(alone, chunks)) + list(range(alone))
    stages = [(seq[0], 1, 0), (0, 1, 1), (1, alone - 1, 2)]
    barrier = pltpu.get_barrier_semaphore()

    @pl.when(s == 2)
    def _():
        for seg in (1, 0, 3):
            tell(barrier, seg, h)


    def load_half(half):
        at = (alone, pl.ds(2 * half, 2))
        sem = kv_sem.at[3 * half]
        return (
            pltpu.make_async_copy(key.at[at], keys.at[at], sem),
            pltpu.make_async_copy(value.at[at], values.at[at], sem),
        )

    for copy in [*load_half(0), *load_half(1), *load_kv(*stages[1])]:
        copy.start()

    @pl.when(side == 0)
    def _():
        tell(barrier, 2, h)
        tell(barrier, 3, h)

    @pl.when(s == 1)
    def _():
        tell(barrier, 0, h)

    @pl.when(s != 1)
    def _():
        for d in range(1, groups):
            tell(barrier, s, ch_peer(d))

    def part_of(peer):
        return pl.ds(pl.multiple_of(peer * share, lane_width), share)

    whole_in = (first_in, last_in, inner_in, inner_back_in, cos_in, sin_in, skip_in)
    whole_here = (first, last, inner, inner_back, cos_t, sin_t, skip)
    moves = list(zip(whole_in, whole_here)) + [
        (kernel.at[pl.ds(0, alone), s], taps.at[pl.ds(0, alone)]),
        (gate.at[:, :, :, part_of(h)], gates.at[h]),
        (weight, weights.at[h]),
    ]
    for p in range(pairs):
        moves.append((kernel.at[alone + p, pl.ds(2 * low, 2)], taps.at[pl.ds(alone + 2 * p, 2)]))
    loads = [pltpu.make_async_copy(a, b, here_sem) for a, b in moves]

    def remote(source, target, recv, seg, peer):
        return pltpu.make_async_remote_copy(
            src_ref=source, dst_ref=target, send_sem=sent, recv_sem=recv,
            device_id=(seg, peer), device_id_type=MESH,
        )

    def bulk(ref, recv):
        return remote(ref, ref, recv, partner, h)

    def send_in(k, seg):
        return remote(mixed_out.at[k, seg], mixed_in.at[k, s], in_recv.at[k], seg, h)

    def send_pair(p, seg):
        source = mixed_out.at[alone + p, pl.ds(2 * lax.rem(seg, 2), 2)]
        return remote(source, pair_in.at[p, s], pair_recv.at[p], seg, h)

    def send_gate(d):
        peer = ch_peer(d)
        return remote(gate.at[:, :, :, part_of(peer)], gates.at[h], g_recv, s, peer)

    def send_weight(d):
        return remote(weight, weights.at[h], w_recv.at[0], s, flipped(h, d))

    def pass_weight(d):
        owner = flipped(h, d)
        return remote(weights.at[owner], weights.at[owner], w_recv.at[1], s, flipped(h, 1))

    def mix_part(k, seg):
        def mix(j, carry):
            both = keys[k, seg, :, lanes(j)].astype(f32) * values[k, seg, :, lanes(j)].astype(f32)
            wide[pl.ds(j, chans, stride=step), :] = both
            return carry

        lax.fori_loop(0, slabs, mix, 0, unroll=4)
        for i in range(chans):
            mixed_out[k, seg, i] = wide[i * step : i * step + slabs, :].astype(bf16)

    def cross(k):
        @pl.when(side == 0)
        def _():
            if k >= alone:
                send_pair(k - alone, 2).start()
            else:
                send_in(k, 2).start()

        @pl.when(side == 1)
        def _():
            if k < alone:
                send_in(k, 0).start()
                send_in(k, 1).start()

    def spread_rest(k):
        @pl.when(side == 0)
        def _():
            if k < alone:
                send_in(k, 3).start()
            else:
                send_pair(k - alone, 3).start()

        if k < alone:
            send_in(k, partner).start()
        else:
            send_pair(k - alone, partner).start()

    for n, k in enumerate(seq):
        if n < len(stages):
            for copy in load_kv(*stages[n]) if n else load_half(0):
                copy.wait()
        if n == 0:
            mix_part(k, 0)
            mix_part(k, 1)

            @pl.when(s == 1)
            def _():
                pl.semaphore_wait(barrier, 1)
                send_pair(0, 2).start()

            @pl.when(s == 0)
            def _():
                pl.semaphore_wait(barrier, groups + 1)
                send_pair(0, 2).start()
                for d in range(1, groups):
                    tell(plane, s, ch_peer(d))

            @pl.when(s == 2)
            def _():
                pl.semaphore_wait(barrier, groups + 1)

            @pl.when(s == tail)
            def _():
                pl.semaphore_wait(barrier, groups + 2)
                for seg in (2, 1, 0):
                    tell(joined, seg, h)

            for copy in load_kv(*stages[2]):
                copy.start()
            for copy in load_half(1):
                copy.wait()
            mix_part(k, 2)
            mix_part(k, 3)

            @pl.when(s != 1)
            def _():
                for d in direct:
                    send_weight(d).start()
        else:
            for seg in (2, 3, 0, 1):
                mix_part(k, seg)
            cross(k)
        if n == 1:
            for copy in loads:
                copy.start()
        if n == 2:

            @pl.when(s == 0)
            def _():
                pl.semaphore_wait(plane, groups - 1)
                tell(released, 1, h)

            @pl.when(s != tail)
            def _():
                pl.semaphore_wait(joined, 1)

            @pl.when(s != 1)
            def _():
                for d in range(1, segs):
                    tell(ready, seg_peer(d), h)

            for e in seq[:n]:
                spread_rest(e)
        if n >= 2:
            spread_rest(k)
        if n == 3:

            @pl.when(s == 1)
            def _():
                pl.semaphore_wait(released, 1)
                for d in range(1, segs):
                    tell(ready, seg_peer(d), h)
                for d in direct:
                    send_weight(d).start()

        if k < alone:
            mixed_in[k, s] = mixed_out[k, s]
        else:
            for e in range(2):
                pair_in[k - alone, s, e] = mixed_out[k, 2 * low + e]

            @pl.when(side == 0)
            def _():
                for seg in (2, 3):
                    pair_in[k - alone, seg] = jnp.zeros((2, chans, slabs, lane_width), bf16)

    for d in range(1, groups):
        send_gate(d).start()

    for copy in loads:
        copy.wait()
    for k in [*range(alone, alone + 2 * pairs), *range(alone)]:

        def spread(j, carry):
            tall[pl.ds(j, chans, stride=long_step), :] = taps[k, :, lanes(j)]
            return carry

        lax.fori_loop(0, outer, spread, 0, unroll=4)
        signal = [tall[i * long_step : i * long_step + outer, :].astype(bf16) for i in range(chans)]
        out = forward(signal, first[...], inner[...], cos_t[...], sin_t[...])
        spectrum[k] = out.astype(bf16).reshape(chans, outer, 2 * lane_width)
    pl.semaphore_wait(ready, segs - 1)

    def slot(k, q):
        return chunks - 1 + q if k == alone - 1 else k if k < alone else k - 1

    def convolve_rows(at, rows_of, row):
        signal = [rows_of(i).reshape(outer, lane_width) for i in range(chans)]
        filt = spectrum[at].reshape(chans * outer, 2 * lane_width)
        tables = (first[...], last[...], inner[...], inner_back[...], cos_t[...], sin_t[...])
        parts = convolve_block(tables, signal, filt)
        for i in range(chans):
            long[i * long_step : i * long_step + outer, :] = parts[i] + skip[row + i] * signal[i].astype(f32)

    for p in range(pairs):
        k = alone + p

        @pl.when(side == 0)
        def _():
            bulk(pair_in.at[p, 0], pair_recv.at[p]).wait_recv()

        @pl.when(side == 1)
        def _():
            bulk(pair_in.at[p, pl.ds(0, segs - 1)], pair_recv.at[p]).wait_recv()

        for e in range(2):
            convolve_rows(k + p + e, lambda i: pair_in[p, :, e, i], (k * segs + 2 * low + e) * chans)

            def gather(j, carry):
                from_row = side * (outer // 2) + j
                pair_out[p, e, j] = long[pl.ds(from_row, chans, stride=long_step), :].astype(bf16)
                return carry

            lax.fori_loop(0, outer // 2, gather, 0, unroll=8)
        for d in range(2):
            seg = s if d else partner

            def send(e, carry):
                peer = ch_peer(groups - 1 - e)
                rows = pl.ds(lax.rem(seg, 2) * slabs + peer * quads, quads)
                target = conv_in.at[k, h, pl.ds(2 * low, 2)]
                remote(pair_out.at[p, :, rows], target, out_recv.at[slot(k, 0)], seg, peer).start()
                return carry

            lax.fori_loop(0, groups - d, send, 0)
        for e in range(2):
            for q in range(quads):
                conv_in[k, h, 2 * low + e, q] = pair_out[p, e, low * slabs + h * quads + q]

    for k in range(alone):
        bulk(mixed_in.at[k, pl.ds(0, segs - 1)], in_recv.at[k]).wait_recv()
        convolve_rows(k, lambda i: mixed_in[k, :, i], (k * segs + s) * chans)

        def gather(j, carry):
            conv_out[k, j] = long[pl.ds(j, chans, stride=long_step), :].astype(bf16)
            return carry

        lax.fori_loop(0, outer, gather, 0, unroll=8)
        if k < alone - 1:
            batches = [(0, quads, 0, groups)]
        else:
            batches = [(q, 1, 0, 2) for q in range(quads)] + [(q, 1, 2, groups) for q in range(quads)]
        for q, size, low_peer, high_peer in batches:
            for d in (2, 3, 1, 0):
                seg = seg_peer(d)

                def send(e, carry):
                    peer = low_peer + lax.rem(h + e, high_peer - low_peer) if k == alone - 1 else ch_peer(groups - 1 - e)

                    def go():
                        source = conv_out.at[k, pl.ds(seg * slabs + peer * quads + q, size)]
                        target = conv_in.at[k, h, s, pl.ds(q, size)]
                        remote(source, target, out_recv.at[slot(k, q)], seg, peer).start()

                    if d:
                        go()
                    else:
                        pl.when(peer != h)(go)
                    return carry

                lax.fori_loop(0, high_peer - low_peer, send, 0)
        for q in range(quads):
            conv_in[k, h, s, q] = conv_out[k, s * slabs + h * quads + q]

    def restack(owner):
        def move(k, into):
            for at in range(0, segs, 2):
                pair = [weights[owner, k, at + e].astype(f32) for e in range(2)]
                rows = pl.ds(pl.multiple_of(owner * block + at * chans, 2 * chans), 2 * chans)
                into[rows, :] = jnp.concatenate(pair, axis=0).astype(bf16)

        def step_of(n, carry):
            move(lax.rem(n + alone, chunks), stacked.at[n])
            return carry

        lax.fori_loop(0, chunks - 1, step_of, 0)
        move(alone - 1, ending_weight)

    order = list(range(alone, chunks)) + list(range(alone))
    bulk(weights.at[pl.ds(0, len(direct))], w_recv.at[0]).wait_recv()
    for d in passed:
        pass_weight(d).start()
    for d in [0] + direct:
        restack(flipped(h, d))
    bulk(gates.at[pl.ds(0, groups - 1)], g_recv).wait_recv()
    bulk(weights.at[pl.ds(0, len(passed))], w_recv.at[1]).wait_recv()
    for d in passed:
        restack(flipped(h, d + 1))

    def all_pieces(k, q, size):
        if k < alone:
            ref = conv_out.at[k, pl.ds(0, (segs * groups - 1) * size)]
        else:
            ref = pair_out.at[k - alone, :, pl.ds(0, outer // 2 - quads)]
        return bulk(ref, out_recv.at[slot(k, q)])

    steps = [(k, 0, quads) for k in order[:-1]] + [(order[-1], q, 1) for q in range(quads)]
    for n, (k, start, size) in enumerate(steps):
        all_pieces(k, start, size).wait_recv()
        ends = n == len(steps) - 1
        into = ending if ends else gated
        shift = start if ends else 0
        weight_of = ending_weight if k == order[-1] else stacked.at[n]

        def combine(g, carry):
            for at in range(0, segs, 2):
                for q in range(start, start + size):
                    both = [
                        conv_in[k, g, at + e, q].astype(f32)
                        * gates[g, k, at + e, :, q * lane_width : (q + 1) * lane_width].astype(f32)
                        for e in range(2)
                    ]
                    rows = pl.ds(pl.multiple_of(g * block + at * chans, 2 * chans), 2 * chans)
                    at_q = slice((q - shift) * lane_width, (q - shift + 1) * lane_width)
                    into[rows, at_q] = jnp.concatenate(both, axis=0).astype(bf16)
            return carry

        lax.fori_loop(0, groups, combine, 0, unroll=2)
        if ends:
            continue
        tokens_at = slice(start * lane_width, (start + size) * lane_width)
        left = gated[:, tokens_at]
        for c in range(features // cols):
            at = slice(c * cols, (c + 1) * cols)
            prod = lax.dot_general(
                left, weight_of[:, at], (((0,), (0,)), ((), ())), preferred_element_type=f32
            )
            if k == order[0]:
                total[:, at] = prod
            elif k == order[-1]:
                result[tokens_at, at] = (total[tokens_at, at] + prod).astype(bf16)
            elif k != order[-2]:
                total[:, at] += prod
            else:
                early = result.shape[0]
                total[:, at] += prod
                rest[:, at] = total[early:, at]

    bulk(mixed_in.at[:, pl.ds(0, segs - 1)], g_recv).wait_send()
    for p in range(pairs):

        @pl.when(side == 0)
        def _():
            bulk(pair_in.at[p, pl.ds(0, segs - 1)], g_recv).wait_send()

        @pl.when(side == 1)
        def _():
            bulk(pair_in.at[p, 0], g_recv).wait_send()

    bulk(gates.at[pl.ds(0, groups - 1)], g_recv).wait_send()
    bulk(weights.at[pl.ds(0, groups - 1)], g_recv).wait_send()
    for k, start, size in steps:
        all_pieces(k, start, size).wait_send()


def finish_kernel(result, rest, ending, ending_weight, output, final, sem):
    early = result.shape[0]
    copies = [pltpu.make_async_copy(result, output.at[pl.ds(0, early)], sem.at[0])]
    copies[0].start()
    blocks = sem.shape[0] - 1
    cols = final.shape[1] // blocks
    for c in range(blocks):
        at = slice(c * cols, (c + 1) * cols)
        prod = lax.dot_general(
            ending[...], ending_weight[:, at], (((0,), (0,)), ((), ())), preferred_element_type=f32
        )
        final[:, at] = (rest[:, at] + prod).astype(bf16)
        target = output.at[pl.ds(early, final.shape[0]), pl.ds(c * cols, cols)]
        copies.append(pltpu.make_async_copy(final.at[:, pl.ds(c * cols, cols)], target, sem.at[1 + c]))
        copies[-1].start()
    for copy in copies:
        copy.wait()


def whole_layer(gate_in, key_in, value_in, kernel, skip_gain, out_weight, chans):
    segs, groups = lax.axis_size("seg"), lax.axis_size("ch")
    channels, tokens = key_in.shape
    full_len = kernel.shape[1]
    outer = full_len // lane_width
    slabs = tokens // lane_width
    features = out_weight.shape[1]
    chunks = channels // segs // chans
    pairs = 1
    alone = chunks - pairs
    share = tokens // groups
    quads = share // lane_width
    tables = make_tables(outer)
    split = (chunks, segs, chans)
    args = (
        *tables,
        skip_gain,
        key_in.reshape(*split, tokens),
        value_in.reshape(*split, tokens),
        gate_in.reshape(*split, tokens),
        kernel.reshape(*split, full_len),
        out_weight.reshape(*split, features),
    )
    hbm = pl.BlockSpec(memory_space=pltpu.HBM)
    dma = pltpu.SemaphoreType.DMA
    regular = pltpu.SemaphoreType.REGULAR
    tall = pltpu.VMEM((chans * (outer + 8), lane_width), f32)
    early = share - lane_width
    vmem = pl.BlockSpec(memory_space=pltpu.VMEM)
    parts = pl.pallas_call(
        layer_kernel,
        in_specs=[hbm] * len(args),
        out_specs=[vmem] * 4,
        out_shape=[
            pltpu.VMEM((early, features), bf16),
            pltpu.VMEM((lane_width, features), f32),
            pltpu.VMEM((groups * segs * chans, lane_width), bf16),
            pltpu.VMEM((groups * segs * chans, features), bf16),
        ],
        scratch_shapes=[pltpu.VMEM(a.shape, a.dtype) for a in tables]
        + [
            pltpu.SMEM(skip_gain.shape, f32),
            pltpu.VMEM((*split, tokens), bf16),
            pltpu.VMEM((*split, tokens), bf16),
            pltpu.VMEM((alone + 2 * pairs, chans, full_len), f32),
            tall,
            pltpu.VMEM((chans * (slabs + 8), lane_width), f32),
            tall,
            pltpu.VMEM((alone + 2 * pairs, chans, outer, 2 * lane_width), bf16),
            pltpu.VMEM((*split, slabs, lane_width), bf16),
            pltpu.VMEM((alone, segs, chans, slabs, lane_width), bf16),
            pltpu.VMEM((pairs, segs, 2, chans, slabs, lane_width), bf16),
            pltpu.VMEM((alone, outer, chans, lane_width), bf16),
            pltpu.VMEM((pairs, 2, outer // 2, chans, lane_width), bf16),
            pltpu.VMEM((chunks, groups, segs, quads, chans, lane_width), bf16),
            pltpu.VMEM((groups, *split, share), bf16),
            pltpu.VMEM((groups, *split, features), bf16),
            pltpu.VMEM((chunks - 1, groups * segs * chans, features), bf16),
            pltpu.VMEM((groups * segs * chans, share), bf16),
            pltpu.VMEM((share, features), f32),
            dma((4,)), dma, regular, regular, regular, regular, dma, dma((alone,)), dma((pairs,)), dma((chunks - 1 + quads,)), dma, dma((2,)),
        ],
        compiler_params=pltpu.CompilerParams(
            collective_id=0, has_side_effects=True, vmem_limit_bytes=56 * 1024 * 1024
        ),
        name="layer",
    )(*args)
    return pl.pallas_call(
        finish_kernel,
        in_specs=[vmem] * 4,
        out_specs=hbm,
        out_shape=jax.ShapeDtypeStruct((share, features), bf16),
        scratch_shapes=[
            pltpu.VMEM((lane_width, features), bf16),
            dma((1 + (features // 512 if features % 512 == 0 else 1),)),
        ],
        compiler_params=pltpu.CompilerParams(vmem_limit_bytes=4 * 1024 * 1024),
        name="finish",
    )(*parts)


def on_device(gate_in, key_in, value_in, kernel, skip_gain, out_weight):
    seg_count = lax.axis_size("seg")
    seg_index = lax.axis_index("seg")
    channels, tokens = key_in.shape
    full_len = kernel.shape[1]
    outer = full_len // lane_width
    tables = make_tables(outer)
    col_count = channels // seg_count
    sublanes = 8
    fits = (seg_count, lax.axis_size("ch")) == (4, 8) and col_count % sublanes == 0 and col_count > sublanes
    if fits and tokens // lax.axis_size("ch") % lane_width == 0:
        return whole_layer(gate_in, key_in, value_in, kernel, skip_gain, out_weight, sublanes)
    mixed = key_in.astype(f32) * value_in.astype(f32)
    mixed_sent = mixed.astype(bf16).reshape(channels, tokens // lane_width, lane_width)
    col_mixed = lax.all_to_all(mixed_sent, "seg", split_axis=0, concat_axis=1, tiled=True)
    taps = lax.dynamic_slice_in_dim(kernel, seg_index * col_count, col_count, 0)
    spectrum = transform_filter(tables, taps.astype(bf16).reshape(col_count, outer, lane_width))
    col_conv = convolve(tables, col_mixed, spectrum)
    conv = lax.all_to_all(col_conv, "seg", split_axis=1, concat_axis=0, tiled=True)
    conv = conv.reshape(channels, tokens).astype(f32)
    gated = (gate_in.astype(f32) * (conv + skip_gain[:, None] * mixed)).astype(bf16)
    mine = lax.all_to_all(gated, "ch", split_axis=1, concat_axis=0, tiled=True)
    weight = lax.all_gather(out_weight, "ch", axis=0, tiled=True)
    result = lax.dot_general(
        mine, weight, (((0,), (0,)), ((), ())), preferred_element_type=f32
    )
    return result.astype(bf16)


def solution(mesh):
    placed = (P("ch", "seg"), P("ch", "seg"), P("ch", "seg"), P("ch", None), P("ch"), P("ch", None))
    return jax.shard_map(
        on_device, mesh=mesh, in_specs=placed, out_specs=P(("seg", "ch"), None), check_vma=False
    )
```
